32 devices in a mesh: lat: 4 (over y, core), lon: 8 (over z, x).
Axes of the slice: x: 2, y: 2, z: 4, core: 2. Of those that a mesh axis runs over, the one named last changes fastest.
Arguments:
- forcing: float32 [640, 1024], P('lat', 'lon'), may hold values from -28 to 28
- search_direction: float32 [640, 1024], P('lat', 'lon'), may hold values from -28 to 28
- ocean_depth: float32 [640, 1024], P('lat', 'lon'), may hold values from 0.5 to 8
- land_mask: int32 [640, 1024], P('lat', 'lon'), may hold values 0 or 1
- fold_map: int32 [1024], replicated, may hold values from 0 to 1023, as said below
Outputs:
- scaled_height: float32 [640, 1024], P('lat', 'lon')
- residual: float32 [640, 1024], P('lat', 'lon')
The draws below stay inside these ranges and needn't reach their ends.
Inputs may be any that keep to these rules, and one draw needn't show every extreme that they name: `fold_map`: column j's partner across the fold is (c - j) mod 1024 for one c of 0 to 1023, so the map is its own inverse.
All inputs are finite; a program needn't handle non-finite values. No bound on the sum of `land_mask` on one device may be relied on, other than what follows from the above.
Results may differ from the reference program's by a relative error of at most 0.0003.
Values sent between devices are 32-bit elements; how exact they have to be, the bound alone decides.
A program may use at most 64 MiB of HBM per device.

```python
import math
import jax
import jax.numpy as jnp
import numpy as np
from jax import lax

STEPS = 8
OUTER = 1
REACH = 256
NX = 640
NY = 1024


def field_profile():
    lat_ramp = jnp.arange(NX, dtype=jnp.float32) / NX
    lon_ramp = jnp.arange(NY, dtype=jnp.float32) / NY
    north_gap = (NX - 1 - jnp.arange(NX, dtype=jnp.float32)) / 8.0
    north_boost = 1.0 + 1.5 * jnp.exp(-north_gap)
    return jnp.exp(jnp.log(3.0) * (lat_ramp[:, None] + lon_ramp[None, :])) * north_boost[:, None]


def rough_field(key):
    first_key = jax.random.fold_in(key, 0)
    values = jax.random.truncated_normal(first_key, -4.0, 4.0, (NX, NY), jnp.float32)
    return (0.3 * values * field_profile()).astype(jnp.float32)


def draw_forcing(key, part):
    return rough_field(jax.random.fold_in(key, 11))


def draw_search_direction(key, part):
    return rough_field(jax.random.fold_in(key, 23))


def draw_fold_map(key, part):
    pivot_column = jax.random.randint(jax.random.fold_in(key, 7), (), 0, NY, dtype=jnp.int32)
    return ((pivot_column - jnp.arange(NY, dtype=jnp.int32)) % NY).astype(jnp.int32)


def set_ends(drawn, stream_key, smallest, top_value):
    longest = drawn.shape.index(max(drawn.shape))
    spots = []
    for shift in (0, 1):
        where = [jax.random.randint(jax.random.fold_in(stream_key, axis), (), 0, length) for axis, length in enumerate(drawn.shape)]
        where[longest] = (where[longest] + shift) % drawn.shape[longest]
        spots.append(tuple(where))
    return drawn.at[spots[0]].set(smallest).at[spots[1]].set(top_value)


def level_of(key, extent, pieces, low, largest):
    level = 1.0
    for dim, shards_of in pieces:
        draws = jax.random.uniform(jax.random.fold_in(jax.random.fold_in(key, 6), dim), (shards_of,), jnp.float32, low / len(pieces), largest / len(pieces))
        level = level * jnp.repeat(jnp.exp(draws), extent[dim] // shards_of).reshape((-1,) + (1,) * (len(extent) - 1 - dim))
    return level


def setup_inputs(seed: int = 0) -> dict:
    key_of = jax.random.split(jax.random.key(seed), 6)
    forcing = draw_forcing(jax.random.fold_in(key_of[5], 71), 0)
    search_direction = draw_search_direction(jax.random.fold_in(key_of[5], 71), 0)
    ocean_depth = jnp.clip(jnp.exp(math.log(8.0) - 2.7725887 * jax.random.uniform(key_of[2], (NX, NY), jnp.float32) ** level_of(key_of[2], (NX, NY), ((0, 4), (1, 8)), -0.2, 0.2)), 0.5, 8.0)
    land_mask = set_ends((jax.random.randint(key_of[3], (NX, NY), 0, 8) < 7).astype(jnp.int32), jax.random.fold_in(key_of[3], 1), 0, 1)
    fold_map = draw_fold_map(jax.random.fold_in(key_of[5], 71), 0)
    return dict(forcing=forcing, search_direction=search_direction, ocean_depth=ocean_depth, land_mask=land_mask, fold_map=fold_map)


PRECISE = lax.Precision.HIGHEST
DIRECTIONS = ((1, 0), (-1, 0), (0, 1), (0, -1), (1, 1), (-1, -1), (1, -1), (-1, 1))
LINK_FACTORS = (1.0, 1.0, 1.0, 1.0, 0.5, 0.5, 0.5, 0.5)

def chebyshev_table(basis_steps):
    number = 2 * basis_steps + 1
    matrix = np.zeros((number, number), np.float32)
    for offset, length in ((0, basis_steps + 1), (basis_steps + 1, basis_steps)):
        for column in range(length - 1):
            matrix[offset + column, offset + column] = 1.0
            if column == 0:
                matrix[offset + 1, offset] = 1.0
            else:
                matrix[offset + column + 1, offset + column] = 0.5
                matrix[offset + column - 1, offset + column] = 0.5
    return matrix

def coordinates(gram_matrix, basis_steps):
    number = 2 * basis_steps + 1
    shift_matrix = jnp.asarray(chebyshev_table(basis_steps))
    unit_rows = jnp.eye(number, dtype=jnp.float32)
    solution_coords = jnp.zeros((number,), jnp.float32)
    direction_coords = unit_rows[0]
    residual_coords = unit_rows[basis_steps + 1]
    norm_now = jnp.dot(residual_coords, jnp.dot(gram_matrix, residual_coords, precision=PRECISE), precision=PRECISE)
    for inner_step in range(basis_steps):
        mapped = jnp.dot(shift_matrix, direction_coords, precision=PRECISE)
        curvature = jnp.dot(direction_coords, jnp.dot(gram_matrix, mapped, precision=PRECISE), precision=PRECISE)
        step_length = norm_now / curvature
        solution_coords = solution_coords + step_length * direction_coords
        residual_coords = residual_coords - step_length * mapped
        norm_next = jnp.dot(residual_coords, jnp.dot(gram_matrix, residual_coords, precision=PRECISE), precision=PRECISE)
        direction_coords = residual_coords + norm_next / norm_now * direction_coords
        norm_now = norm_next
    return (solution_coords, residual_coords, direction_coords)

def pad_ghosts(source, fold_map):
    fold_row = jnp.take(source[-1], fold_map)
    zeros_row = jnp.zeros((1, source.shape[1]), source.dtype)
    stacked = jnp.concatenate([zeros_row, source, fold_row[None, :]], axis=0)
    return jnp.concatenate([stacked[:, -1:], stacked, stacked[:, :1]], axis=1)

def neighbour(padded, north_step, east_step):
    row_total = padded.shape[0] - 2
    column_total = padded.shape[1] - 2
    return padded[1 + north_step:1 + north_step + row_total, 1 + east_step:1 + east_step + column_total]

def reference(forcing, search_direction, ocean_depth, land_mask, fold_map):
    ocean_flag = land_mask.astype(jnp.float32)
    column_depth = ocean_depth * ocean_flag
    padded_depth = pad_ghosts(column_depth, fold_map)
    padded_wet = (padded_depth > 0.0).astype(jnp.float32)
    centre_wet = padded_wet[1:-1, 1:-1]
    weight_list = []
    link_sum = jnp.zeros_like(column_depth)
    for direction_index in range(8):
        north_step, east_step = DIRECTIONS[direction_index]
        weight = LINK_FACTORS[direction_index] * 0.5 * (column_depth + neighbour(padded_depth, north_step, east_step)) * centre_wet * neighbour(padded_wet, north_step, east_step)
        weight_list.append(weight)
        link_sum = link_sum + weight
    diagonal = centre_wet * (column_depth / (REACH * REACH) + link_sum) + (1.0 - centre_wet)
    inverse_root = lax.rsqrt(diagonal)

    def operate(source):
        padded = pad_ghosts(inverse_root * source, fold_map)
        running = jnp.zeros_like(source)
        for direction_index in range(8):
            north_step, east_step = DIRECTIONS[direction_index]
            running = running + weight_list[direction_index] * neighbour(padded, north_step, east_step)
        return -inverse_root * running
    operate_many = jax.vmap(operate)
    scaled_height = jnp.zeros_like(forcing)
    residual = ocean_flag * forcing
    direction = ocean_flag * search_direction
    for outer_step in range(OUTER):
        earlier = jnp.stack([direction, residual])
        current = operate_many(earlier)
        stored = [earlier, current]
        for power in range(1, STEPS):
            if power == STEPS - 1:
                earlier = earlier[:1]
                current = current[:1]
            upcoming = 2.0 * operate_many(current) - earlier
            earlier = current
            current = upcoming
            stored.append(current)
        krylov_basis = jnp.stack([member[0] for member in stored] + [member[1] for member in stored[:STEPS]])
        flattened = krylov_basis.reshape(krylov_basis.shape[0], -1)
        gram_matrix = jnp.dot(flattened, flattened.T, precision=PRECISE)
        solution_coords, residual_coords, direction_coords = coordinates(gram_matrix, STEPS)
        scaled_height = scaled_height + jnp.einsum('k,kij->ij', solution_coords, krylov_basis, precision=PRECISE)
        residual = jnp.einsum('k,kij->ij', residual_coords, krylov_basis, precision=PRECISE)
        direction = jnp.einsum('k,kij->ij', direction_coords, krylov_basis, precision=PRECISE)
    return (scaled_height, residual)
```

```python
import functools

import jax
import jax.numpy as jnp
from jax import lax
from jax.experimental import pallas as pl
from jax.experimental.pallas import tpu as pltpu
from jax.sharding import PartitionSpec as P

STEPS = 8
REACH = 256
MESH = pl.DeviceIdType.MESH
PAD = 16
GROUP = 32
CHUNK = 16
DIRECT_LIMIT = 64

DIRECTIONS = ((1, 0), (-1, 0), (0, 1), (0, -1), (1, 1), (-1, -1), (1, -1), (-1, 1))
SLOT = {offset: index for index, offset in enumerate(DIRECTIONS)}


def halves(offset):
    return 0.5 if 0 in offset else 0.25


def chunks_of(low, high, size):
    return [(at, min(size, high - at)) for at in range(low, high, size)]


def shift_pair(centre, halo, step):
    width = centre.shape[1]
    lane = lax.broadcasted_iota(jnp.int32, centre.shape, 1)
    edge = lane == (0 if step == 1 else width - 1)
    turn = width - 1 if step == 1 else 1
    return (
        pltpu.roll(jnp.where(edge, halo, centre), turn, 1),
        pltpu.roll(jnp.where(edge, centre, halo), turn, 1),
    )


def turned(x, shift):
    shift = shift % x.shape[1]
    return x if shift == 0 else pltpu.roll(x, shift, 1)


def bilinear(left, right, gram):
    total = None
    for i in sorted(left):
        inner = None
        for j in sorted(right):
            term = gram(i, j) * right[j]
            inner = term if inner is None else inner + term
        inner = left[i] * inner
        total = inner if total is None else total + inner
    return total


def plus(left, right):
    result = dict(left)
    for key, value in right.items():
        result[key] = result[key] + value if key in result else value
    return result


def scaled(factor, vector):
    return {key: factor * value for key, value in vector.items()}


def apply_shift(vector):
    result = {}
    for (chain, power), value in vector.items():
        parts = [((chain, power), value)]
        if power == 0:
            parts.append(((chain, 1), value))
        else:
            half = 0.5 * value
            parts += [((chain, power + 1), half), ((chain, power - 1), half)]
        result = plus(result, {}) if not parts else result
        for key, part in parts:
            result = plus(result, {key: part})
    return result


def coordinates(moments):
    cache = {}

    def gram(left, right):
        kind = (left[0], right[0]) if left[0] <= right[0] else (right[0], left[0])
        low, high = sorted((left[1], right[1]))
        key = (kind, low, high)
        if key not in cache:
            series = moments[kind]
            cache[key] = 0.5 * (series[high + low] + series[high - low])
        return cache[key]

    solution_coords = {}
    one = jnp.ones_like(moments[("p", "p")][0])
    direction_coords = {("p", 0): one}
    residual_coords = {("r", 0): one}
    norm_now = bilinear(residual_coords, residual_coords, gram)
    for _ in range(STEPS):
        mapped = apply_shift(direction_coords)
        step_length = norm_now / bilinear(direction_coords, mapped, gram)
        solution_coords = plus(solution_coords, scaled(step_length, direction_coords))
        residual_coords = plus(residual_coords, scaled(-step_length, mapped))
        norm_next = bilinear(residual_coords, residual_coords, gram)
        direction_coords = plus(
            residual_coords, scaled(norm_next / norm_now, direction_coords)
        )
        norm_now = norm_next
    return solution_coords, residual_coords


def fold_sublanes(parts):
    row = lax.broadcasted_iota(jnp.int32, parts[0].shape, 0)
    parts = list(parts)
    span = 4
    while span:
        low = (row & span) == 0
        half = len(parts) // 2
        parts = [
            jnp.where(low, first, second)
            + pltpu.roll(jnp.where(low, second, first), span, 0)
            if span == 4
            else jnp.where(low, first, second)
            + jnp.where(low, pltpu.roll(first, 8 - span, 0), pltpu.roll(second, span, 0))
            for first, second in zip(parts[:half], parts[half:])
        ]
        span //= 2
    return parts[0]


def kernel(
    n_lat, n_lon, forcing_hbm, search_hbm, depth_hbm, mask_hbm, fold_hbm,
    out_height, out_residual, forcing, search, depth_in, mask_in, fold_map,
    depth, depth_e, depth_w, root, root_e, root_w, weights, basis, basis_halo,
    row_north, row_south, fold_rows, packed, got_north, got_south, got_east, got_west,
    corners, fold_all, dots, sums_lat, sums_lon, sums_all, moment_rows, load_sem,
    near_send, near_recv, fold_send, fold_recv, lat_send, lat_recv, lon_send, lon_recv,
    all_send, all_recv,
):
    rows, width = forcing_hbm.shape
    lat, lon = lax.axis_index("lat"), lax.axis_index("lon")
    top = n_lat - 1
    north, south = lax.rem(lat + 1, n_lat), lax.rem(lat + n_lat - 1, n_lat)
    east, west = lax.rem(lon + 1, n_lon), lax.rem(lon + n_lon - 1, n_lon)
    has_north, has_south = lat < top, lat > 0
    group_rows = rows * GROUP // width
    n_groups = width // GROUP

    barrier = pltpu.get_barrier_semaphore()

    def greet(place):
        pl.semaphore_signal(barrier, inc=1, device_id=place, device_id_type=MESH)

    loads = [
        pltpu.make_async_copy(source, target, load_sem.at[index])
        for index, (source, target) in enumerate(
            ((mask_hbm, mask_in), (depth_hbm, depth_in), (search_hbm, search),
             (forcing_hbm, forcing), (fold_hbm, fold_map))
        )
    ]
    for load in loads:
        load.start()
    direct = n_lat * n_lon <= DIRECT_LIMIT
    everyone = [(a, b) for a in range(n_lat) for b in range(n_lon) if a or b]
    everyone.sort(key=lambda d: -min(d[0], n_lat - d[0]) - min(d[1], n_lon - d[1]))
    if direct:
        for a, b in everyone:
            greet((lax.rem(lat + a, n_lat), lax.rem(lon + b, n_lon)))
        greeted = len(everyone)
    else:
        for d in range(1, n_lat):
            greet((lax.rem(lat + d, n_lat), lon))
        for d in range(1, n_lon):
            greet((lat, lax.rem(lon + d, n_lon)))
        for place in ((north, east), (north, west), (south, east), (south, west)):
            greet(place)
        greeted = n_lat - 1 + n_lon - 1 + 4

    for load in loads:
        load.wait()
    lane_group = lax.broadcasted_iota(jnp.int32, (group_rows, width), 1)
    west_edge = east_edge = None
    for g in range(n_groups):
        here = pl.ds(g * group_rows, group_rows)
        there = pl.ds(PAD + g * group_rows, group_rows)
        flag = mask_in[here, :].astype(jnp.float32)
        deep = depth_in[here, :] * flag
        moving = search[here, :] * flag
        left = forcing[here, :] * flag
        depth[0, there, :] = deep
        basis[0, there, :] = moving
        basis[STEPS + 1, there, :] = left
        inside = lane_group - g * GROUP
        to_west = jnp.where(
            inside < 9,
            turned(deep, g * GROUP),
            jnp.where(inside < 17, turned(moving, g * GROUP + 9), turned(left, g * GROUP + 17)),
        )
        to_east = jnp.where(
            inside < 9,
            turned(deep, g * GROUP + 9),
            jnp.where(inside < 17, turned(moving, g * GROUP + 17), turned(left, g * GROUP + 25)),
        )
        west_edge = to_west if g == 0 else jnp.where(inside >= 0, to_west, west_edge)
        east_edge = to_east if g == 0 else jnp.where(inside >= 0, to_east, east_edge)
    packed[0] = west_edge
    packed[1] = east_edge
    first, last = PAD, PAD + rows
    row_south[0:16, :] = depth[0, first : first + 16, :]
    row_south[16:24, :] = basis[0, first : first + 8, :]
    row_south[24:32, :] = basis[STEPS + 1, first : first + 8, :]
    row_north[0:16, :] = depth[0, last - 16 : last, :]
    row_north[16:24, :] = basis[0, last - 8 : last, :]
    row_north[24:32, :] = basis[STEPS + 1, last - 8 : last, :]

    @pl.when(lat == top)
    def _():
        for r in range(16):
            fold_rows[r : r + 1, :] = depth[0, last - 1 - r : last - r, :]
        for r in range(8):
            fold_rows[16 + r : 17 + r, :] = basis[0, last - 1 - r : last - r, :]
            fold_rows[24 + r : 25 + r, :] = basis[STEPS + 1, last - 1 - r : last - r, :]
        fold_all[lon] = fold_rows[...]

    pl.semaphore_wait(barrier, greeted)

    def near(index, source, target, place):
        return pltpu.make_async_remote_copy(
            src_ref=source, dst_ref=target, send_sem=near_send.at[index],
            recv_sem=near_recv.at[index], device_id=place, device_id_type=MESH,
        )

    tail = pl.ds(group_rows - 16, 16)
    head = pl.ds(0, 16)
    to_north = near(0, row_north, got_south, (north, lon))
    to_south = near(1, row_south, got_north, (south, lon))
    to_east = near(2, packed.at[1], got_west, (lat, east))
    to_west = near(3, packed.at[0], got_east, (lat, west))
    to_ne = near(4, packed.at[1, tail], corners.at[0], (north, east))
    to_nw = near(5, packed.at[0, tail], corners.at[1], (north, west))
    to_se = near(6, packed.at[1, head], corners.at[2], (south, east))
    to_sw = near(7, packed.at[0, head], corners.at[3], (south, west))
    northward, southward = (to_north, to_ne, to_nw), (to_south, to_se, to_sw)

    def spread(source, slots, send_sem, recv_sem, along_lat):
        size = n_lat if along_lat else n_lon
        me = lat if along_lat else lon
        copies = []
        for d in range(1, size):
            peer = lax.rem(me + d, size)
            copies.append(
                pltpu.make_async_remote_copy(
                    src_ref=source, dst_ref=slots.at[me], send_sem=send_sem.at[d - 1],
                    recv_sem=recv_sem.at[d - 1],
                    device_id=(peer, lon) if along_lat else (lat, peer),
                    device_id_type=MESH,
                )
            )
        return copies

    across = spread(fold_rows, fold_all, fold_send, fold_recv, False)

    @pl.when(lat == top)
    def _():
        for copy in across:
            copy.start()

    to_east.start()
    to_west.start()

    @pl.when(has_north)
    def _():
        for copy in northward:
            copy.start()

    @pl.when(has_south)
    def _():
        for copy in southward:
            copy.start()

    def unpack(got_e, got_w, start, g, count):
        lane = lax.broadcasted_iota(jnp.int32, (count, width), 1)
        base = -g * GROUP
        spans = ((0, 9, depth.at[1]), (9, 8, basis_halo.at[0]), (17, 8, basis_halo.at[STEPS + 1]))
        for offset, cells, target in spans:
            from_east = turned(got_e, base - offset)
            from_west = turned(got_w, base - offset - cells)
            target[start : start + count, :] = jnp.where(
                lane < cells,
                from_east,
                jnp.where(lane >= width - cells, from_west, jnp.zeros_like(got_e)),
            )

    to_east.wait_recv()
    to_west.wait_recv()
    for g in range(n_groups):
        unpack(got_east[...], got_west[...], PAD + g * group_rows, g, group_rows)

    @pl.when(has_south)
    def _():
        for copy in northward:
            copy.wait_recv()
        depth[0, 0:16, :] = got_south[0:16, :]
        basis[0, 8:16, :] = got_south[16:24, :]
        basis[STEPS + 1, 8:16, :] = got_south[24:32, :]
        unpack(corners[1], corners[0], 0, n_groups - 1, 16)

    @pl.when(lat == 0)
    def _():
        nothing = jnp.zeros((16, width), jnp.float32)
        for target in (depth.at[0], depth.at[1]):
            target[0:16, :] = nothing
        for power in (0, STEPS + 1):
            basis[power, 0:16, :] = nothing
            basis_halo[power, 0:16, :] = nothing

    @pl.when(has_north)
    def _():
        for copy in southward:
            copy.wait_recv()
        depth[0, last : last + 16, :] = got_north[0:16, :]
        basis[0, last : last + 8, :] = got_north[16:24, :]
        basis[STEPS + 1, last : last + 8, :] = got_north[24:32, :]
        unpack(corners[3], corners[2], last, 0, 16)

    @pl.when(lat == top)
    def _():
        for copy in across:
            copy.wait_recv()
        total = n_lon * width
        pivot = lax.rem(fold_map[0] - lon * width + total, total)
        block, offset = pivot // width, lax.rem(pivot, width)
        lane = lax.broadcasted_iota(jnp.int32, (32, width), 1)
        index = lax.rem(offset - lane + width, width)

        def mirrored(which):
            rows_of = fold_all[lax.rem(block + which + n_lon, n_lon)]
            return jnp.take_along_axis(rows_of, index, axis=1, mode="promise_in_bounds")

        ahead, same, behind, beyond = (mirrored(which) for which in (1, 0, -1, -2))
        close = lane <= offset
        centre = jnp.where(close, same, behind)
        halo = jnp.where(
            lane < width // 2, jnp.where(close, behind, beyond), jnp.where(close, ahead, same)
        )
        for value, deep, fields in ((centre, depth.at[0], basis), (halo, depth.at[1], basis_halo)):
            deep[last : last + 16, :] = value[0:16, :]
            fields[0, last : last + 8, :] = value[16:24, :]
            fields[STEPS + 1, last : last + 8, :] = value[24:32, :]

    low, high = PAD - 8, last + 8
    for at, count in chunks_of(0, rows + 2 * PAD, CHUNK):
        span = pl.ds(at, count)
        centre, halo = depth[0, span, :], depth[1, span, :]
        depth_e[0, span, :], depth_e[1, span, :] = shift_pair(centre, halo, 1)
        depth_w[0, span, :], depth_w[1, span, :] = shift_pair(centre, halo, -1)
    shifted_depth = {0: depth, 1: depth_e, -1: depth_w}
    for at, count in chunks_of(low, high, CHUNK):
        roots = []
        for tile in (0, 1):
            here = depth[tile, at : at + count, :]
            sums = {0.5: None, 0.25: None}
            for a, b in DIRECTIONS:
                beside = shifted_depth[b][tile, at + a : at + a + count, :]
                link = jnp.where(beside > 0.0, here + beside, 0.0)
                factor = halves((a, b))
                sums[factor] = link if sums[factor] is None else sums[factor] + link
            diagonal = here * (1.0 / (REACH * REACH)) + (0.5 * sums[0.5] + 0.25 * sums[0.25])
            value = lax.rsqrt(jnp.where(here > 0.0, diagonal, 1.0))
            root[tile, at : at + count, :] = value
            roots.append(value)
        span = pl.ds(at, count)
        root_e[0, span, :], root_e[1, span, :] = shift_pair(roots[0], roots[1], 1)
        root_w[0, span, :], root_w[1, span, :] = shift_pair(roots[0], roots[1], -1)
    shifted_root = {0: root, 1: root_e, -1: root_w}
    for at, count in chunks_of(low, high, CHUNK):
        for tile in (0, 1):
            for b in (-1, 0, 1):
                goal_depth = shifted_depth[-b][tile, at : at + count, :]
                goal_root = shifted_root[-b][tile, at : at + count, :]
                goal_wet = goal_depth > 0.0
                for a in (-1, 0, 1):
                    if (a, b) == (0, 0):
                        continue
                    from_depth = depth[tile, at + a : at + a + count, :]
                    from_root = root[tile, at + a : at + a + count, :]
                    link = jnp.where(
                        jnp.minimum(goal_depth, from_depth) > 0.0, goal_depth + from_depth, 0.0
                    )
                    weights[SLOT[(a, b)], tile, at : at + count, :] = (
                        goal_root * (-2.0 * halves((a, b)))
                    ) * (link * from_root)

    dot_sums = {}

    def add_dot(key, left, right):
        product = left * right
        for r in range(0, product.shape[0], 8):
            piece = product[r : r + 8, :]
            dot_sums[key] = piece if key not in dot_sums else dot_sums[key] + piece

    row_chunks = [(low, 8)] + chunks_of(first, last, CHUNK) + [(last, 8)]
    for at, count in chunks_of(first, last, CHUNK):
        p0 = basis[0, at : at + count, :]
        r0 = basis[STEPS + 1, at : at + count, :]
        add_dot(("p", "p", 0), p0, p0)
        add_dot(("r", "r", 0), r0, r0)
        add_dot(("p", "r", 0), p0, r0)

    for power in range(1, STEPS + 1):
        chains = [("p", 0, power == STEPS)]
        if power < STEPS:
            chains.append(("r", STEPS + 1, power == STEPS - 1))
        for at, count in row_chunks:
            inner = first <= at < last
            fresh = {}
            held = {}
            factors = [
                {ab: weights[SLOT[ab], tile, at : at + count, :] for ab in DIRECTIONS}
                for tile in (0, 1)
            ]
            for name, origin, only_block in chains:
                if only_block and not inner:
                    continue
                slot = origin + power
                parts = []
                for tile, fields in ((0, basis), (1, basis_halo)):
                    taken = {
                        a: fields[slot - 1, at + a : at + a + count, :] for a in (-1, 0, 1)
                    }
                    if tile == 0:
                        held[name] = taken[0]
                    columns = {}
                    for b in (-1, 0, 1):
                        total = None
                        for a in (-1, 0, 1):
                            if (a, b) == (0, 0):
                                continue
                            term = factors[tile][(a, b)] * taken[a]
                            total = term if total is None else total + term
                        columns[b] = total
                    parts.append(columns)
                ahead = shift_pair(parts[0][1], parts[1][1], 1)
                behind = shift_pair(parts[0][-1], parts[1][-1], -1)
                for tile, fields in ((0, basis), (1, basis_halo)):
                    if tile == 1 and only_block:
                        continue
                    value = parts[tile][0] + ahead[tile] + behind[tile]
                    if power == 1:
                        value = 0.5 * value
                    else:
                        value = value - fields[slot - 2, at : at + count, :]
                    fields[slot, at : at + count, :] = value
                    if tile == 0:
                        fresh[name] = value
            if not inner:
                continue
            for name, _, _ in chains:
                add_dot((name, name, 2 * power), fresh[name], fresh[name])
                add_dot((name, name, 2 * power - 1), fresh[name], held[name])
            if power < STEPS:
                add_dot(("p", "r", 2 * power), fresh["p"], fresh["r"])
                add_dot(("p", "r", 2 * power - 1), fresh["p"], held["r"])
            else:
                add_dot(
                    ("p", "r", 2 * power - 1),
                    fresh["p"],
                    basis[STEPS + power, at : at + count, :],
                )
        for key in [key for key in dot_sums]:
            dots[order_of()[key]] = dot_sums.pop(key)

    number = len(order_of())
    pending = []
    lane = lax.broadcasted_iota(jnp.int32, (8, width), 1)
    home = lane - lax.broadcasted_iota(jnp.int32, (8, width), 0)
    message = jnp.zeros((8, width), jnp.float32)
    for g in range(number // 8):
        grouped = fold_sublanes([dots[8 * g + s] for s in range(8)])
        message = jnp.where(home == 8 * g, jnp.sum(grouped, axis=1, keepdims=True), message)
    message = jnp.sum(message, axis=0, keepdims=True)
    if direct:
        me = lat * n_lon + lon
        sums_all[me] = message
        copies = [
            pltpu.make_async_remote_copy(
                src_ref=sums_all.at[me], dst_ref=sums_all.at[me], send_sem=all_send.at[index],
                recv_sem=all_recv.at[index],
                device_id=(lax.rem(lat + a, n_lat), lax.rem(lon + b, n_lon)),
                device_id_type=MESH,
            )
            for index, (a, b) in enumerate(everyone)
        ]
        rounds = ((sums_all, n_lat * n_lon, copies),)
    else:
        rounds = (
            (sums_lat, n_lat, None, lat, True, lat_send, lat_recv),
            (sums_lon, n_lon, None, lon, False, lon_send, lon_recv),
        )
    for slots, size, copies, *rest in rounds:
        if copies is None:
            me, along_lat, send_sem, recv_sem = rest
            slots[me] = message
            copies = spread(slots.at[me], slots, send_sem, recv_sem, along_lat)
        for copy in copies:
            copy.start()
        for copy in copies:
            copy.wait_recv()
        terms = [slots[index] for index in range(size)]
        while len(terms) > 1:
            odd = terms[len(terms) // 2 * 2 :]
            terms = [x + y for x, y in zip(terms[0::2], terms[1::2])] + odd
        message = terms[0]
        pending.extend(copies)
    message = jnp.broadcast_to(message, (8, width))
    for g in range(number // 8):
        picked = jnp.sum(jnp.where(home == 8 * g, message, 0.0), axis=1, keepdims=True)
        moment_rows[8 * g : 8 * g + 8, :] = jnp.broadcast_to(picked, (8, width))
    moments = {}
    for kind in (("p", "p"), ("p", "r"), ("r", "r")):
        series = []
        for index in range(17 if kind == ("p", "p") else 16 if kind == ("p", "r") else 15):
            spot = order_of()[kind + (index,)]
            value = jnp.broadcast_to(moment_rows[spot : spot + 1, :], (8, width))
            series.append(value if index < 2 else 2.0 * value - series[index % 2])
        moments[kind] = series
    height_coords, residual_coords = coordinates(moments)
    for at in range(0, rows, 8):
        for coords, out in ((height_coords, out_height), (residual_coords, out_residual)):
            total = None
            for (chain, power), factor in sorted(coords.items(), key=lambda item: item[0]):
                slot = power + (0 if chain == "p" else STEPS + 1)
                term = factor * basis[slot, PAD + at : PAD + at + 8, :]
                total = term if total is None else total + term
            out[at : at + 8, :] = total

    for copy in pending:
        copy.wait_send()
    to_east.wait_send()
    to_west.wait_send()

    @pl.when(has_north)
    def _():
        for copy in northward:
            copy.wait_send()

    @pl.when(has_south)
    def _():
        for copy in southward:
            copy.wait_send()

    @pl.when(lat == top)
    def _():
        for copy in across:
            copy.wait_send()


@functools.cache
def order_of():
    keys = [("p", "p", k) for k in range(2 * STEPS + 1)]
    keys += [("p", "r", k) for k in range(2 * STEPS)]
    keys += [("r", "r", k) for k in range(2 * STEPS - 1)]
    return {key: index for index, key in enumerate(keys)}


def hand_over(height, residual, out_height, out_residual):
    out_height[...] = height[...]
    out_residual[...] = residual[...]


def per_device(n_lat, n_lon, forcing, search_direction, ocean_depth, land_mask, fold_map):
    rows, width = forcing.shape
    tall = rows + 2 * PAD
    f32 = jnp.float32
    own = pltpu.VMEM((rows, width), f32)
    pair = pltpu.VMEM((2, tall, width), f32)
    edge = pltpu.VMEM((32, width), f32)
    group_rows = rows * GROUP // width
    strip = pltpu.VMEM((group_rows, width), f32)
    everyone = n_lat * n_lon if n_lat * n_lon <= DIRECT_LIMIT else 2
    dma = pltpu.SemaphoreType.DMA
    block = pl.BlockSpec(memory_space=pltpu.VMEM)
    outs = pl.pallas_call(
        functools.partial(kernel, n_lat, n_lon),
        out_shape=[pltpu.VMEM((rows, width), f32)] * 2,
        in_specs=[pl.BlockSpec(memory_space=pl.ANY)] * 5,
        out_specs=[block] * 2,
        scratch_shapes=[
            own, own, own, pltpu.VMEM((rows, width), jnp.int32),
            pltpu.SMEM(fold_map.shape, jnp.int32),
            pair, pair, pair, pair, pair, pair,
            pltpu.VMEM((8, 2, tall, width), f32),
            pltpu.VMEM((2 * STEPS + 1, tall, width), f32),
            pltpu.VMEM((2 * STEPS + 1, tall, width), f32),
            edge, edge, edge,
            pltpu.VMEM((2, group_rows, width), f32),
            edge, edge, strip, strip,
            pltpu.VMEM((4, 16, width), f32),
            pltpu.VMEM((n_lon, 32, width), f32),
            pltpu.VMEM((6 * STEPS, 8, width), f32),
            pltpu.VMEM((n_lat, 1, width), f32),
            pltpu.VMEM((n_lon, 1, width), f32),
            pltpu.VMEM((everyone, 1, width), f32),
            pltpu.VMEM((6 * STEPS, width), f32),
            dma((5,)),
            dma((8,)), dma((8,)),
            dma((n_lon - 1,)), dma((n_lon - 1,)),
            dma((n_lat - 1,)), dma((n_lat - 1,)),
            dma((n_lon - 1,)), dma((n_lon - 1,)),
            dma((everyone - 1,)), dma((everyone - 1,)),
        ],
        compiler_params=pltpu.CompilerParams(collective_id=0, has_side_effects=True),
        name="tripole_cg",
    )(forcing, search_direction, ocean_depth, land_mask, fold_map)
    return pl.pallas_call(
        hand_over,
        out_shape=[jax.ShapeDtypeStruct((rows, width), f32)] * 2,
        in_specs=[block] * 2,
        out_specs=[block] * 2,
        name="hand_over",
    )(*(pltpu.with_memory_space_constraint(out, pltpu.VMEM) for out in outs))


def solution(mesh):
    cells = P("lat", "lon")
    return jax.shard_map(
        functools.partial(per_device, mesh.shape["lat"], mesh.shape["lon"]),
        mesh=mesh,
        in_specs=(cells, cells, cells, cells, P()),
        out_specs=(cells, cells),
        check_vma=False,
    )
```

```python
import functools

import jax
import jax.numpy as jnp
from jax import lax
from jax.experimental import pallas as pl
from jax.experimental.pallas import tpu as pltpu
from jax.sharding import PartitionSpec as P

STEPS = 8
REACH = 256
MESH = pl.DeviceIdType.MESH
PAD = 16
GROUP = 32
CHUNK = 16
DIRECT_LIMIT = 64

DIRECTIONS = ((1, 0), (-1, 0), (0, 1), (0, -1), (1, 1), (-1, -1), (1, -1), (-1, 1))
SLOT = {offset: index for index, offset in enumerate(DIRECTIONS)}


def halves(offset):
    return 0.5 if 0 in offset else 0.25


def chunks_of(low, high, size):
    return [(at, min(size, high - at)) for at in range(low, high, size)]


def shift_pair(centre, halo, step):
    width = centre.shape[1]
    lane = lax.broadcasted_iota(jnp.int32, centre.shape, 1)
    edge = lane == (0 if step == 1 else width - 1)
    turn = width - 1 if step == 1 else 1
    return (
        pltpu.roll(jnp.where(edge, halo, centre), turn, 1),
        pltpu.roll(jnp.where(edge, centre, halo), turn, 1),
    )


def turned(x, shift):
    shift = shift % x.shape[1]
    return x if shift == 0 else pltpu.roll(x, shift, 1)


def bilinear(left, right, gram):
    total = None
    for i in sorted(left):
        inner = None
        for j in sorted(right):
            term = gram(i, j) * right[j]
            inner = term if inner is None else inner + term
        inner = left[i] * inner
        total = inner if total is None else total + inner
    return total


def plus(left, right):
    result = dict(left)
    for key, value in right.items():
        result[key] = result[key] + value if key in result else value
    return result


def scaled(factor, vector):
    return {key: factor * value for key, value in vector.items()}


def apply_shift(vector):
    result = {}
    for (chain, power), value in vector.items():
        parts = [((chain, power), value)]
        if power == 0:
            parts.append(((chain, 1), value))
        else:
            half = 0.5 * value
            parts += [((chain, power + 1), half), ((chain, power - 1), half)]
        result = plus(result, {}) if not parts else result
        for key, part in parts:
            result = plus(result, {key: part})
    return result


def coordinates(moments):
    cache = {}

    def gram(left, right):
        kind = (left[0], right[0]) if left[0] <= right[0] else (right[0], left[0])
        low, high = sorted((left[1], right[1]))
        key = (kind, low, high)
        if key not in cache:
            series = moments[kind]
            cache[key] = 0.5 * (series[high + low] + series[high - low])
        return cache[key]

    solution_coords = {}
    one = jnp.ones_like(moments[("p", "p")][0])
    direction_coords = {("p", 0): one}
    residual_coords = {("r", 0): one}
    norm_now = bilinear(residual_coords, residual_coords, gram)
    for _ in range(STEPS):
        mapped = apply_shift(direction_coords)
        step_length = norm_now / bilinear(direction_coords, mapped, gram)
        solution_coords = plus(solution_coords, scaled(step_length, direction_coords))
        residual_coords = plus(residual_coords, scaled(-step_length, mapped))
        norm_next = bilinear(residual_coords, residual_coords, gram)
        direction_coords = plus(
            residual_coords, scaled(norm_next / norm_now, direction_coords)
        )
        norm_now = norm_next
    return solution_coords, residual_coords


def fold_sublanes(parts):
    row = lax.broadcasted_iota(jnp.int32, parts[0].shape, 0)
    parts = list(parts)
    span = 4
    while span:
        low = (row & span) == 0
        half = len(parts) // 2
        parts = [
            jnp.where(low, first, second)
            + pltpu.roll(jnp.where(low, second, first), span, 0)
            if span == 4
            else jnp.where(low, first, second)
            + jnp.where(low, pltpu.roll(first, 8 - span, 0), pltpu.roll(second, span, 0))
            for first, second in zip(parts[:half], parts[half:])
        ]
        span //= 2
    return parts[0]


def kernel(
    n_lat, n_lon, forcing_hbm, search_hbm, depth_hbm, mask_hbm, fold_hbm,
    out_height, out_residual, loaded, mask_in, fold_map,
    depth, depth_e, depth_w, root, root_e, root_w, weights, basis, basis_halo,
    row_north, row_south, fold_rows, packed, got_rows, got_sides,
    fold_all, dots, moment_rows, load_sem, near_send, near_recv, *moment_refs,
):
    rows, width = forcing_hbm.shape
    lat, lon = lax.axis_index("lat"), lax.axis_index("lon")
    top = n_lat - 1
    north, south = lax.rem(lat + 1, n_lat), lax.rem(lat + n_lat - 1, n_lat)
    east, west = lax.rem(lon + 1, n_lon), lax.rem(lon + n_lon - 1, n_lon)
    has_north, has_south = lat < top, lat > 0
    group_rows = rows * GROUP // width
    n_groups = width // GROUP

    barrier = pltpu.get_barrier_semaphore()

    def greet(place):
        pl.semaphore_signal(barrier, inc=1, device_id=place, device_id_type=MESH)

    for source, target, index in (
        (mask_hbm, mask_in, 0), (depth_hbm, loaded.at[0], 1), (search_hbm, loaded.at[1], 1),
        (forcing_hbm, loaded.at[2], 1), (fold_hbm, fold_map, 2),
    ):
        pltpu.make_async_copy(source, target, load_sem.at[index]).start()
    depth_in, search, forcing = loaded.at[0], loaded.at[1], loaded.at[2]
    direct = n_lat * n_lon <= DIRECT_LIMIT
    everyone = [(a, b) for a in range(n_lat) for b in range(n_lon) if a or b]
    everyone.sort(key=lambda d: -min(d[0], n_lat - d[0]) - min(d[1], n_lon - d[1]))
    if direct:
        for a, b in everyone:
            greet((lax.rem(lat + a, n_lat), lax.rem(lon + b, n_lon)))
        greeted = len(everyone)
    else:
        for d in range(1, n_lat):
            greet((lax.rem(lat + d, n_lat), lon))
        for d in range(1, n_lon):
            greet((lat, lax.rem(lon + d, n_lon)))
        for place in ((north, east), (north, west), (south, east), (south, west)):
            greet(place)
        greeted = n_lat - 1 + n_lon - 1 + 4

    pltpu.make_async_copy(mask_hbm, mask_in, load_sem.at[0]).wait()
    pltpu.make_async_copy(loaded, loaded, load_sem.at[1]).wait()
    pltpu.make_async_copy(fold_hbm, fold_map, load_sem.at[2]).wait()
    lane_group = lax.broadcasted_iota(jnp.int32, (group_rows, width), 1)
    west_edge = east_edge = None
    for g in range(n_groups):
        here = pl.ds(g * group_rows, group_rows)
        there = pl.ds(PAD + g * group_rows, group_rows)
        flag = mask_in[here, :].astype(jnp.float32)
        deep = depth_in[here, :] * flag
        moving = search[here, :] * flag
        left = forcing[here, :] * flag
        depth[0, there, :] = deep
        basis[0, there, :] = moving
        basis[STEPS + 1, there, :] = left
        inside = lane_group - g * GROUP
        to_west = jnp.where(
            inside < 9,
            turned(deep, g * GROUP),
            jnp.where(inside < 17, turned(moving, g * GROUP + 9), turned(left, g * GROUP + 17)),
        )
        to_east = jnp.where(
            inside < 9,
            turned(deep, g * GROUP + 9),
            jnp.where(inside < 17, turned(moving, g * GROUP + 17), turned(left, g * GROUP + 25)),
        )
        west_edge = to_west if g == 0 else jnp.where(inside >= 0, to_west, west_edge)
        east_edge = to_east if g == 0 else jnp.where(inside >= 0, to_east, east_edge)
    packed[0] = west_edge
    packed[1] = east_edge
    first, last = PAD, PAD + rows
    row_south[0:16, :] = depth[0, first : first + 16, :]
    row_south[16:24, :] = basis[0, first : first + 8, :]
    row_south[24:32, :] = basis[STEPS + 1, first : first + 8, :]
    row_north[0:16, :] = depth[0, last - 16 : last, :]
    row_north[16:24, :] = basis[0, last - 8 : last, :]
    row_north[24:32, :] = basis[STEPS + 1, last - 8 : last, :]

    @pl.when(lat == top)
    def _():
        for r in range(16):
            fold_rows[r : r + 1, :] = depth[0, last - 1 - r : last - r, :]
        for r in range(8):
            fold_rows[16 + r : 17 + r, :] = basis[0, last - 1 - r : last - r, :]
            fold_rows[24 + r : 25 + r, :] = basis[STEPS + 1, last - 1 - r : last - r, :]
        fold_all[lon] = fold_rows[...]

    pl.semaphore_wait(barrier, greeted)

    def near(index, source, target, place):
        return pltpu.make_async_remote_copy(
            src_ref=source, dst_ref=target, send_sem=near_send.at[index],
            recv_sem=near_recv.at[index], device_id=place, device_id_type=MESH,
        )

    tail = pl.ds(group_rows - 16, 16)
    head = pl.ds(0, 16)
    got_south, got_north = got_rows.at[0, 0:32], got_rows.at[1, 0:32]
    got_west, got_east = got_sides.at[0], got_sides.at[1]
    corners = [got_rows.at[index // 2, pl.ds(32 + 16 * (index % 2), 16)] for index in range(4)]
    northward = (
        near(0, row_north, got_south, (north, lon)),
        near(0, packed.at[1, tail], corners[0], (north, east)),
        near(0, packed.at[0, tail], corners[1], (north, west)),
    )
    southward = (
        near(1, row_south, got_north, (south, lon)),
        near(1, packed.at[1, head], corners[2], (south, east)),
        near(1, packed.at[0, head], corners[3], (south, west)),
    )
    to_east = near(2, packed.at[1], got_west, (lat, east))
    to_west = near(2, packed.at[0], got_east, (lat, west))

    def arrival(index, block):
        return near(index, block, block, (lat, lon))

    from_south, from_north = arrival(0, got_rows.at[0]), arrival(1, got_rows.at[1])
    from_sides = arrival(2, got_sides)
    from_fold = arrival(3, fold_all.at[0 : n_lon - 1])

    def spread(source, slots, send_sem, recv_sem, along_lat):
        size = n_lat if along_lat else n_lon
        me = lat if along_lat else lon
        copies = []
        for d in range(1, size):
            peer = lax.rem(me + d, size)
            copies.append(
                pltpu.make_async_remote_copy(
                    src_ref=source, dst_ref=slots.at[me], send_sem=send_sem,
                    recv_sem=recv_sem,
                    device_id=(peer, lon) if along_lat else (lat, peer),
                    device_id_type=MESH,
                )
            )
        return copies

    across = spread(fold_rows, fold_all, near_send.at[3], near_recv.at[3], False)

    @pl.when(lat == top)
    def _():
        for copy in across:
            copy.start()

    to_east.start()
    to_west.start()

    @pl.when(has_north)
    def _():
        for copy in northward:
            copy.start()

    @pl.when(has_south)
    def _():
        for copy in southward:
            copy.start()

    def unpack(got_e, got_w, start, g, count):
        lane = lax.broadcasted_iota(jnp.int32, (count, width), 1)
        base = -g * GROUP
        spans = ((0, 9, depth.at[1]), (9, 8, basis_halo.at[0]), (17, 8, basis_halo.at[STEPS + 1]))
        for offset, cells, target in spans:
            from_east = turned(got_e, base - offset)
            from_west = turned(got_w, base - offset - cells)
            target[start : start + count, :] = jnp.where(
                lane < cells,
                from_east,
                jnp.where(lane >= width - cells, from_west, jnp.zeros_like(got_e)),
            )

    from_sides.wait_recv()
    for g in range(n_groups):
        unpack(got_east[...], got_west[...], PAD + g * group_rows, g, group_rows)

    @pl.when(has_south)
    def _():
        from_south.wait_recv()
        depth[0, 0:16, :] = got_south[0:16, :]
        basis[0, 8:16, :] = got_south[16:24, :]
        basis[STEPS + 1, 8:16, :] = got_south[24:32, :]
        unpack(corners[1][...], corners[0][...], 0, n_groups - 1, 16)

    @pl.when(lat == 0)
    def _():
        nothing = jnp.zeros((16, width), jnp.float32)
        for target in (depth.at[0], depth.at[1]):
            target[0:16, :] = nothing
        for power in (0, STEPS + 1):
            basis[power, 0:16, :] = nothing
            basis_halo[power, 0:16, :] = nothing

    @pl.when(has_north)
    def _():
        from_north.wait_recv()
        depth[0, last : last + 16, :] = got_north[0:16, :]
        basis[0, last : last + 8, :] = got_north[16:24, :]
        basis[STEPS + 1, last : last + 8, :] = got_north[24:32, :]
        unpack(corners[3][...], corners[2][...], last, 0, 16)

    @pl.when(lat == top)
    def _():
        from_fold.wait_recv()
        total = n_lon * width
        pivot = lax.rem(fold_map[0] - lon * width + total, total)
        block, offset = pivot // width, lax.rem(pivot, width)
        lane = lax.broadcasted_iota(jnp.int32, (32, width), 1)
        index = lax.rem(offset - lane + width, width)

        def mirrored(which):
            rows_of = fold_all[lax.rem(block + which + n_lon, n_lon)]
            return jnp.take_along_axis(rows_of, index, axis=1, mode="promise_in_bounds")

        ahead, same, behind, beyond = (mirrored(which) for which in (1, 0, -1, -2))
        close = lane <= offset
        centre = jnp.where(close, same, behind)
        halo = jnp.where(
            lane < width // 2, jnp.where(close, behind, beyond), jnp.where(close, ahead, same)
        )
        for value, deep, fields in ((centre, depth.at[0], basis), (halo, depth.at[1], basis_halo)):
            deep[last : last + 16, :] = value[0:16, :]
            fields[0, last : last + 8, :] = value[16:24, :]
            fields[STEPS + 1, last : last + 8, :] = value[24:32, :]

    low, high = PAD - 8, last + 8
    for at, count in chunks_of(0, rows + 2 * PAD, CHUNK):
        span = pl.ds(at, count)
        centre, halo = depth[0, span, :], depth[1, span, :]
        depth_e[0, span, :], depth_e[1, span, :] = shift_pair(centre, halo, 1)
        depth_w[0, span, :], depth_w[1, span, :] = shift_pair(centre, halo, -1)
    shifted_depth = {0: depth, 1: depth_e, -1: depth_w}
    for at, count in chunks_of(low, high, CHUNK):
        roots = []
        for tile in (0, 1):
            here = depth[tile, at : at + count, :]
            sums = {0.5: None, 0.25: None}
            for a, b in DIRECTIONS:
                beside = shifted_depth[b][tile, at + a : at + a + count, :]
                link = jnp.where(beside > 0.0, here + beside, 0.0)
                factor = halves((a, b))
                sums[factor] = link if sums[factor] is None else sums[factor] + link
            diagonal = here * (1.0 / (REACH * REACH)) + (0.5 * sums[0.5] + 0.25 * sums[0.25])
            value = lax.rsqrt(jnp.where(here > 0.0, diagonal, 1.0))
            root[tile, at : at + count, :] = value
            roots.append(value)
        span = pl.ds(at, count)
        root_e[0, span, :], root_e[1, span, :] = shift_pair(roots[0], roots[1], 1)
        root_w[0, span, :], root_w[1, span, :] = shift_pair(roots[0], roots[1], -1)
    shifted_root = {0: root, 1: root_e, -1: root_w}
    for at, count in chunks_of(low, high, CHUNK):
        for tile in (0, 1):
            for b in (-1, 0, 1):
                goal_depth = shifted_depth[-b][tile, at : at + count, :]
                goal_root = shifted_root[-b][tile, at : at + count, :]
                goal_wet = goal_depth > 0.0
                for a in (-1, 0, 1):
                    if (a, b) == (0, 0):
                        continue
                    from_depth = depth[tile, at + a : at + a + count, :]
                    from_root = root[tile, at + a : at + a + count, :]
                    link = jnp.where(
                        jnp.minimum(goal_depth, from_depth) > 0.0, goal_depth + from_depth, 0.0
                    )
                    weights[SLOT[(a, b)], tile, at : at + count, :] = (
                        goal_root * (-2.0 * halves((a, b)))
                    ) * (link * from_root)

    dot_sums = {}

    def add_dot(key, left, right):
        product = left * right
        for r in range(0, product.shape[0], 8):
            piece = product[r : r + 8, :]
            dot_sums[key] = piece if key not in dot_sums else dot_sums[key] + piece

    row_chunks = [(low, 8)] + chunks_of(first, last, CHUNK) + [(last, 8)]
    for at, count in chunks_of(first, last, CHUNK):
        p0 = basis[0, at : at + count, :]
        r0 = basis[STEPS + 1, at : at + count, :]
        add_dot(("p", "p", 0), p0, p0)
        add_dot(("r", "r", 0), r0, r0)
        add_dot(("p", "r", 0), p0, r0)

    for power in range(1, STEPS + 1):
        chains = [("p", 0, power == STEPS)]
        if power < STEPS:
            chains.append(("r", STEPS + 1, power == STEPS - 1))
        for at, count in row_chunks:
            inner = first <= at < last
            fresh = {}
            held = {}
            factors = [
                {ab: weights[SLOT[ab], tile, at : at + count, :] for ab in DIRECTIONS}
                for tile in (0, 1)
            ]
            for name, origin, only_block in chains:
                if only_block and not inner:
                    continue
                slot = origin + power
                parts = []
                for tile, fields in ((0, basis), (1, basis_halo)):
                    taken = {
                        a: fields[slot - 1, at + a : at + a + count, :] for a in (-1, 0, 1)
                    }
                    if tile == 0:
                        held[name] = taken[0]
                    columns = {}
                    for b in (-1, 0, 1):
                        total = None
                        for a in (-1, 0, 1):
                            if (a, b) == (0, 0):
                                continue
                            term = factors[tile][(a, b)] * taken[a]
                            total = term if total is None else total + term
                        columns[b] = total
                    parts.append(columns)
                ahead = shift_pair(parts[0][1], parts[1][1], 1)
                behind = shift_pair(parts[0][-1], parts[1][-1], -1)
                for tile, fields in ((0, basis), (1, basis_halo)):
                    if tile == 1 and only_block:
                        continue
                    value = parts[tile][0] + ahead[tile] + behind[tile]
                    if power == 1:
                        value = 0.5 * value
                    else:
                        value = value - fields[slot - 2, at : at + count, :]
                    fields[slot, at : at + count, :] = value
                    if tile == 0:
                        fresh[name] = value
            if not inner:
                continue
            for name, _, _ in chains:
                add_dot((name, name, 2 * power), fresh[name], fresh[name])
                add_dot((name, name, 2 * power - 1), fresh[name], held[name])
            if power < STEPS:
                add_dot(("p", "r", 2 * power), fresh["p"], fresh["r"])
                add_dot(("p", "r", 2 * power - 1), fresh["p"], held["r"])
            else:
                add_dot(
                    ("p", "r", 2 * power - 1),
                    fresh["p"],
                    basis[STEPS + power, at : at + count, :],
                )
        for key in [key for key in dot_sums]:
            dots[order_of()[key]] = dot_sums.pop(key)

    number = len(order_of())
    pending = []
    lane = lax.broadcasted_iota(jnp.int32, (8, width), 1)
    home = lane - lax.broadcasted_iota(jnp.int32, (8, width), 0)
    message = jnp.zeros((8, width), jnp.float32)
    for g in range(number // 8):
        grouped = fold_sublanes([dots[8 * g + s] for s in range(8)])
        message = jnp.where(home == 8 * g, jnp.sum(grouped, axis=1, keepdims=True), message)
    message = jnp.sum(message, axis=0, keepdims=True)
    if direct:
        slots, send_sem, recv_sem = moment_refs
        me = lat * n_lon + lon
        slots[me] = message
        copies = [
            pltpu.make_async_remote_copy(
                src_ref=slots.at[me], dst_ref=slots.at[me], send_sem=send_sem,
                recv_sem=recv_sem,
                device_id=(lax.rem(lat + a, n_lat), lax.rem(lon + b, n_lon)),
                device_id_type=MESH,
            )
            for a, b in everyone
        ]
        rounds = ((slots, n_lat * n_lon, copies, send_sem, recv_sem),)
    else:
        slots_lat, slots_lon, lat_send, lat_recv, lon_send, lon_recv = moment_refs
        rounds = (
            (slots_lat, n_lat, None, lat_send, lat_recv, lat, True),
            (slots_lon, n_lon, None, lon_send, lon_recv, lon, False),
        )
    for slots, size, copies, send_sem, recv_sem, *rest in rounds:
        if copies is None:
            me, along_lat = rest
            slots[me] = message
            copies = spread(slots.at[me], slots, send_sem, recv_sem, along_lat)
        for copy in copies:
            copy.start()
        others = slots.at[0 : size - 1]
        whole = pltpu.make_async_remote_copy(
            src_ref=others, dst_ref=others, send_sem=send_sem, recv_sem=recv_sem,
            device_id=(lat, lon), device_id_type=MESH,
        )
        whole.wait_recv()
        terms = [slots[index] for index in range(size)]
        while len(terms) > 1:
            odd = terms[len(terms) // 2 * 2 :]
            terms = [x + y for x, y in zip(terms[0::2], terms[1::2])] + odd
        message = terms[0]
        pending.append(whole)
    message = jnp.broadcast_to(message, (8, width))
    for g in range(number // 8):
        picked = jnp.sum(jnp.where(home == 8 * g, message, 0.0), axis=1, keepdims=True)
        moment_rows[8 * g : 8 * g + 8, :] = jnp.broadcast_to(picked, (8, width))
    moments = {}
    for kind in (("p", "p"), ("p", "r"), ("r", "r")):
        series = []
        for index in range(17 if kind == ("p", "p") else 16 if kind == ("p", "r") else 15):
            spot = order_of()[kind + (index,)]
            value = jnp.broadcast_to(moment_rows[spot : spot + 1, :], (8, width))
            series.append(value if index < 2 else 2.0 * value - series[index % 2])
        moments[kind] = series
    height_coords, residual_coords = coordinates(moments)
    for at in range(0, rows, 8):
        for coords, out in ((height_coords, out_height), (residual_coords, out_residual)):
            total = None
            for (chain, power), factor in sorted(coords.items(), key=lambda item: item[0]):
                slot = power + (0 if chain == "p" else STEPS + 1)
                term = factor * basis[slot, PAD + at : PAD + at + 8, :]
                total = term if total is None else total + term
            out[at : at + 8, :] = total

    for copy in pending:
        copy.wait_send()
    from_sides.wait_send()

    @pl.when(has_north)
    def _():
        from_south.wait_send()

    @pl.when(has_south)
    def _():
        from_north.wait_send()

    @pl.when(lat == top)
    def _():
        from_fold.wait_send()


@functools.cache
def order_of():
    keys = [("p", "p", k) for k in range(2 * STEPS + 1)]
    keys += [("p", "r", k) for k in range(2 * STEPS)]
    keys += [("r", "r", k) for k in range(2 * STEPS - 1)]
    return {key: index for index, key in enumerate(keys)}


def hand_over(height, residual, out_height, out_residual):
    out_height[...] = height[...]
    out_residual[...] = residual[...]


def per_device(n_lat, n_lon, forcing, search_direction, ocean_depth, land_mask, fold_map):
    rows, width = forcing.shape
    tall = rows + 2 * PAD
    f32 = jnp.float32
    pair = pltpu.VMEM((2, tall, width), f32)
    edge = pltpu.VMEM((32, width), f32)
    group_rows = rows * GROUP // width
    dma = pltpu.SemaphoreType.DMA
    if n_lat * n_lon <= DIRECT_LIMIT:
        moment_refs = [pltpu.VMEM((n_lat * n_lon, 1, width), f32), dma, dma]
    else:
        moment_refs = [pltpu.VMEM((size, 1, width), f32) for size in (n_lat, n_lon)] + [dma] * 4
    block = pl.BlockSpec(memory_space=pltpu.VMEM)
    outs = pl.pallas_call(
        functools.partial(kernel, n_lat, n_lon),
        out_shape=[pltpu.VMEM((rows, width), f32)] * 2,
        in_specs=[pl.BlockSpec(memory_space=pl.ANY)] * 5,
        out_specs=[block] * 2,
        scratch_shapes=[
            pltpu.VMEM((3, rows, width), f32), pltpu.VMEM((rows, width), jnp.int32),
            pltpu.SMEM(fold_map.shape, jnp.int32),
            pair, pair, pair, pair, pair, pair,
            pltpu.VMEM((8, 2, tall, width), f32),
            pltpu.VMEM((2 * STEPS + 1, tall, width), f32),
            pltpu.VMEM((2 * STEPS + 1, tall, width), f32),
            edge, edge, edge,
            pltpu.VMEM((2, group_rows, width), f32),
            pltpu.VMEM((2, 64, width), f32),
            pltpu.VMEM((2, group_rows, width), f32),
            pltpu.VMEM((n_lon, 32, width), f32),
            pltpu.VMEM((6 * STEPS, 8, width), f32),
            pltpu.VMEM((6 * STEPS, width), f32),
            dma((3,)), dma((4,)), dma((4,)),
            *moment_refs,
        ],
        compiler_params=pltpu.CompilerParams(collective_id=0, has_side_effects=True),
        name="tripole_cg",
    )(forcing, search_direction, ocean_depth, land_mask, fold_map)
    return pl.pallas_call(
        hand_over,
        out_shape=[jax.ShapeDtypeStruct((rows, width), f32)] * 2,
        in_specs=[block] * 2,
        out_specs=[block] * 2,
        name="hand_over",
    )(*(pltpu.with_memory_space_constraint(out, pltpu.VMEM) for out in outs))


def solution(mesh):
    cells = P("lat", "lon")
    return jax.shard_map(
        functools.partial(per_device, mesh.shape["lat"], mesh.shape["lon"]),
        mesh=mesh,
        in_specs=(cells, cells, cells, cells, P()),
        out_specs=(cells, cells),
        check_vma=False,
    )
```

```python
import functools

import jax
import jax.numpy as jnp
from jax import lax
from jax.experimental import pallas as pl
from jax.experimental.pallas import tpu as pltpu
from jax.sharding import PartitionSpec as P

STEPS = 8
REACH = 256
MESH = pl.DeviceIdType.MESH
PAD = 16
GROUP = 32
CHUNK = 16
LIP = STEPS + 1
MARGIN = 12
BAND = 32
DIRECT_LIMIT = 64

DIRECTIONS = ((1, 0), (-1, 0), (0, 1), (0, -1), (1, 1), (-1, -1), (1, -1), (-1, 1))
SLOT = {offset: index for index, offset in enumerate(DIRECTIONS)}


def halves(offset):
    return 0.5 if 0 in offset else 0.25


def chunks_of(low, high, size):
    return [(at, min(size, high - at)) for at in range(low, high, size)]


def turned(x, shift):
    shift = shift % x.shape[1]
    return x if shift == 0 else pltpu.roll(x, shift, 1)


def bilinear(left, right, gram):
    total = None
    for i in sorted(left):
        inner = None
        for j in sorted(right):
            term = gram(i, j) * right[j]
            inner = term if inner is None else inner + term
        inner = left[i] * inner
        total = inner if total is None else total + inner
    return total


def plus(left, right):
    result = dict(left)
    for key, value in right.items():
        result[key] = result[key] + value if key in result else value
    return result


def scaled(factor, vector):
    return {key: factor * value for key, value in vector.items()}


def apply_shift(vector):
    result = {}
    for (chain, power), value in vector.items():
        parts = [((chain, power), value)]
        if power == 0:
            parts.append(((chain, 1), value))
        else:
            half = 0.5 * value
            parts += [((chain, power + 1), half), ((chain, power - 1), half)]
        result = plus(result, {}) if not parts else result
        for key, part in parts:
            result = plus(result, {key: part})
    return result


def coordinates(moments):
    cache = {}

    def gram(left, right):
        kind = (left[0], right[0]) if left[0] <= right[0] else (right[0], left[0])
        low, high = sorted((left[1], right[1]))
        key = (kind, low, high)
        if key not in cache:
            series = moments[kind]
            cache[key] = 0.5 * (series[high + low] + series[high - low])
        return cache[key]

    solution_coords = {}
    one = jnp.ones_like(moments[("p", "p")][0])
    direction_coords = {("p", 0): one}
    residual_coords = {("r", 0): one}
    norm_now = bilinear(residual_coords, residual_coords, gram)
    for _ in range(STEPS):
        mapped = apply_shift(direction_coords)
        step_length = norm_now / bilinear(direction_coords, mapped, gram)
        solution_coords = plus(solution_coords, scaled(step_length, direction_coords))
        residual_coords = plus(residual_coords, scaled(-step_length, mapped))
        norm_next = bilinear(residual_coords, residual_coords, gram)
        direction_coords = plus(
            residual_coords, scaled(norm_next / norm_now, direction_coords)
        )
        norm_now = norm_next
    return solution_coords, residual_coords


def fold_sublanes(parts):
    row = lax.broadcasted_iota(jnp.int32, parts[0].shape, 0)
    parts = list(parts)
    span = 4
    while span:
        low = (row & span) == 0
        half = len(parts) // 2
        parts = [
            jnp.where(low, first, second)
            + pltpu.roll(jnp.where(low, second, first), span, 0)
            if span == 4
            else jnp.where(low, first, second)
            + jnp.where(low, pltpu.roll(first, 8 - span, 0), pltpu.roll(second, span, 0))
            for first, second in zip(parts[:half], parts[half:])
        ]
        span //= 2
    return parts[0]


def kept(at, count, regions):
    row = lax.broadcasted_iota(jnp.int32, (8, regions[0][2].shape[1]), 0)
    masks = []
    for r in range(at, at + count, 8):
        mask = None
        for low, high, lanes in regions:
            if low >= r + 8 or high <= r:
                continue
            part = lanes
            if low > r or high < r + 8:
                part = lanes & (row >= low - r) & (row < high - r)
            mask = part if mask is None else mask | part
        masks.append(mask)
    return masks


def prepare(rows, depth_root, shifted, weights, basis):
    width = depth_root.shape[2]
    zero = jnp.zeros((8, width), jnp.float32)
    for at in (0, 8 + rows):
        span = pl.ds(at, 8)
        depth_root[0, span, :] = zero
        depth_root[1, span, :] = zero
        for slot in range(2 * STEPS + 1):
            if slot not in (STEPS, 2 * STEPS):
                basis[slot, span, :] = zero

    depth, root = depth_root.at[0], depth_root.at[1]
    for at, count in chunks_of(0, rows + 16, CHUNK):
        span = pl.ds(at, count)
        shifted[0, span, :] = turned(depth[span, :], -1)
        shifted[1, span, :] = turned(depth[span, :], 1)
    shifted_depth = {0: depth, 1: shifted.at[0], -1: shifted.at[1]}
    for at, count in chunks_of(8, 8 + rows, CHUNK):
        here = depth[at : at + count, :]
        sums = {0.5: None, 0.25: None}
        for a, b in DIRECTIONS:
            beside = shifted_depth[b][at + a : at + a + count, :]
            link = jnp.where(beside > 0.0, here + beside, 0.0)
            factor = halves((a, b))
            sums[factor] = link if sums[factor] is None else sums[factor] + link
        diagonal = here * (1.0 / (REACH * REACH)) + (0.5 * sums[0.5] + 0.25 * sums[0.25])
        value = lax.rsqrt(jnp.where(here > 0.0, diagonal, 1.0))
        span = pl.ds(at, count)
        root[span, :] = value
        shifted[2, span, :] = turned(value, -1)
        shifted[3, span, :] = turned(value, 1)
    shifted_root = {0: root, 1: shifted.at[2], -1: shifted.at[3]}
    for at, count in chunks_of(8, 8 + rows, CHUNK):
        for b in (-1, 0, 1):
            goal_depth = shifted_depth[-b][at : at + count, :]
            goal_root = shifted_root[-b][at : at + count, :]
            for a in (-1, 0, 1):
                if (a, b) == (0, 0):
                    continue
                from_depth = depth[at + a : at + a + count, :]
                from_root = root[at + a : at + a + count, :]
                link = jnp.where(
                    jnp.minimum(goal_depth, from_depth) > 0.0, goal_depth + from_depth, 0.0
                )
                weights[SLOT[(a, b)], at : at + count, :] = (
                    goal_root * (-2.0 * halves((a, b)))
                ) * (link * from_root)


def march(rows, weights, basis, keep, add_dot, flush, new):
    def masked(masks, value):
        return [
            None if mask is None else jnp.where(mask, value[8 * i : 8 * i + 8, :], 0.0)
            for i, mask in enumerate(masks)
        ]

    def dot(key, left, right):
        for i, piece in enumerate(left):
            if piece is not None:
                add_dot(key, piece, right[8 * i : 8 * i + 8, :])

    row_chunks = chunks_of(8, 8 + rows, CHUNK)
    for at, count in row_chunks:
        p0 = basis[0, at : at + count, :]
        r0 = basis[STEPS + 1, at : at + count, :]
        masks = keep(at - 8, count)
        p0_kept, r0_kept = masked(masks, p0), masked(masks, r0)
        dot(("p", "p", 0), p0_kept, p0)
        dot(("r", "r", 0), r0_kept, r0)
        dot(("p", "r", 0), p0_kept, r0)

    for power in range(1, STEPS + 1):
        chains = [("p", 0)] + ([("r", STEPS + 1)] if power < STEPS else [])
        for at, count in row_chunks:
            fresh = {}
            held = {}
            factors = {ab: weights[SLOT[ab], at : at + count, :] for ab in DIRECTIONS}
            for name, origin in chains:
                slot = origin + power
                taken = {a: basis[slot - 1, at + a : at + a + count, :] for a in (-1, 0, 1)}
                held[name] = taken[0]
                columns = {}
                for b in (-1, 0, 1):
                    total = None
                    for a in (-1, 0, 1):
                        if (a, b) == (0, 0):
                            continue
                        term = factors[(a, b)] * taken[a]
                        total = term if total is None else total + term
                    columns[b] = total
                value = columns[0] + turned(columns[1], -1) + turned(columns[-1], 1)
                if power == 1:
                    value = 0.5 * value
                else:
                    value = value - basis[slot - 2, at : at + count, :]
                basis[slot, at : at + count, :] = value
                fresh[name] = value
            masks = keep(at - 8, count)
            fresh_kept = {name: masked(masks, fresh[name]) for name, _ in chains}
            for name, _ in chains:
                dot((name, name, 2 * power), fresh_kept[name], fresh[name])
                dot((name, name, 2 * power - 1), fresh_kept[name], held[name])
            if power < STEPS:
                dot(("p", "r", 2 * power), fresh_kept["p"], fresh["r"])
                dot(("p", "r", 2 * power - 1), fresh_kept["p"], held["r"])
            else:
                dot(
                    ("p", "r", 2 * power - 1),
                    fresh_kept["p"],
                    basis[STEPS + power, at : at + count, :],
                )
        flush(new)


def kernel(
    n_lat, n_lon, forcing_hbm, search_hbm, depth_hbm, mask_hbm, fold_hbm,
    out_height, out_residual, loaded, mask_in, fold_map,
    centre, side, wide, wide_shifted, wide_weights, wide_basis, seam, seam_shifted,
    seam_weights, seam_basis, patch, row_north, row_south, fold_rows, packed, got_rows, got_sides,
    fold_all, dots, moment_rows, load_sem, near_send, near_recv, *moment_refs,
):
    rows, width = forcing_hbm.shape
    lat, lon = lax.axis_index("lat"), lax.axis_index("lon")
    top = n_lat - 1
    north, south = lax.rem(lat + 1, n_lat), lax.rem(lat + n_lat - 1, n_lat)
    east, west = lax.rem(lon + 1, n_lon), lax.rem(lon + n_lon - 1, n_lon)
    has_north, has_south = lat < top, lat > 0
    group_rows = rows * GROUP // width
    n_groups = width // GROUP

    barrier = pltpu.get_barrier_semaphore()

    def greet(place):
        pl.semaphore_signal(barrier, inc=1, device_id=place, device_id_type=MESH)

    for source, target, index in (
        (mask_hbm, mask_in, 0), (depth_hbm, loaded.at[0], 1), (search_hbm, loaded.at[1], 1),
        (forcing_hbm, loaded.at[2], 1), (fold_hbm, fold_map, 2),
    ):
        pltpu.make_async_copy(source, target, load_sem.at[index]).start()
    depth_in, search, forcing = loaded.at[0], loaded.at[1], loaded.at[2]
    direct = n_lat * n_lon <= DIRECT_LIMIT
    everyone = [(a, b) for a in range(n_lat) for b in range(n_lon) if a or b]
    everyone.sort(key=lambda d: (d[1] or n_lon, d[0] or n_lat))
    if direct:
        for a, b in everyone:
            greet((lax.rem(lat + a, n_lat), lax.rem(lon + b, n_lon)))
        greeted = len(everyone)
    else:
        for d in range(1, n_lat):
            greet((lax.rem(lat + d, n_lat), lon))
        for d in range(1, n_lon):
            greet((lat, lax.rem(lon + d, n_lon)))
        for place in ((north, east), (north, west), (south, east), (south, west)):
            greet(place)
        greeted = n_lat - 1 + n_lon - 1 + 4

    pltpu.make_async_copy(mask_hbm, mask_in, load_sem.at[0]).wait()
    pltpu.make_async_copy(loaded, loaded, load_sem.at[1]).wait()
    pltpu.make_async_copy(fold_hbm, fold_map, load_sem.at[2]).wait()
    lane_group = lax.broadcasted_iota(jnp.int32, (group_rows, width), 1)
    west_edge = east_edge = None
    for g in range(n_groups):
        here = pl.ds(g * group_rows, group_rows)
        there = pl.ds(PAD + g * group_rows, group_rows)
        flag = mask_in[here, :].astype(jnp.float32)
        deep = depth_in[here, :] * flag
        moving = search[here, :] * flag
        left = forcing[here, :] * flag
        for index, value in enumerate((deep, moving, left)):
            centre[index, there, :] = value
        inner = pl.ds(8 + g * group_rows, group_rows)
        wide[0, inner, :] = deep
        wide_basis[0, inner, :] = moving
        wide_basis[STEPS + 1, inner, :] = left
        inside = lane_group - g * GROUP
        to_west = jnp.where(
            inside < 9,
            turned(deep, g * GROUP),
            jnp.where(inside < 17, turned(moving, g * GROUP + 9), turned(left, g * GROUP + 17)),
        )
        to_east = jnp.where(
            inside < 9,
            turned(deep, g * GROUP + 9),
            jnp.where(inside < 17, turned(moving, g * GROUP + 17), turned(left, g * GROUP + 25)),
        )
        west_edge = to_west if g == 0 else jnp.where(inside >= 0, to_west, west_edge)
        east_edge = to_east if g == 0 else jnp.where(inside >= 0, to_east, east_edge)
    packed[0] = west_edge
    packed[1] = east_edge
    first, last = PAD, PAD + rows
    spans = ((0, 0, 16), (1, 16, 8), (2, 24, 8))
    for index, at, count in spans:
        row_south[at : at + count, :] = centre[index, first : first + count, :]
        row_north[at : at + count, :] = centre[index, last - count : last, :]

    @pl.when(lat == top)
    def _():
        for index, at, count in spans:
            for r in range(count):
                fold_rows[at + r : at + r + 1, :] = centre[index, last - 1 - r : last - r, :]
        fold_all[lon] = fold_rows[...]

    pl.semaphore_wait(barrier, greeted)

    def near(index, source, target, place):
        return pltpu.make_async_remote_copy(
            src_ref=source, dst_ref=target, send_sem=near_send.at[index],
            recv_sem=near_recv.at[index], device_id=place, device_id_type=MESH,
        )

    tail = pl.ds(group_rows - 16, 16)
    head = pl.ds(0, 16)
    got_south, got_north = got_rows.at[0, 0:32], got_rows.at[1, 0:32]
    got_west, got_east = got_sides.at[0], got_sides.at[1]
    corners = [got_rows.at[index // 2, pl.ds(32 + 16 * (index % 2), 16)] for index in range(4)]
    northward = (
        near(0, row_north, got_south, (north, lon)),
        near(0, packed.at[1, tail], corners[0], (north, east)),
        near(0, packed.at[0, tail], corners[1], (north, west)),
    )
    southward = (
        near(1, row_south, got_north, (south, lon)),
        near(1, packed.at[1, head], corners[2], (south, east)),
        near(1, packed.at[0, head], corners[3], (south, west)),
    )
    to_east = near(2, packed.at[1], got_west, (lat, east))
    to_west = near(2, packed.at[0], got_east, (lat, west))

    def arrival(index, block):
        return near(index, block, block, (lat, lon))

    from_south, from_north = arrival(0, got_rows.at[0]), arrival(1, got_rows.at[1])
    from_sides = arrival(2, got_sides)
    from_fold = arrival(3, fold_all.at[0 : n_lon - 1])

    def spread(source, slots, send_sem, recv_sem, along_lat):
        size = n_lat if along_lat else n_lon
        me = lat if along_lat else lon
        copies = []
        for d in range(1, size):
            peer = lax.rem(me + d, size)
            copies.append(
                pltpu.make_async_remote_copy(
                    src_ref=source, dst_ref=slots.at[me], send_sem=send_sem,
                    recv_sem=recv_sem,
                    device_id=(peer, lon) if along_lat else (lat, peer),
                    device_id_type=MESH,
                )
            )
        return copies

    across = spread(fold_rows, fold_all, near_send.at[3], near_recv.at[3], False)

    @pl.when(lat == top)
    def _():
        for copy in across:
            copy.start()

    to_east.start()
    to_west.start()

    @pl.when(has_north)
    def _():
        for copy in northward:
            copy.start()

    @pl.when(has_south)
    def _():
        for copy in southward:
            copy.start()

    dot_sums = {}

    def add_dot(key, left, right):
        product = left * right
        for r in range(0, product.shape[0], 8):
            piece = product[r : r + 8, :]
            dot_sums[key] = piece if key not in dot_sums else dot_sums[key] + piece

    def flush(new):
        for key in list(dot_sums):
            total = dot_sums.pop(key)
            spot = order_of()[key]
            dots[spot] = total if new else dots[spot] + total

    lane8 = lax.broadcasted_iota(jnp.int32, (8, width), 1)
    nothing = jnp.zeros((8, width), jnp.float32)

    prepare(rows, wide, wide_shifted, wide_weights, wide_basis)
    middle = (lane8 >= LIP) & (lane8 < width - LIP)

    def keep_wide(at, count):
        return kept(at, count, [(LIP, rows - LIP, middle)])

    march(rows, wide_weights, wide_basis, keep_wide, add_dot, flush, True)

    def unpack(got_e, got_w, start, g, count):
        lane = lax.broadcasted_iota(jnp.int32, (count, width), 1)
        base = -g * GROUP
        for index, offset, cells in ((0, 0, 9), (1, 9, 8), (2, 17, 8)):
            from_east = turned(got_e, base - offset)
            from_west = turned(got_w, base - offset - cells)
            side[index, start : start + count, :] = jnp.where(
                lane < cells,
                from_east,
                jnp.where(lane >= width - cells, from_west, jnp.zeros_like(got_e)),
            )

    for index in (1, 2):
        for at in (0, last + 8):
            centre[index, at : at + 8, :] = nothing
            side[index, at : at + 8, :] = nothing

    from_sides.wait_recv()
    for g in range(n_groups):
        unpack(got_east[...], got_west[...], PAD + g * group_rows, g, group_rows)

    @pl.when(has_south)
    def _():
        from_south.wait_recv()
        centre[0, 0:16, :] = got_south[0:16, :]
        centre[1, 8:16, :] = got_south[16:24, :]
        centre[2, 8:16, :] = got_south[24:32, :]
        unpack(corners[1][...], corners[0][...], 0, n_groups - 1, 16)

    @pl.when(lat == 0)
    def _():
        for target in (centre, side):
            for index, at in ((0, 0), (0, 8), (1, 8), (2, 8)):
                target[index, at : at + 8, :] = nothing

    @pl.when(has_north)
    def _():
        from_north.wait_recv()
        centre[0, last : last + 16, :] = got_north[0:16, :]
        centre[1, last : last + 8, :] = got_north[16:24, :]
        centre[2, last : last + 8, :] = got_north[24:32, :]
        unpack(corners[3][...], corners[2][...], last, 0, 16)

    @pl.when(lat == top)
    def _():
        from_fold.wait_recv()
        total = n_lon * width
        pivot = lax.rem(fold_map[0] - lon * width + total, total)
        block, offset = pivot // width, lax.rem(pivot, width)
        lane = lax.broadcasted_iota(jnp.int32, (32, width), 1)
        index = lax.rem(offset - lane + width, width)

        def mirrored(which):
            rows_of = fold_all[lax.rem(block + which + n_lon, n_lon)]
            return jnp.take_along_axis(rows_of, index, axis=1, mode="promise_in_bounds")

        ahead, same, behind, beyond = (mirrored(which) for which in (1, 0, -1, -2))
        close = lane <= offset
        value = jnp.where(close, same, behind)
        halo = jnp.where(
            lane < width // 2, jnp.where(close, behind, beyond), jnp.where(close, ahead, same)
        )
        for source, target in ((value, centre), (halo, side)):
            target[0, last : last + 16, :] = source[0:16, :]
            target[1, last : last + 8, :] = source[16:24, :]
            target[2, last : last + 8, :] = source[24:32, :]

    n_parts = width // GROUP // 2
    part_rows = rows // n_parts
    strip_rows = part_rows + 2 * MARGIN
    seam_rows = strip_rows + 2 * BAND
    north_at, south_at = strip_rows, strip_rows + BAND
    own = GROUP - LIP
    targets = (seam.at[0], seam_basis.at[0], seam_basis.at[STEPS + 1])
    for index, target in enumerate(targets):
        for at in range(0, strip_rows, 8):
            value = None
            for q in range(n_parts):
                span = slice(PAD + q * part_rows - MARGIN + at, PAD + q * part_rows - MARGIN + at + 8)
                inside, outside = centre[index, span, :], side[index, span, :]
                east_slot = turned(
                    jnp.where(lane8 >= width - own, inside, outside), q * GROUP - (width - own)
                )
                west_slot = turned(
                    jnp.where(lane8 < own, inside, outside), (n_parts + q) * GROUP + LIP
                )
                if q == 0:
                    value = jnp.where(lane8 < n_parts * GROUP, east_slot, west_slot)
                else:
                    mixed = jnp.where(lane8 < n_parts * GROUP, east_slot, west_slot)
                    value = jnp.where((lane8 // GROUP) % n_parts >= q, mixed, value)
            target[8 + at : 16 + at, :] = value
        for at in range(0, BAND, 8):
            low = last + LIP - BAND + at
            target[8 + north_at + at : 16 + north_at + at, :] = centre[index, low : low + 8, :]
            low = first - LIP + at
            target[8 + south_at + at : 16 + south_at + at, :] = centre[index, low : low + 8, :]

    prepare(seam_rows, seam, seam_shifted, seam_weights, seam_basis)
    slot_lane = lax.rem(lane8, GROUP)
    east_half = lane8 < n_parts * GROUP
    strip_lanes = jnp.where(east_half, slot_lane - (own - LIP), slot_lane - LIP)
    strip_lanes = (strip_lanes >= 0) & (strip_lanes < LIP)

    def keep_seam(at, count):
        return kept(
            at,
            count,
            [
                (MARGIN, MARGIN + part_rows, strip_lanes),
                (north_at + BAND - 2 * LIP, north_at + BAND - LIP, middle),
                (south_at + LIP, south_at + 2 * LIP, middle),
            ],
        )

    march(seam_rows, seam_weights, seam_basis, keep_seam, add_dot, flush, False)

    number = len(order_of())
    pending = []
    lane = lax.broadcasted_iota(jnp.int32, (8, width), 1)
    home = lane - lax.broadcasted_iota(jnp.int32, (8, width), 0)
    message = jnp.zeros((8, width), jnp.float32)
    for g in range(number // 8):
        grouped = fold_sublanes([dots[8 * g + s] for s in range(8)])
        message = jnp.where(home == 8 * g, jnp.sum(grouped, axis=1, keepdims=True), message)
    message = jnp.sum(message, axis=0, keepdims=True)
    if direct:
        slots, send_sem, recv_sem = moment_refs
        me = lat * n_lon + lon
        slots[me] = message
        copies = [
            pltpu.make_async_remote_copy(
                src_ref=slots.at[me], dst_ref=slots.at[me], send_sem=send_sem,
                recv_sem=recv_sem,
                device_id=(lax.rem(lat + a, n_lat), lax.rem(lon + b, n_lon)),
                device_id_type=MESH,
            )
            for a, b in everyone
        ]
        rounds = ((slots, n_lat * n_lon, copies, send_sem, recv_sem),)
    else:
        slots_lat, slots_lon, lat_send, lat_recv, lon_send, lon_recv = moment_refs
        rounds = (
            (slots_lat, n_lat, None, lat_send, lat_recv, lat, True),
            (slots_lon, n_lon, None, lon_send, lon_recv, lon, False),
        )
    for slots, size, copies, send_sem, recv_sem, *rest in rounds:
        if copies is None:
            me, along_lat = rest
            slots[me] = message
            copies = spread(slots.at[me], slots, send_sem, recv_sem, along_lat)
        for copy in copies:
            copy.start()
        others = slots.at[0 : size - 1]
        whole = pltpu.make_async_remote_copy(
            src_ref=others, dst_ref=others, send_sem=send_sem, recv_sem=recv_sem,
            device_id=(lat, lon), device_id_type=MESH,
        )
        whole.wait_recv()
        terms = [slots[index] for index in range(size)]
        while len(terms) > 1:
            odd = terms[len(terms) // 2 * 2 :]
            terms = [x + y for x, y in zip(terms[0::2], terms[1::2])] + odd
        message = terms[0]
        pending.append(whole)
    message = jnp.broadcast_to(message, (8, width))
    for g in range(number // 8):
        picked = jnp.sum(jnp.where(home == 8 * g, message, 0.0), axis=1, keepdims=True)
        moment_rows[8 * g : 8 * g + 8, :] = jnp.broadcast_to(picked, (8, width))
    moments = {}
    for kind in (("p", "p"), ("p", "r"), ("r", "r")):
        series = []
        for index in range(17 if kind == ("p", "p") else 16 if kind == ("p", "r") else 15):
            spot = order_of()[kind + (index,)]
            value = jnp.broadcast_to(moment_rows[spot : spot + 1, :], (8, width))
            series.append(value if index < 2 else 2.0 * value - series[index % 2])
        moments[kind] = series
    height_coords, residual_coords = coordinates(moments)
    wanted = (height_coords, residual_coords)

    def combined(fields, at):
        totals = [None, None]
        for chain, power in sorted(height_coords | residual_coords):
            slot = power + (0 if chain == "p" else STEPS + 1)
            field = fields[slot, 8 + at : 16 + at, :]
            for which, coords in enumerate(wanted):
                if (chain, power) in coords:
                    term = coords[(chain, power)] * field
                    totals[which] = term if totals[which] is None else totals[which] + term
        return totals

    for at in range(0, seam_rows, 8):
        for which, total in enumerate(combined(seam_basis, at)):
            patch[which, at : at + 8, :] = total
    row8 = lax.broadcasted_iota(jnp.int32, (8, width), 0)
    for at in range(0, rows, 8):
        q = at // part_rows
        for which, total in enumerate(combined(wide_basis, at)):
            for low, high, source in (
                (0, LIP, south_at + LIP),
                (rows - LIP, rows, north_at + BAND - LIP - rows),
            ):
                if low < at + 8 and high > at:
                    edge = patch[which, source + at : source + at + 8, :]
                    if low <= at and high >= at + 8:
                        total = edge
                    else:
                        total = jnp.where((row8 >= low - at) & (row8 < high - at), edge, total)
            spot = at - q * part_rows + MARGIN
            strip = patch[which, spot : spot + 8, :]
            total = jnp.where(lane8 < LIP, turned(strip, -(n_parts + q) * GROUP - LIP), total)
            total = jnp.where(
                lane8 >= width - LIP, turned(strip, width - own - q * GROUP), total
            )
            (out_height, out_residual)[which][at : at + 8, :] = total

    for copy in pending:
        copy.wait_send()
    from_sides.wait_send()

    @pl.when(has_north)
    def _():
        from_south.wait_send()

    @pl.when(has_south)
    def _():
        from_north.wait_send()

    @pl.when(lat == top)
    def _():
        from_fold.wait_send()


@functools.cache
def order_of():
    keys = [("p", "p", k) for k in range(2 * STEPS + 1)]
    keys += [("p", "r", k) for k in range(2 * STEPS)]
    keys += [("r", "r", k) for k in range(2 * STEPS - 1)]
    return {key: index for index, key in enumerate(keys)}


def hand_over(height, residual, out_height, out_residual):
    out_height[...] = height[...]
    out_residual[...] = residual[...]


def per_device(n_lat, n_lon, forcing, search_direction, ocean_depth, land_mask, fold_map):
    rows, width = forcing.shape
    tall = rows + 2 * PAD
    f32 = jnp.float32
    n_parts = width // GROUP // 2
    seam_rows = rows // n_parts + 2 * MARGIN + 2 * BAND

    def tile(count):
        return [
            pltpu.VMEM((planes, count + 16, width), f32)
            for planes in (2, 4, 8, 2 * STEPS + 1)
        ]

    edge = pltpu.VMEM((32, width), f32)
    group_rows = rows * GROUP // width
    dma = pltpu.SemaphoreType.DMA
    if n_lat * n_lon <= DIRECT_LIMIT:
        moment_refs = [pltpu.VMEM((n_lat * n_lon, 1, width), f32), dma, dma]
    else:
        moment_refs = [pltpu.VMEM((size, 1, width), f32) for size in (n_lat, n_lon)] + [dma] * 4
    block = pl.BlockSpec(memory_space=pltpu.VMEM)
    outs = pl.pallas_call(
        functools.partial(kernel, n_lat, n_lon),
        out_shape=[pltpu.VMEM((rows, width), f32)] * 2,
        in_specs=[pl.BlockSpec(memory_space=pl.ANY)] * 5,
        out_specs=[block] * 2,
        scratch_shapes=[
            pltpu.VMEM((3, rows, width), f32), pltpu.VMEM((rows, width), jnp.int32),
            pltpu.SMEM(fold_map.shape, jnp.int32),
            pltpu.VMEM((3, tall, width), f32), pltpu.VMEM((3, tall, width), f32),
            *tile(rows),
            *tile(seam_rows),
            pltpu.VMEM((2, seam_rows, width), f32),
            edge, edge, edge,
            pltpu.VMEM((2, group_rows, width), f32),
            pltpu.VMEM((2, 64, width), f32),
            pltpu.VMEM((2, group_rows, width), f32),
            pltpu.VMEM((n_lon, 32, width), f32),
            pltpu.VMEM((6 * STEPS, 8, width), f32),
            pltpu.VMEM((6 * STEPS, width), f32),
            dma((3,)), dma((4,)), dma((4,)),
            *moment_refs,
        ],
        compiler_params=pltpu.CompilerParams(collective_id=0, has_side_effects=True),
        name="tripole_cg",
    )(forcing, search_direction, ocean_depth, land_mask, fold_map)
    return pl.pallas_call(
        hand_over,
        out_shape=[jax.ShapeDtypeStruct((rows, width), f32)] * 2,
        in_specs=[block] * 2,
        out_specs=[block] * 2,
        name="hand_over",
    )(*(pltpu.with_memory_space_constraint(out, pltpu.VMEM) for out in outs))


def solution(mesh):
    cells = P("lat", "lon")
    return jax.shard_map(
        functools.partial(per_device, mesh.shape["lat"], mesh.shape["lon"]),
        mesh=mesh,
        in_specs=(cells, cells, cells, cells, P()),
        out_specs=(cells, cells),
        check_vma=False,
    )
```

```python
import functools

import jax
import jax.numpy as jnp
from jax import lax
from jax.experimental import pallas as pl
from jax.experimental.pallas import tpu as pltpu
from jax.sharding import PartitionSpec as P

STEPS = 8
REACH = 256
MESH = pl.DeviceIdType.MESH
PAD = 16
GROUP = 32
CHUNK = 16
LIP = STEPS + 1
MARGIN = 12
BAND = 32
DIRECT_LIMIT = 64

DIRECTIONS = ((1, 0), (-1, 0), (0, 1), (0, -1), (1, 1), (-1, -1), (1, -1), (-1, 1))
SLOT = {offset: index for index, offset in enumerate(DIRECTIONS)}


def halves(offset):
    return 0.5 if 0 in offset else 0.25


def chunks_of(low, high, size):
    return [(at, min(size, high - at)) for at in range(low, high, size)]


def turned(x, shift):
    shift = shift % x.shape[1]
    return x if shift == 0 else pltpu.roll(x, shift, 1)


def bilinear(left, right, gram):
    total = None
    for i in sorted(left):
        inner = None
        for j in sorted(right):
            term = gram(i, j) * right[j]
            inner = term if inner is None else inner + term
        inner = left[i] * inner
        total = inner if total is None else total + inner
    return total


def plus(left, right):
    result = dict(left)
    for key, value in right.items():
        result[key] = result[key] + value if key in result else value
    return result


def scaled(factor, vector):
    return {key: factor * value for key, value in vector.items()}


def apply_shift(vector):
    result = {}
    for (chain, power), value in vector.items():
        parts = [((chain, power), value)]
        if power == 0:
            parts.append(((chain, 1), value))
        else:
            half = 0.5 * value
            parts += [((chain, power + 1), half), ((chain, power - 1), half)]
        result = plus(result, {}) if not parts else result
        for key, part in parts:
            result = plus(result, {key: part})
    return result


def coordinates(moments):
    cache = {}

    def gram(left, right):
        kind = (left[0], right[0]) if left[0] <= right[0] else (right[0], left[0])
        low, high = sorted((left[1], right[1]))
        key = (kind, low, high)
        if key not in cache:
            series = moments[kind]
            cache[key] = 0.5 * (series[high + low] + series[high - low])
        return cache[key]

    solution_coords = {}
    one = jnp.ones_like(moments[("p", "p")][0])
    direction_coords = {("p", 0): one}
    residual_coords = {("r", 0): one}
    norm_now = bilinear(residual_coords, residual_coords, gram)
    for _ in range(STEPS):
        mapped = apply_shift(direction_coords)
        step_length = norm_now / bilinear(direction_coords, mapped, gram)
        solution_coords = plus(solution_coords, scaled(step_length, direction_coords))
        residual_coords = plus(residual_coords, scaled(-step_length, mapped))
        norm_next = bilinear(residual_coords, residual_coords, gram)
        direction_coords = plus(
            residual_coords, scaled(norm_next / norm_now, direction_coords)
        )
        norm_now = norm_next
    return solution_coords, residual_coords


def fold_sublanes(parts):
    row = lax.broadcasted_iota(jnp.int32, parts[0].shape, 0)
    parts = list(parts)
    span = 4
    while span:
        low = (row & span) == 0
        half = len(parts) // 2
        parts = [
            jnp.where(low, first, second)
            + pltpu.roll(jnp.where(low, second, first), span, 0)
            if span == 4
            else jnp.where(low, first, second)
            + jnp.where(low, pltpu.roll(first, 8 - span, 0), pltpu.roll(second, span, 0))
            for first, second in zip(parts[:half], parts[half:])
        ]
        span //= 2
    return parts[0]


def kept(at, count, regions):
    row = lax.broadcasted_iota(jnp.int32, (8, regions[0][2].shape[1]), 0)
    masks = []
    for r in range(at, at + count, 8):
        mask = None
        for low, high, lanes in regions:
            if low >= r + 8 or high <= r:
                continue
            part = lanes
            if low > r or high < r + 8:
                part = lanes & (row >= low - r) & (row < high - r)
            mask = part if mask is None else mask | part
        masks.append(mask)
    return masks


def prepare(rows, depth_root, shifted, weights, basis):
    width = depth_root.shape[2]
    zero = jnp.zeros((8, width), jnp.float32)
    for at in (0, 8 + rows):
        span = pl.ds(at, 8)
        depth_root[0, span, :] = zero
        depth_root[1, span, :] = zero
        for slot in range(2 * STEPS + 1):
            if slot not in (STEPS, 2 * STEPS):
                basis[slot, span, :] = zero

    depth, root = depth_root.at[0], depth_root.at[1]
    for at, count in chunks_of(0, rows + 16, CHUNK):
        span = pl.ds(at, count)
        shifted[0, span, :] = turned(depth[span, :], -1)
        shifted[1, span, :] = turned(depth[span, :], 1)
    shifted_depth = {0: depth, 1: shifted.at[0], -1: shifted.at[1]}
    for at, count in chunks_of(8, 8 + rows, CHUNK):
        here = depth[at : at + count, :]
        sums = {0.5: None, 0.25: None}
        for a, b in DIRECTIONS:
            beside = shifted_depth[b][at + a : at + a + count, :]
            link = jnp.where(beside > 0.0, here + beside, 0.0)
            factor = halves((a, b))
            sums[factor] = link if sums[factor] is None else sums[factor] + link
        diagonal = here * (1.0 / (REACH * REACH)) + (0.5 * sums[0.5] + 0.25 * sums[0.25])
        value = lax.rsqrt(jnp.where(here > 0.0, diagonal, 1.0))
        span = pl.ds(at, count)
        root[span, :] = value
        shifted[2, span, :] = turned(value, -1)
        shifted[3, span, :] = turned(value, 1)
    shifted_root = {0: root, 1: shifted.at[2], -1: shifted.at[3]}
    for at, count in chunks_of(8, 8 + rows, CHUNK):
        for b in (-1, 0, 1):
            goal_depth = shifted_depth[-b][at : at + count, :]
            goal_root = shifted_root[-b][at : at + count, :]
            for a in (-1, 0, 1):
                if (a, b) == (0, 0):
                    continue
                from_depth = depth[at + a : at + a + count, :]
                from_root = root[at + a : at + a + count, :]
                link = jnp.where(
                    jnp.minimum(goal_depth, from_depth) > 0.0, goal_depth + from_depth, 0.0
                )
                weights[SLOT[(a, b)], at : at + count, :] = (
                    goal_root * (-2.0 * halves((a, b)))
                ) * (link * from_root)


def march(rows, weights, basis, keep, add_dot, flush, new):
    def masked(masks, value):
        return [
            None if mask is None else jnp.where(mask, value[8 * i : 8 * i + 8, :], 0.0)
            for i, mask in enumerate(masks)
        ]

    def dot(key, left, right):
        for i, piece in enumerate(left):
            if piece is not None:
                add_dot(key, piece, right[8 * i : 8 * i + 8, :])

    row_chunks = chunks_of(8, 8 + rows, CHUNK)
    for at, count in row_chunks if keep else []:
        p0 = basis[0, at : at + count, :]
        r0 = basis[STEPS + 1, at : at + count, :]
        masks = keep(at - 8, count)
        p0_kept, r0_kept = masked(masks, p0), masked(masks, r0)
        dot(("p", "p", 0), p0_kept, p0)
        dot(("r", "r", 0), r0_kept, r0)
        dot(("p", "r", 0), p0_kept, r0)

    for power in range(1, STEPS + 1):
        chains = [("p", 0)] + ([("r", STEPS + 1)] if power < STEPS else [])
        for at, count in row_chunks:
            fresh = {}
            held = {}
            factors = {ab: weights[SLOT[ab], at : at + count, :] for ab in DIRECTIONS}
            for name, origin in chains:
                slot = origin + power
                taken = {a: basis[slot - 1, at + a : at + a + count, :] for a in (-1, 0, 1)}
                held[name] = taken[0]
                columns = {}
                for b in (-1, 0, 1):
                    total = None
                    for a in (-1, 0, 1):
                        if (a, b) == (0, 0):
                            continue
                        term = factors[(a, b)] * taken[a]
                        total = term if total is None else total + term
                    columns[b] = total
                value = columns[0] + turned(columns[1], -1) + turned(columns[-1], 1)
                if power == 1:
                    value = 0.5 * value
                else:
                    value = value - basis[slot - 2, at : at + count, :]
                basis[slot, at : at + count, :] = value
                fresh[name] = value
            if not keep:
                continue
            masks = keep(at - 8, count)
            fresh_kept = {name: masked(masks, fresh[name]) for name, _ in chains}
            for name, _ in chains:
                dot((name, name, 2 * power), fresh_kept[name], fresh[name])
                dot((name, name, 2 * power - 1), fresh_kept[name], held[name])
            if power < STEPS:
                dot(("p", "r", 2 * power), fresh_kept["p"], fresh["r"])
                dot(("p", "r", 2 * power - 1), fresh_kept["p"], held["r"])
            else:
                dot(
                    ("p", "r", 2 * power - 1),
                    fresh_kept["p"],
                    basis[STEPS + power, at : at + count, :],
                )
        if keep:
            flush(new)


def kernel(
    n_lat, n_lon, forcing_hbm, search_hbm, depth_hbm, mask_hbm, fold_hbm,
    out_height, out_residual, loaded, mask_in, fold_map,
    centre, side, wide, wide_shifted, wide_weights, wide_basis, seam, seam_shifted,
    seam_weights, seam_basis, far, far_shifted, far_weights, far_basis, patch, row_north, row_south,
    fold_rows, packed, got_rows, got_sides, fold_all, deep_packed, got_deep, deep_rows, got_far,
    far_centre, far_side, dots, moment_rows, load_sem, near_send, near_recv, *moment_refs,
):
    rows, width = forcing_hbm.shape
    lat, lon = lax.axis_index("lat"), lax.axis_index("lon")
    top = n_lat - 1
    north, south = lax.rem(lat + 1, n_lat), lax.rem(lat + n_lat - 1, n_lat)
    east, west = lax.rem(lon + 1, n_lon), lax.rem(lon + n_lon - 1, n_lon)
    has_north, has_south = lat < top, lat > 0
    group_rows = rows * GROUP // width
    n_groups = width // GROUP

    barrier = pltpu.get_barrier_semaphore()

    def greet(place):
        pl.semaphore_signal(barrier, inc=1, device_id=place, device_id_type=MESH)

    for source, target, index in (
        (mask_hbm, mask_in, 0), (depth_hbm, loaded.at[0], 1), (search_hbm, loaded.at[1], 1),
        (forcing_hbm, loaded.at[2], 1), (fold_hbm, fold_map, 2),
    ):
        pltpu.make_async_copy(source, target, load_sem.at[index]).start()
    depth_in, search, forcing = loaded.at[0], loaded.at[1], loaded.at[2]
    direct = n_lat * n_lon <= DIRECT_LIMIT
    everyone = [(a, b) for a in range(n_lat) for b in range(n_lon) if a or b]
    everyone.sort(key=lambda d: (d[1] or n_lon, d[0] or n_lat))
    if direct:
        for a, b in everyone:
            greet((lax.rem(lat + a, n_lat), lax.rem(lon + b, n_lon)))
        greeted = len(everyone)
    else:
        for d in range(1, n_lat):
            greet((lax.rem(lat + d, n_lat), lon))
        for d in range(1, n_lon):
            greet((lat, lax.rem(lon + d, n_lon)))
        for place in ((north, east), (north, west), (south, east), (south, west)):
            greet(place)
        greeted = n_lat - 1 + n_lon - 1 + 4

    pltpu.make_async_copy(mask_hbm, mask_in, load_sem.at[0]).wait()
    pltpu.make_async_copy(loaded, loaded, load_sem.at[1]).wait()
    pltpu.make_async_copy(fold_hbm, fold_map, load_sem.at[2]).wait()
    lane_group = lax.broadcasted_iota(jnp.int32, (group_rows, width), 1)
    west_edge = east_edge = None
    for g in range(n_groups):
        here = pl.ds(g * group_rows, group_rows)
        there = pl.ds(PAD + g * group_rows, group_rows)
        flag = mask_in[here, :].astype(jnp.float32)
        deep = depth_in[here, :] * flag
        moving = search[here, :] * flag
        left = forcing[here, :] * flag
        for index, value in enumerate((deep, moving, left)):
            centre[index, there, :] = value
        inner = pl.ds(8 + g * group_rows, group_rows)
        wide[0, inner, :] = deep
        wide_basis[0, inner, :] = moving
        wide_basis[STEPS + 1, inner, :] = left
        inside = lane_group - g * GROUP
        to_west = jnp.where(
            inside < 9,
            turned(deep, g * GROUP),
            jnp.where(inside < 17, turned(moving, g * GROUP + 9), turned(left, g * GROUP + 17)),
        )
        to_east = jnp.where(
            inside < 9,
            turned(deep, g * GROUP + 9),
            jnp.where(inside < 17, turned(moving, g * GROUP + 17), turned(left, g * GROUP + 25)),
        )
        west_edge = to_west if g == 0 else jnp.where(inside >= 0, to_west, west_edge)
        east_edge = to_east if g == 0 else jnp.where(inside >= 0, to_east, east_edge)
    packed[0] = west_edge
    packed[1] = east_edge
    first, last = PAD, PAD + rows
    spans = ((0, 0, LIP), (1, LIP, STEPS), (2, LIP + STEPS, STEPS))
    depth_of = LIP + 2 * STEPS
    for index, at, count in spans:
        row_south[at : at + count, :] = centre[index, first : first + count, :]
        row_north[at : at + count, :] = centre[index, last - count : last, :]

    @pl.when(lat == top)
    def _():
        for index, at, count in spans:
            for r in range(count):
                fold_rows[at + r : at + r + 1, :] = centre[index, last - 1 - r : last - r, :]
        fold_all[lon, 0:depth_of, :] = fold_rows[0:depth_of, :]

    pl.semaphore_wait(barrier, greeted)

    half = n_lon // 2
    at_seam, past_seam = lon == n_lon - 1, lon == 0
    on_top = lat == top
    fold_late, fold_early = on_top & (lon >= half), on_top & (lon < half)

    def near(gone, arrived, source, target, place):
        return pltpu.make_async_remote_copy(
            src_ref=source, dst_ref=target, send_sem=near_send.at[gone],
            recv_sem=near_recv.at[arrived], device_id=place, device_id_type=MESH,
        )

    def arrival(index, block):
        return near(0, index, block, block, (lat, lon))

    def departure(index, block):
        return near(index, 0, block, block, (lat, lon))

    tail, head = pl.ds(group_rows - LIP, LIP), pl.ds(0, LIP)
    tall_tail = pl.ds(group_rows - 2 * LIP, 2 * LIP)
    full = pl.ds(0, depth_of)
    near_rows = pl.ds(0, depth_of + LIP)
    got_south, got_north = got_rows.at[0, full], got_rows.at[1, full]
    got_west, got_east = got_sides.at[0], got_sides.at[1]
    corners = [got_rows.at[index // 2, pl.ds(depth_of + LIP * (index % 2), LIP)] for index in range(4)]
    deep_strip = got_deep.at[0:group_rows]
    deep_south = got_deep.at[group_rows : group_rows + LIP]
    deep_north = got_deep.at[group_rows + LIP : group_rows + 2 * LIP]
    far_rows = got_far.at[0 : 3 * LIP]
    far_edges = [got_far.at[at : at + 2 * LIP] for at in (3 * LIP, 5 * LIP)]
    northward = (
        near(0, 0, row_north.at[full], got_south, (north, lon)),
        near(0, 0, packed.at[1, tail], corners[0], (north, east)),
        near(0, 4, packed.at[0, tail], corners[1], (north, west)),
    )
    southward = (
        near(1, 1, row_south.at[full], got_north, (south, lon)),
        near(1, 1, packed.at[1, head], corners[2], (south, east)),
        near(1, 5, packed.at[0, head], corners[3], (south, west)),
    )
    to_east = near(2, 2, packed.at[1], got_west, (lat, east))
    to_west = near(2, 3, packed.at[0], got_east, (lat, west))
    deep_east = near(4, 7, deep_packed, deep_strip, (lat, east))
    deep_up = near(5, 8, deep_packed.at[tail], deep_south, (north, east))
    deep_down = near(6, 9, deep_packed.at[head], deep_north, (south, east))

    def across_half(step):
        return (lat, lax.rem(lon + step + n_lon, n_lon))

    far_away = near(7, 10, deep_rows, far_rows, across_half(-half))
    far_west_edge = near(8, 10, packed.at[1, tall_tail], far_edges[0], across_half(1 - half))
    far_east_edge = near(9, 10, packed.at[0, tall_tail], far_edges[1], across_half(-1 - half))
    gives_west_edge = on_top & (lon >= half - 1) & (lon < n_lon - 1)
    gives_east_edge = on_top & ((lon > half) | (lon == 0))

    def spread(source, slot, send_sem, recv_sem, along_lat):
        size = n_lat if along_lat else n_lon
        me = lat if along_lat else lon
        copies = []
        for d in range(1, size):
            peer = lax.rem(me + d, size)
            copies.append(
                pltpu.make_async_remote_copy(
                    src_ref=source, dst_ref=slot, send_sem=send_sem,
                    recv_sem=recv_sem,
                    device_id=(peer, lon) if along_lat else (lat, peer),
                    device_id_type=MESH,
                )
            )
        return copies

    across = spread(
        fold_rows.at[full], fold_all.at[lon, full], near_send.at[3], near_recv.at[6], False
    )

    to_west.start()
    to_east.start()

    @pl.when(has_north)
    def _():
        for copy in northward:
            copy.start()

    @pl.when(has_south)
    def _():
        for copy in southward:
            copy.start()

    @pl.when(at_seam)
    def _():
        for g in range(n_groups):
            here = pl.ds(PAD + g * group_rows, group_rows)
            inside = lane_group - g * GROUP
            value = jnp.where(
                inside < LIP,
                turned(centre[0, here, :], g * GROUP + 2 * LIP),
                jnp.where(
                    inside < 2 * LIP,
                    turned(centre[1, here, :], g * GROUP + 3 * LIP - 1),
                    turned(centre[2, here, :], g * GROUP + 4 * LIP - 1),
                ),
            )
            if g:
                value = jnp.where(inside >= 0, value, deep_packed[...])
            deep_packed[...] = value
        deep_east.start()

        @pl.when(has_north)
        def _():
            deep_up.start()

        @pl.when(has_south)
        def _():
            deep_down.start()

    @pl.when(on_top)
    def _():
        for index, top_row in enumerate((LIP, STEPS, STEPS)):
            low = last - top_row - LIP
            deep_rows[index * LIP : (index + 1) * LIP, :] = centre[index, low : low + LIP, :]
        for copy in reversed(across):
            copy.start()

    for condition, copy in (
        (fold_late, far_away),
        (gives_west_edge, far_west_edge),
        (gives_east_edge, far_east_edge),
    ):
        @pl.when(condition)
        def _():
            copy.start()

    dot_sums = {}

    def add_dot(key, left, right):
        product = left * right
        for r in range(0, product.shape[0], 8):
            piece = product[r : r + 8, :]
            dot_sums[key] = piece if key not in dot_sums else dot_sums[key] + piece

    def flush(new):
        for key in list(dot_sums):
            total = dot_sums.pop(key)
            spot = order_of()[key]
            dots[spot] = total if new else dots[spot] + total

    lane8 = lax.broadcasted_iota(jnp.int32, (8, width), 1)
    nothing = jnp.zeros((8, width), jnp.float32)

    prepare(rows, wide, wide_shifted, wide_weights, wide_basis)
    middle = (lane8 >= LIP) & (lane8 < width - LIP)

    def keep_wide(at, count):
        return kept(at, count, [(LIP, rows - LIP, middle)])

    march(rows, wide_weights, wide_basis, keep_wide, add_dot, flush, True)

    part_spans = ((0, 0, LIP), (1, LIP, STEPS), (2, LIP + STEPS, STEPS))

    def unpack_west(got, target, start, g, count):
        lane = lax.broadcasted_iota(jnp.int32, (count, width), 1)
        for index, offset, cells in part_spans:
            value = turned(got, -g * GROUP - offset - cells)
            target[index, start : start + count, :] = jnp.where(lane >= width - cells, value, 0.0)

    def unpack_east(got, target, start, g, count):
        lane = lax.broadcasted_iota(jnp.int32, (count, width), 1)
        for index, offset, cells in part_spans:
            value = turned(got, -g * GROUP - offset)
            target[index, start : start + count, :] = jnp.where(
                lane < cells, value, target[index, start : start + count, :]
            )

    def unpack_deep(got, start, g, count):
        lane = lax.broadcasted_iota(jnp.int32, (count, width), 1)
        for index, cells in ((0, LIP), (1, STEPS), (2, STEPS)):
            low = width - cells - LIP
            value = turned(got, low - g * GROUP - index * LIP)
            side[index, start : start + count, :] = jnp.where(
                (lane >= low) & (lane < low + LIP), value, side[index, start : start + count, :]
            )

    for index in (0, 1, 2):
        for at in (0, 8, last, last + 8):
            centre[index, at : at + 8, :] = nothing
            side[index, at : at + 8, :] = nothing

    def take_east():
        arrival(3, got_east).wait_recv()
        for g in range(n_groups):
            unpack_east(got_east[...], side, first + g * group_rows, g, group_rows)

        @pl.when(has_south)
        def _():
            arrival(4, corners[1]).wait_recv()
            unpack_east(corners[1][...], side, first - LIP, n_groups - 1, LIP)

        @pl.when(has_north)
        def _():
            arrival(5, corners[3]).wait_recv()
            unpack_east(corners[3][...], side, last, 0, LIP)

    def folded(home):
        total = n_lon * width
        pivot = lax.rem(fold_map[0] - home * width + total, total)
        block, offset = pivot // width, lax.rem(pivot, width)
        lane = lax.broadcasted_iota(jnp.int32, (32, width), 1)
        index = lax.rem(offset - lane + width, width)

        def mirrored(which):
            rows_of = fold_all[lax.rem(block + which + n_lon, n_lon)]
            return jnp.take_along_axis(rows_of, index, axis=1, mode="promise_in_bounds")

        ahead, same, behind, beyond = (mirrored(which) for which in (1, 0, -1, -2))
        close = lane <= offset
        value = jnp.where(close, same, behind)
        halo = jnp.where(
            lane < width // 2, jnp.where(close, behind, beyond), jnp.where(close, ahead, same)
        )
        return value, halo

    def take_fold():
        arrival(6, fold_all.at[0 : n_lon - 1, full]).wait_recv()
        for source, target in zip(folded(lon), (centre, side)):
            for index, at, count in spans:
                target[index, last : last + count, :] = source[at : at + count, :]

    n_parts = width // GROUP // 2
    part_rows = rows // n_parts
    strip_rows = part_rows + 2 * MARGIN
    seam_rows = strip_rows + 2 * BAND
    north_at, south_at = strip_rows, strip_rows + BAND
    own = GROUP - LIP
    slot_of = lane8 // GROUP
    slot_lane = lane8 - slot_of * GROUP

    def assemble():
        targets = (seam.at[0], seam_basis.at[0], seam_basis.at[STEPS + 1])
        for index, target in enumerate(targets):
            for at in range(0, strip_rows, 8):
                value = None
                for q in range(n_parts):
                    low = PAD + q * part_rows - MARGIN + at
                    inside, outside = centre[index, low : low + 8, :], side[index, low : low + 8, :]
                    east_slot = turned(
                        jnp.where(lane8 >= width - own, inside, outside),
                        q * GROUP - (width - own),
                    )
                    west_slot = turned(
                        jnp.where(lane8 < own, inside, outside), (n_parts + q) * GROUP + LIP
                    )
                    mixed = jnp.where(lane8 < n_parts * GROUP, east_slot, west_slot)
                    value = mixed if q == 0 else jnp.where(
                        lax.rem(slot_of, n_parts) >= q, mixed, value
                    )
                target[8 + at : 16 + at, :] = value
            for at in range(0, BAND, 8):
                low = last + LIP - BAND + at
                target[8 + north_at + at : 16 + north_at + at, :] = centre[index, low : low + 8, :]
                low = first - LIP + at
                target[8 + south_at + at : 16 + south_at + at, :] = centre[index, low : low + 8, :]
        prepare(seam_rows, seam, seam_shifted, seam_weights, seam_basis)

    arrival(2, got_west).wait_recv()
    for g in range(n_groups):
        unpack_west(got_west[...], side, first + g * group_rows, g, group_rows)

    @pl.when(has_south)
    def _():
        arrival(0, got_rows.at[0, near_rows]).wait_recv()
        for index, at, count in spans:
            centre[index, first - count : first, :] = got_south[at : at + count, :]
        unpack_west(corners[0][...], side, first - LIP, n_groups - 1, LIP)

    @pl.when(has_north)
    def _():
        arrival(1, got_rows.at[1, near_rows]).wait_recv()
        for index, at, count in spans:
            centre[index, last : last + count, :] = got_north[at : at + count, :]
        unpack_west(corners[2][...], side, last, 0, LIP)

    @pl.when(jnp.logical_not(at_seam))
    def _():
        take_east()

    @pl.when(fold_early)
    def _():
        take_fold()

    assemble()
    east_half = lane8 < n_parts * GROUP
    strip_at = jnp.where(east_half, slot_lane - (own - LIP), slot_lane - LIP)
    closed = jnp.where(fold_late, 1, 0)
    strip_lanes = (strip_at >= 0) & (strip_at < LIP) & (
        jnp.where(east_half, lon, -1) < n_lon - 1
    )
    last_part = lax.rem(slot_of, n_parts) == n_parts - 1
    north_lanes = strip_lanes & (jnp.where(last_part, closed, 0) == 0)
    band_lanes = jnp.where(middle, closed, 1) == 0

    def keep_seam(at, count):
        return kept(
            at,
            count,
            [
                (MARGIN, MARGIN + part_rows - LIP, strip_lanes),
                (MARGIN + part_rows - LIP, MARGIN + part_rows, north_lanes),
                (north_at + BAND - 2 * LIP, north_at + BAND - LIP, band_lanes),
                (south_at + LIP, south_at + 2 * LIP, middle),
            ],
        )

    march(seam_rows, seam_weights, seam_basis, keep_seam, add_dot, flush, False)

    patch_rows = group_rows + 2 * MARGIN
    far_tile_rows = patch_rows + 2 * BAND

    @pl.when(past_seam | fold_early)
    def _():
        @pl.when(past_seam)
        def _():
            arrival(7, deep_strip).wait_recv()
            for g in range(n_groups):
                unpack_deep(deep_strip[...], first + g * group_rows, g, group_rows)

            @pl.when(has_south)
            def _():
                arrival(8, deep_south).wait_recv()
                unpack_deep(deep_south[...], first - LIP, n_groups - 1, LIP)

            @pl.when(has_north)
            def _():
                arrival(9, deep_north).wait_recv()
                unpack_deep(deep_north[...], last, 0, LIP)

        for target in (far_centre, far_side):
            for index in (0, 1, 2):
                for at in range(0, BAND, 8):
                    target[index, at : at + 8, :] = nothing

        edge_row = BAND - LIP

        @pl.when(fold_early)
        def _():
            arrival(10, got_far).wait_recv()
            home = lon + half
            low = edge_row - 2 * LIP
            unpack_west(far_edges[0][...], far_side, low, n_groups - 1, 2 * LIP)
            unpack_east(far_edges[1][...], far_side, low, n_groups - 1, 2 * LIP)
            mirror = folded(home)
            for index, at, count in spans:
                low = edge_row - count - LIP
                far_centre[index, low : low + LIP, :] = far_rows[
                    index * LIP : (index + 1) * LIP, :
                ]
                for r in range(count):
                    far_centre[index, edge_row - 1 - r : edge_row - r, :] = fold_all[
                        home, at + r : at + r + 1, :
                    ]
                for source, target in zip(mirror, (far_centre, far_side)):
                    target[index, edge_row : edge_row + count, :] = source[at : at + count, :]

        span_lanes = GROUP - 2 * LIP
        targets = (far.at[0], far_basis.at[0], far_basis.at[STEPS + 1])
        for index, target in enumerate(targets):
            for at in range(0, patch_rows, 8):
                value = None
                for g in range(n_groups):
                    low = PAD + g * group_rows - MARGIN + at
                    mixed = turned(
                        jnp.where(
                            lane8 < span_lanes,
                            centre[index, low : low + 8, :],
                            side[index, low : low + 8, :],
                        ),
                        g * GROUP + 2 * LIP,
                    )
                    value = mixed if g == 0 else jnp.where(slot_of >= g, mixed, value)
                target[8 + at : 16 + at, :] = value
            for at in range(0, BAND, 8):
                inside, outside = far_centre[index, at : at + 8, :], far_side[index, at : at + 8, :]
                spot = 8 + patch_rows + at
                target[spot : spot + 8, :] = inside
                spot += BAND
                target[spot : spot + 8, :] = jnp.where(
                    lane8 < GROUP,
                    turned(jnp.where(lane8 >= width - own, inside, outside), own - width),
                    turned(jnp.where(lane8 < own, inside, outside), GROUP + LIP),
                )
        prepare(far_tile_rows, far, far_shifted, far_weights, far_basis)
        patch_lanes = jnp.where((slot_lane >= LIP) & (slot_lane < 2 * LIP), lon, 1) == 0
        upper = jnp.where(slot_of == n_groups - 1, jnp.where(on_top, 1, 0), 0) == 0
        idle = jnp.where(fold_early, 0, 1)
        fold_lanes = jnp.where(middle, idle, 1) == 0
        edge_at = jnp.where(slot_of == 0, slot_lane - (own - LIP), slot_lane - LIP)
        edge_lanes = jnp.where(
            (slot_of < 2) & (edge_at >= 0) & (edge_at < LIP), idle, 1
        ) == 0

        def keep_far(at, count):
            fold_at = patch_rows + BAND - 2 * LIP
            return kept(
                at,
                count,
                [
                    (MARGIN, MARGIN + group_rows - LIP, patch_lanes),
                    (MARGIN + group_rows - LIP, MARGIN + group_rows, patch_lanes & upper),
                    (fold_at, fold_at + LIP, fold_lanes),
                    (fold_at + BAND, fold_at + BAND + LIP, edge_lanes),
                ],
            )

        march(far_tile_rows, far_weights, far_basis, keep_far, add_dot, flush, False)

    def finish_late():
        @pl.when(at_seam | fold_late)
        def _():
            @pl.when(at_seam)
            def _():
                take_east()

            @pl.when(fold_late)
            def _():
                take_fold()

            assemble()
            march(seam_rows, seam_weights, seam_basis, None, None, None, False)

    number = len(order_of())
    pending = []
    lane = lax.broadcasted_iota(jnp.int32, (8, width), 1)
    home = lane - lax.broadcasted_iota(jnp.int32, (8, width), 0)
    message = jnp.zeros((8, width), jnp.float32)
    for g in range(number // 8):
        grouped = fold_sublanes([dots[8 * g + s] for s in range(8)])
        message = jnp.where(home == 8 * g, jnp.sum(grouped, axis=1, keepdims=True), message)
    message = jnp.sum(message, axis=0, keepdims=True)
    if direct:
        slots, send_sem, recv_sem = moment_refs
        me = lat * n_lon + lon
        slots[me] = message
        copies = [
            pltpu.make_async_remote_copy(
                src_ref=slots.at[me], dst_ref=slots.at[me], send_sem=send_sem,
                recv_sem=recv_sem,
                device_id=(lax.rem(lat + a, n_lat), lax.rem(lon + b, n_lon)),
                device_id_type=MESH,
            )
            for a, b in everyone
        ]
        rounds = ((slots, n_lat * n_lon, copies, send_sem, recv_sem),)
    else:
        slots_lat, slots_lon, lat_send, lat_recv, lon_send, lon_recv = moment_refs
        rounds = (
            (slots_lat, n_lat, None, lat_send, lat_recv, lat, True),
            (slots_lon, n_lon, None, lon_send, lon_recv, lon, False),
        )
    for slots, size, copies, send_sem, recv_sem, *rest in rounds:
        if copies is None:
            me, along_lat = rest
            slots[me] = message
            copies = spread(slots.at[me], slots.at[me], send_sem, recv_sem, along_lat)
        for copy in copies:
            copy.start()
        if not pending:
            finish_late()
        others = slots.at[0 : size - 1]
        whole = pltpu.make_async_remote_copy(
            src_ref=others, dst_ref=others, send_sem=send_sem, recv_sem=recv_sem,
            device_id=(lat, lon), device_id_type=MESH,
        )
        whole.wait_recv()
        terms = [slots[index] for index in range(size)]
        while len(terms) > 1:
            odd = terms[len(terms) // 2 * 2 :]
            terms = [x + y for x, y in zip(terms[0::2], terms[1::2])] + odd
        message = terms[0]
        pending.append(whole)
    message = jnp.broadcast_to(message, (8, width))
    for g in range(number // 8):
        picked = jnp.sum(jnp.where(home == 8 * g, message, 0.0), axis=1, keepdims=True)
        moment_rows[8 * g : 8 * g + 8, :] = jnp.broadcast_to(picked, (8, width))
    moments = {}
    for kind in (("p", "p"), ("p", "r"), ("r", "r")):
        series = []
        for index in range(17 if kind == ("p", "p") else 16 if kind == ("p", "r") else 15):
            spot = order_of()[kind + (index,)]
            value = jnp.broadcast_to(moment_rows[spot : spot + 1, :], (8, width))
            series.append(value if index < 2 else 2.0 * value - series[index % 2])
        moments[kind] = series
    height_coords, residual_coords = coordinates(moments)
    wanted = (height_coords, residual_coords)

    def combined(fields, at):
        totals = [None, None]
        for chain, power in sorted(height_coords | residual_coords):
            slot = power + (0 if chain == "p" else STEPS + 1)
            field = fields[slot, 8 + at : 16 + at, :]
            for which, coords in enumerate(wanted):
                if (chain, power) in coords:
                    term = coords[(chain, power)] * field
                    totals[which] = term if totals[which] is None else totals[which] + term
        return totals

    for at in range(0, seam_rows, 8):
        for which, total in enumerate(combined(seam_basis, at)):
            patch[which, at : at + 8, :] = total
    row8 = lax.broadcasted_iota(jnp.int32, (8, width), 0)
    for at in range(0, rows, 8):
        q = at // part_rows
        for which, total in enumerate(combined(wide_basis, at)):
            for low, high, source in (
                (0, LIP, south_at + LIP),
                (rows - LIP, rows, north_at + BAND - LIP - rows),
            ):
                if low < at + 8 and high > at:
                    edge = patch[which, source + at : source + at + 8, :]
                    if low <= at and high >= at + 8:
                        total = edge
                    else:
                        total = jnp.where((row8 >= low - at) & (row8 < high - at), edge, total)
            spot = at - q * part_rows + MARGIN
            strip = patch[which, spot : spot + 8, :]
            total = jnp.where(lane8 < LIP, turned(strip, -(n_parts + q) * GROUP - LIP), total)
            total = jnp.where(
                lane8 >= width - LIP, turned(strip, width - own - q * GROUP), total
            )
            (out_height, out_residual)[which][at : at + 8, :] = total

    for copy in pending:
        copy.wait_send()
    departure(2, got_sides).wait_send()
    for condition, index, block in (
        (has_north, 0, got_rows.at[0]),
        (has_south, 1, got_rows.at[1]),
        (on_top, 3, fold_all.at[0 : n_lon - 1, full]),
        (at_seam, 4, deep_packed),
        (at_seam & has_north, 5, deep_south),
        (at_seam & has_south, 6, deep_north),
        (fold_late, 7, far_rows),
        (gives_west_edge, 8, far_edges[0]),
        (gives_east_edge, 9, far_edges[1]),
    ):
        @pl.when(condition)
        def _():
            departure(index, block).wait_send()


@functools.cache
def order_of():
    keys = [("p", "p", k) for k in range(2 * STEPS + 1)]
    keys += [("p", "r", k) for k in range(2 * STEPS)]
    keys += [("r", "r", k) for k in range(2 * STEPS - 1)]
    return {key: index for index, key in enumerate(keys)}


def hand_over(height, residual, out_height, out_residual):
    out_height[...] = height[...]
    out_residual[...] = residual[...]


def per_device(n_lat, n_lon, forcing, search_direction, ocean_depth, land_mask, fold_map):
    rows, width = forcing.shape
    tall = rows + 2 * PAD
    f32 = jnp.float32
    n_parts = width // GROUP // 2
    seam_rows = rows // n_parts + 2 * MARGIN + 2 * BAND

    def tile(count):
        return [
            pltpu.VMEM((planes, count + 16, width), f32)
            for planes in (2, 4, 8, 2 * STEPS + 1)
        ]

    edge = pltpu.VMEM((32, width), f32)
    group_rows = rows * GROUP // width
    dma = pltpu.SemaphoreType.DMA
    if n_lat * n_lon <= DIRECT_LIMIT:
        moment_refs = [pltpu.VMEM((n_lat * n_lon, 1, width), f32), dma, dma]
    else:
        moment_refs = [pltpu.VMEM((size, 1, width), f32) for size in (n_lat, n_lon)] + [dma] * 4
    block = pl.BlockSpec(memory_space=pltpu.VMEM)
    outs = pl.pallas_call(
        functools.partial(kernel, n_lat, n_lon),
        out_shape=[pltpu.VMEM((rows, width), f32)] * 2,
        in_specs=[pl.BlockSpec(memory_space=pl.ANY)] * 5,
        out_specs=[block] * 2,
        scratch_shapes=[
            pltpu.VMEM((3, rows, width), f32), pltpu.VMEM((rows, width), jnp.int32),
            pltpu.SMEM(fold_map.shape, jnp.int32),
            pltpu.VMEM((3, tall, width), f32), pltpu.VMEM((3, tall, width), f32),
            *tile(rows),
            *tile(seam_rows),
            *tile(group_rows + 2 * MARGIN + 2 * BAND),
            pltpu.VMEM((2, seam_rows, width), f32),
            edge, edge, edge,
            pltpu.VMEM((2, group_rows, width), f32),
            pltpu.VMEM((2, 3 * LIP + 2 * STEPS, width), f32),
            pltpu.VMEM((2, group_rows, width), f32),
            pltpu.VMEM((n_lon, 32, width), f32),
            pltpu.VMEM((group_rows, width), f32),
            pltpu.VMEM((group_rows + 2 * LIP, width), f32),
            pltpu.VMEM((3 * LIP, width), f32),
            pltpu.VMEM((7 * LIP, width), f32),
            pltpu.VMEM((3, BAND, width), f32), pltpu.VMEM((3, BAND, width), f32),
            pltpu.VMEM((6 * STEPS, 8, width), f32),
            pltpu.VMEM((6 * STEPS, width), f32),
            dma((3,)), dma((10,)), dma((11,)),
            *moment_refs,
        ],
        compiler_params=pltpu.CompilerParams(collective_id=0, has_side_effects=True),
        name="tripole_cg",
    )(forcing, search_direction, ocean_depth, land_mask, fold_map)
    return pl.pallas_call(
        hand_over,
        out_shape=[jax.ShapeDtypeStruct((rows, width), f32)] * 2,
        in_specs=[block] * 2,
        out_specs=[block] * 2,
        name="hand_over",
    )(*(pltpu.with_memory_space_constraint(out, pltpu.VMEM) for out in outs))


def solution(mesh):
    cells = P("lat", "lon")
    return jax.shard_map(
        functools.partial(per_device, mesh.shape["lat"], mesh.shape["lon"]),
        mesh=mesh,
        in_specs=(cells, cells, cells, cells, P()),
        out_specs=(cells, cells),
        check_vma=False,
    )
```

```python
import functools

import jax
import jax.numpy as jnp
from jax import lax
from jax.experimental import pallas as pl
from jax.experimental.pallas import tpu as pltpu
from jax.sharding import PartitionSpec as P

STEPS = 8
REACH = 256
MESH = pl.DeviceIdType.MESH
PAD = 16
GROUP = 32
CHUNK = 16
LIP = STEPS + 1
MARGIN = 12
BAND = 32
DIRECT_LIMIT = 64

DIRECTIONS = ((1, 0), (-1, 0), (0, 1), (0, -1), (1, 1), (-1, -1), (1, -1), (-1, 1))
SLOT = {offset: index for index, offset in enumerate(DIRECTIONS)}


def halves(offset):
    return 0.5 if 0 in offset else 0.25


def chunks_of(low, high, size):
    return [(at, min(size, high - at)) for at in range(low, high, size)]


def turned(x, shift):
    shift = shift % x.shape[1]
    return x if shift == 0 else pltpu.roll(x, shift, 1)


def bilinear(left, right, gram):
    total = None
    for i in sorted(left):
        inner = None
        for j in sorted(right):
            term = gram(i, j) * right[j]
            inner = term if inner is None else inner + term
        inner = left[i] * inner
        total = inner if total is None else total + inner
    return total


def plus(left, right):
    result = dict(left)
    for key, value in right.items():
        result[key] = result[key] + value if key in result else value
    return result


def scaled(factor, vector):
    return {key: factor * value for key, value in vector.items()}


def apply_shift(vector):
    result = {}
    for (chain, power), value in vector.items():
        parts = [((chain, power), value)]
        if power == 0:
            parts.append(((chain, 1), value))
        else:
            half = 0.5 * value
            parts += [((chain, power + 1), half), ((chain, power - 1), half)]
        result = plus(result, {}) if not parts else result
        for key, part in parts:
            result = plus(result, {key: part})
    return result


def coordinates(moments):
    cache = {}

    def gram(left, right):
        kind = (left[0], right[0]) if left[0] <= right[0] else (right[0], left[0])
        low, high = sorted((left[1], right[1]))
        key = (kind, low, high)
        if key not in cache:
            series = moments[kind]
            cache[key] = 0.5 * (series[high + low] + series[high - low])
        return cache[key]

    solution_coords = {}
    one = jnp.ones_like(moments[("p", "p")][0])
    direction_coords = {("p", 0): one}
    residual_coords = {("r", 0): one}
    norm_now = bilinear(residual_coords, residual_coords, gram)
    for _ in range(STEPS):
        mapped = apply_shift(direction_coords)
        step_length = norm_now / bilinear(direction_coords, mapped, gram)
        solution_coords = plus(solution_coords, scaled(step_length, direction_coords))
        residual_coords = plus(residual_coords, scaled(-step_length, mapped))
        norm_next = bilinear(residual_coords, residual_coords, gram)
        direction_coords = plus(
            residual_coords, scaled(norm_next / norm_now, direction_coords)
        )
        norm_now = norm_next
    return solution_coords, residual_coords


def fold_sublanes(parts):
    row = lax.broadcasted_iota(jnp.int32, parts[0].shape, 0)
    parts = list(parts)
    span = 4
    while span:
        low = (row & span) == 0
        half = len(parts) // 2
        parts = [
            jnp.where(low, first, second)
            + pltpu.roll(jnp.where(low, second, first), span, 0)
            if span == 4
            else jnp.where(low, first, second)
            + jnp.where(low, pltpu.roll(first, 8 - span, 0), pltpu.roll(second, span, 0))
            for first, second in zip(parts[:half], parts[half:])
        ]
        span //= 2
    return parts[0]


def kept(at, count, regions):
    row = lax.broadcasted_iota(jnp.int32, (8, regions[0][2].shape[1]), 0)
    masks = []
    for r in range(at, at + count, 8):
        mask = None
        for low, high, lanes in regions:
            if low >= r + 8 or high <= r:
                continue
            part = lanes
            if low > r or high < r + 8:
                part = lanes & (row >= low - r) & (row < high - r)
            mask = part if mask is None else mask | part
        masks.append(mask)
    return masks


def prepare(rows, depth_root, shifted, weights, basis):
    width = depth_root.shape[2]
    zero = jnp.zeros((8, width), jnp.float32)
    for at in (0, 8 + rows):
        span = pl.ds(at, 8)
        depth_root[0, span, :] = zero
        depth_root[1, span, :] = zero
        for slot in range(2 * STEPS + 1):
            if slot not in (STEPS, 2 * STEPS):
                basis[slot, span, :] = zero

    depth, root = depth_root.at[0], depth_root.at[1]
    for at, count in chunks_of(0, rows + 16, CHUNK):
        span = pl.ds(at, count)
        shifted[0, span, :] = turned(depth[span, :], -1)
        shifted[1, span, :] = turned(depth[span, :], 1)
    shifted_depth = {0: depth, 1: shifted.at[0], -1: shifted.at[1]}
    for at, count in chunks_of(8, 8 + rows, CHUNK):
        here = depth[at : at + count, :]
        sums = {0.5: None, 0.25: None}
        for a, b in DIRECTIONS:
            beside = shifted_depth[b][at + a : at + a + count, :]
            link = jnp.where(beside > 0.0, here + beside, 0.0)
            factor = halves((a, b))
            sums[factor] = link if sums[factor] is None else sums[factor] + link
        diagonal = here * (1.0 / (REACH * REACH)) + (0.5 * sums[0.5] + 0.25 * sums[0.25])
        value = lax.rsqrt(jnp.where(here > 0.0, diagonal, 1.0))
        span = pl.ds(at, count)
        root[span, :] = value
        shifted[2, span, :] = turned(value, -1)
        shifted[3, span, :] = turned(value, 1)
    shifted_root = {0: root, 1: shifted.at[2], -1: shifted.at[3]}
    for at, count in chunks_of(8, 8 + rows, CHUNK):
        for b in (-1, 0, 1):
            goal_depth = shifted_depth[-b][at : at + count, :]
            goal_root = shifted_root[-b][at : at + count, :]
            for a in (-1, 0, 1):
                if (a, b) == (0, 0):
                    continue
                from_depth = depth[at + a : at + a + count, :]
                from_root = root[at + a : at + a + count, :]
                link = jnp.where(
                    jnp.minimum(goal_depth, from_depth) > 0.0, goal_depth + from_depth, 0.0
                )
                weights[SLOT[(a, b)], at : at + count, :] = (
                    goal_root * (-2.0 * halves((a, b)))
                ) * (link * from_root)


def needed(rows, regions, reach):
    tiles = sorted({
        at
        for low, high, _ in regions
        for at in range(max(low - reach, 0) // 8 * 8, min(high + reach, rows), 8)
    })
    runs = []
    for at in tiles:
        if runs and runs[-1][0] + runs[-1][1] == at and runs[-1][1] < CHUNK:
            runs[-1][1] += 8
        else:
            runs.append([at, 8])
    return [(8 + at, count) for at, count in runs]


def march(rows, weights, basis, regions, add_dot, flush, new):
    def keep(at, count):
        return kept(at, count, regions)

    def masked(masks, value):
        return [
            None if mask is None else jnp.where(mask, value[8 * i : 8 * i + 8, :], 0.0)
            for i, mask in enumerate(masks)
        ]

    def dot(key, left, right):
        for i, piece in enumerate(left):
            if piece is not None:
                add_dot(key, piece, right[8 * i : 8 * i + 8, :])

    for at, count in needed(rows, regions, 0) if add_dot else []:
        p0 = basis[0, at : at + count, :]
        r0 = basis[STEPS + 1, at : at + count, :]
        masks = keep(at - 8, count)
        p0_kept, r0_kept = masked(masks, p0), masked(masks, r0)
        dot(("p", "p", 0), p0_kept, p0)
        dot(("r", "r", 0), r0_kept, r0)
        dot(("p", "r", 0), p0_kept, r0)

    for power in range(1, STEPS + 1):
        chains = [("p", 0)] + ([("r", STEPS + 1)] if power < STEPS else [])
        for at, count in needed(rows, regions, STEPS - power):
            fresh = {}
            held = {}
            factors = {ab: weights[SLOT[ab], at : at + count, :] for ab in DIRECTIONS}
            for name, origin in chains:
                slot = origin + power
                taken = {a: basis[slot - 1, at + a : at + a + count, :] for a in (-1, 0, 1)}
                held[name] = taken[0]
                columns = {}
                for b in (-1, 0, 1):
                    total = None
                    for a in (-1, 0, 1):
                        if (a, b) == (0, 0):
                            continue
                        term = factors[(a, b)] * taken[a]
                        total = term if total is None else total + term
                    columns[b] = total
                value = columns[0] + turned(columns[1], -1) + turned(columns[-1], 1)
                if power == 1:
                    value = 0.5 * value
                else:
                    value = value - basis[slot - 2, at : at + count, :]
                basis[slot, at : at + count, :] = value
                fresh[name] = value
            if not add_dot:
                continue
            masks = keep(at - 8, count)
            fresh_kept = {name: masked(masks, fresh[name]) for name, _ in chains}
            for name, _ in chains:
                dot((name, name, 2 * power), fresh_kept[name], fresh[name])
                dot((name, name, 2 * power - 1), fresh_kept[name], held[name])
            if power < STEPS:
                dot(("p", "r", 2 * power), fresh_kept["p"], fresh["r"])
                dot(("p", "r", 2 * power - 1), fresh_kept["p"], held["r"])
            else:
                dot(
                    ("p", "r", 2 * power - 1),
                    fresh_kept["p"],
                    basis[STEPS + power, at : at + count, :],
                )
        if add_dot:
            flush(new)


def kernel(
    n_lat, n_lon, forcing_hbm, search_hbm, depth_hbm, mask_hbm, fold_hbm,
    out_height, out_residual, loaded, mask_in, fold_map,
    centre, side, wide, wide_shifted, wide_weights, wide_basis, seam, seam_shifted,
    seam_weights, seam_basis, far, far_shifted, far_weights, far_basis, patch, row_north, row_south,
    fold_rows, packed, got_rows, got_sides, fold_all, deep_packed, got_deep, deep_rows, got_far,
    far_centre, far_side, dots, moment_rows, load_sem, near_send, near_recv, *moment_refs,
):
    rows, width = forcing_hbm.shape
    lat, lon = lax.axis_index("lat"), lax.axis_index("lon")
    top = n_lat - 1
    north, south = lax.rem(lat + 1, n_lat), lax.rem(lat + n_lat - 1, n_lat)
    east, west = lax.rem(lon + 1, n_lon), lax.rem(lon + n_lon - 1, n_lon)
    has_north, has_south = lat < top, lat > 0
    group_rows = rows * GROUP // width
    n_groups = width // GROUP

    barrier = pltpu.get_barrier_semaphore()

    def greet(place):
        pl.semaphore_signal(barrier, inc=1, device_id=place, device_id_type=MESH)

    for source, target, index in (
        (mask_hbm, mask_in, 0), (depth_hbm, loaded.at[0], 1), (search_hbm, loaded.at[1], 1),
        (forcing_hbm, loaded.at[2], 1), (fold_hbm, fold_map, 2),
    ):
        pltpu.make_async_copy(source, target, load_sem.at[index]).start()
    depth_in, search, forcing = loaded.at[0], loaded.at[1], loaded.at[2]
    direct = n_lat * n_lon <= DIRECT_LIMIT
    everyone = [(a, b) for a in range(n_lat) for b in range(n_lon) if a or b]
    everyone.sort(key=lambda d: (d[1] or n_lon, d[0] or n_lat))
    if direct:
        for a, b in everyone:
            greet((lax.rem(lat + a, n_lat), lax.rem(lon + b, n_lon)))
        greeted = len(everyone)
    else:
        for d in range(1, n_lat):
            greet((lax.rem(lat + d, n_lat), lon))
        for d in range(1, n_lon):
            greet((lat, lax.rem(lon + d, n_lon)))
        for place in ((north, east), (north, west), (south, east), (south, west)):
            greet(place)
        greeted = n_lat - 1 + n_lon - 1 + 4

    pltpu.make_async_copy(mask_hbm, mask_in, load_sem.at[0]).wait()
    pltpu.make_async_copy(loaded, loaded, load_sem.at[1]).wait()
    pltpu.make_async_copy(fold_hbm, fold_map, load_sem.at[2]).wait()
    lane_group = lax.broadcasted_iota(jnp.int32, (group_rows, width), 1)
    west_edge = east_edge = None
    for g in range(n_groups):
        here = pl.ds(g * group_rows, group_rows)
        there = pl.ds(PAD + g * group_rows, group_rows)
        flag = mask_in[here, :].astype(jnp.float32)
        deep = depth_in[here, :] * flag
        moving = search[here, :] * flag
        left = forcing[here, :] * flag
        for index, value in enumerate((deep, moving, left)):
            centre[index, there, :] = value
        inner = pl.ds(8 + g * group_rows, group_rows)
        wide[0, inner, :] = deep
        wide_basis[0, inner, :] = moving
        wide_basis[STEPS + 1, inner, :] = left
        inside = lane_group - g * GROUP
        to_west = jnp.where(
            inside < 9,
            turned(deep, g * GROUP),
            jnp.where(inside < 17, turned(moving, g * GROUP + 9), turned(left, g * GROUP + 17)),
        )
        to_east = jnp.where(
            inside < 9,
            turned(deep, g * GROUP + 9),
            jnp.where(inside < 17, turned(moving, g * GROUP + 17), turned(left, g * GROUP + 25)),
        )
        west_edge = to_west if g == 0 else jnp.where(inside >= 0, to_west, west_edge)
        east_edge = to_east if g == 0 else jnp.where(inside >= 0, to_east, east_edge)
    packed[0] = west_edge
    packed[1] = east_edge
    first, last = PAD, PAD + rows
    spans = ((0, 0, LIP), (1, LIP, STEPS), (2, LIP + STEPS, STEPS))
    depth_of = LIP + 2 * STEPS
    for index, at, count in spans:
        row_south[at : at + count, :] = centre[index, first : first + count, :]
        row_north[at : at + count, :] = centre[index, last - count : last, :]

    @pl.when(lat == top)
    def _():
        for index, at, count in spans:
            for r in range(count):
                fold_rows[at + r : at + r + 1, :] = centre[index, last - 1 - r : last - r, :]
        fold_all[lon, 0:depth_of, :] = fold_rows[0:depth_of, :]

    pl.semaphore_wait(barrier, greeted)

    half = n_lon // 2
    at_seam, past_seam = lon == n_lon - 1, lon == 0
    on_top = lat == top
    fold_late, fold_early = on_top & (lon > half), on_top & (lon >= 1) & (lon < half)

    def near(gone, arrived, source, target, place):
        return pltpu.make_async_remote_copy(
            src_ref=source, dst_ref=target, send_sem=near_send.at[gone],
            recv_sem=near_recv.at[arrived], device_id=place, device_id_type=MESH,
        )

    def arrival(index, block):
        return near(0, index, block, block, (lat, lon))

    def departure(index, block):
        return near(index, 0, block, block, (lat, lon))

    tail, head = pl.ds(group_rows - LIP, LIP), pl.ds(0, LIP)
    tall_tail = pl.ds(group_rows - 2 * LIP, 2 * LIP)
    full = pl.ds(0, depth_of)
    near_rows = pl.ds(0, depth_of + LIP)
    got_south, got_north = got_rows.at[0, full], got_rows.at[1, full]
    got_west, got_east = got_sides.at[0], got_sides.at[1]
    corners = [got_rows.at[index // 2, pl.ds(depth_of + LIP * (index % 2), LIP)] for index in range(4)]
    deep_strip = got_deep.at[0:group_rows]
    deep_south = got_deep.at[group_rows : group_rows + LIP]
    deep_north = got_deep.at[group_rows + LIP : group_rows + 2 * LIP]
    far_rows = got_far.at[0 : 3 * LIP]
    far_edges = [got_far.at[at : at + 2 * LIP] for at in (3 * LIP, 5 * LIP)]
    northward = (
        near(0, 0, row_north.at[full], got_south, (north, lon)),
        near(0, 0, packed.at[1, tail], corners[0], (north, east)),
        near(0, 4, packed.at[0, tail], corners[1], (north, west)),
    )
    southward = (
        near(1, 1, row_south.at[full], got_north, (south, lon)),
        near(1, 1, packed.at[1, head], corners[2], (south, east)),
        near(1, 5, packed.at[0, head], corners[3], (south, west)),
    )
    to_east = near(2, 2, packed.at[1], got_west, (lat, east))
    to_west = near(2, 3, packed.at[0], got_east, (lat, west))
    deep_east = near(4, 7, deep_packed, deep_strip, (lat, east))
    deep_up = near(5, 8, deep_packed.at[tail], deep_south, (north, east))
    deep_down = near(6, 9, deep_packed.at[head], deep_north, (south, east))

    def across_half(step):
        return (lat, lax.rem(lon + step + n_lon, n_lon))

    far_away = near(7, 10, deep_rows, far_rows, across_half(-half))
    far_west_edge = near(8, 10, packed.at[1, tall_tail], far_edges[0], across_half(1 - half))
    far_east_edge = near(9, 10, packed.at[0, tall_tail], far_edges[1], across_half(-1 - half))
    gives_west_edge = on_top & (lon >= half) & (lon < n_lon - 1)
    gives_east_edge = on_top & ((lon > half + 1) | (lon == 0))

    def spread(source, slot, send_sem, recv_sem, along_lat):
        size = n_lat if along_lat else n_lon
        me = lat if along_lat else lon
        copies = []
        for d in range(1, size):
            peer = lax.rem(me + d, size)
            copies.append(
                pltpu.make_async_remote_copy(
                    src_ref=source, dst_ref=slot, send_sem=send_sem,
                    recv_sem=recv_sem,
                    device_id=(peer, lon) if along_lat else (lat, peer),
                    device_id_type=MESH,
                )
            )
        return copies

    across = spread(
        fold_rows.at[full], fold_all.at[lon, full], near_send.at[3], near_recv.at[6], False
    )

    to_west.start()
    to_east.start()

    @pl.when(has_north)
    def _():
        for copy in northward:
            copy.start()

    @pl.when(has_south)
    def _():
        for copy in southward:
            copy.start()

    @pl.when(at_seam)
    def _():
        for g in range(n_groups):
            here = pl.ds(PAD + g * group_rows, group_rows)
            inside = lane_group - g * GROUP
            value = jnp.where(
                inside < LIP,
                turned(centre[0, here, :], g * GROUP + 2 * LIP),
                jnp.where(
                    inside < 2 * LIP,
                    turned(centre[1, here, :], g * GROUP + 3 * LIP - 1),
                    turned(centre[2, here, :], g * GROUP + 4 * LIP - 1),
                ),
            )
            if g:
                value = jnp.where(inside >= 0, value, deep_packed[...])
            deep_packed[...] = value
        deep_east.start()

        @pl.when(has_north)
        def _():
            deep_up.start()

        @pl.when(has_south)
        def _():
            deep_down.start()

    @pl.when(on_top)
    def _():
        for index, top_row in enumerate((LIP, STEPS, STEPS)):
            low = last - top_row - LIP
            deep_rows[index * LIP : (index + 1) * LIP, :] = centre[index, low : low + LIP, :]
        for copy in reversed(across):
            copy.start()

    for condition, copy in (
        (fold_late, far_away),
        (gives_west_edge, far_west_edge),
        (gives_east_edge, far_east_edge),
    ):
        @pl.when(condition)
        def _():
            copy.start()

    dot_sums = {}

    def add_dot(key, left, right):
        product = left * right
        for r in range(0, product.shape[0], 8):
            piece = product[r : r + 8, :]
            dot_sums[key] = piece if key not in dot_sums else dot_sums[key] + piece

    def flush(new):
        for key in list(dot_sums):
            total = dot_sums.pop(key)
            spot = order_of()[key]
            dots[spot] = total if new else dots[spot] + total

    lane8 = lax.broadcasted_iota(jnp.int32, (8, width), 1)
    nothing = jnp.zeros((8, width), jnp.float32)

    prepare(rows, wide, wide_shifted, wide_weights, wide_basis)
    middle = (lane8 >= LIP) & (lane8 < width - LIP)

    march(
        rows, wide_weights, wide_basis, [(LIP, rows - LIP, middle)], add_dot, flush, True
    )

    part_spans = ((0, 0, LIP), (1, LIP, STEPS), (2, LIP + STEPS, STEPS))

    def unpack_west(got, target, start, g, count):
        lane = lax.broadcasted_iota(jnp.int32, (count, width), 1)
        for index, offset, cells in part_spans:
            value = turned(got, -g * GROUP - offset - cells)
            target[index, start : start + count, :] = jnp.where(lane >= width - cells, value, 0.0)

    def unpack_east(got, target, start, g, count):
        lane = lax.broadcasted_iota(jnp.int32, (count, width), 1)
        for index, offset, cells in part_spans:
            value = turned(got, -g * GROUP - offset)
            target[index, start : start + count, :] = jnp.where(
                lane < cells, value, target[index, start : start + count, :]
            )

    def unpack_deep(got, start, g, count):
        lane = lax.broadcasted_iota(jnp.int32, (count, width), 1)
        for index, cells in ((0, LIP), (1, STEPS), (2, STEPS)):
            low = width - cells - LIP
            value = turned(got, low - g * GROUP - index * LIP)
            side[index, start : start + count, :] = jnp.where(
                (lane >= low) & (lane < low + LIP), value, side[index, start : start + count, :]
            )

    for index in (0, 1, 2):
        for at in (0, 8, last, last + 8):
            centre[index, at : at + 8, :] = nothing
            side[index, at : at + 8, :] = nothing

    def take_east():
        arrival(3, got_east).wait_recv()
        for g in range(n_groups):
            unpack_east(got_east[...], side, first + g * group_rows, g, group_rows)

        @pl.when(has_south)
        def _():
            arrival(4, corners[1]).wait_recv()
            unpack_east(corners[1][...], side, first - LIP, n_groups - 1, LIP)

        @pl.when(has_north)
        def _():
            arrival(5, corners[3]).wait_recv()
            unpack_east(corners[3][...], side, last, 0, LIP)

    def folded(home):
        total = n_lon * width
        pivot = lax.rem(fold_map[0] - home * width + total, total)
        block, offset = pivot // width, lax.rem(pivot, width)
        lane = lax.broadcasted_iota(jnp.int32, (32, width), 1)
        index = lax.rem(offset - lane + width, width)

        def mirrored(which):
            rows_of = fold_all[lax.rem(block + which + n_lon, n_lon)]
            return jnp.take_along_axis(rows_of, index, axis=1, mode="promise_in_bounds")

        ahead, same, behind, beyond = (mirrored(which) for which in (1, 0, -1, -2))
        close = lane <= offset
        value = jnp.where(close, same, behind)
        halo = jnp.where(
            lane < width // 2, jnp.where(close, behind, beyond), jnp.where(close, ahead, same)
        )
        return value, halo

    def take_fold():
        arrival(6, fold_all.at[0 : n_lon - 1, full]).wait_recv()
        for source, target in zip(folded(lon), (centre, side)):
            for index, at, count in spans:
                target[index, last : last + count, :] = source[at : at + count, :]

    n_parts = width // GROUP // 2
    part_rows = rows // n_parts
    strip_rows = part_rows + 2 * MARGIN
    seam_rows = strip_rows + 2 * BAND
    north_at, south_at = strip_rows, strip_rows + BAND
    own = GROUP - LIP
    slot_of = lane8 // GROUP
    slot_lane = lane8 - slot_of * GROUP

    def assemble():
        targets = (seam.at[0], seam_basis.at[0], seam_basis.at[STEPS + 1])
        for index, target in enumerate(targets):
            for at in range(0, strip_rows, 8):
                value = None
                for q in range(n_parts):
                    low = PAD + q * part_rows - MARGIN + at
                    inside, outside = centre[index, low : low + 8, :], side[index, low : low + 8, :]
                    east_slot = turned(
                        jnp.where(lane8 >= width - own, inside, outside),
                        q * GROUP - (width - own),
                    )
                    west_slot = turned(
                        jnp.where(lane8 < own, inside, outside), (n_parts + q) * GROUP + LIP
                    )
                    mixed = jnp.where(lane8 < n_parts * GROUP, east_slot, west_slot)
                    value = mixed if q == 0 else jnp.where(
                        lax.rem(slot_of, n_parts) >= q, mixed, value
                    )
                target[8 + at : 16 + at, :] = value
            for at in range(0, BAND, 8):
                low = last + LIP - BAND + at
                target[8 + north_at + at : 16 + north_at + at, :] = centre[index, low : low + 8, :]
                low = first - LIP + at
                target[8 + south_at + at : 16 + south_at + at, :] = centre[index, low : low + 8, :]
        prepare(seam_rows, seam, seam_shifted, seam_weights, seam_basis)

    arrival(2, got_west).wait_recv()
    for g in range(n_groups):
        unpack_west(got_west[...], side, first + g * group_rows, g, group_rows)

    @pl.when(has_south)
    def _():
        arrival(0, got_rows.at[0, near_rows]).wait_recv()
        for index, at, count in spans:
            centre[index, first - count : first, :] = got_south[at : at + count, :]
        unpack_west(corners[0][...], side, first - LIP, n_groups - 1, LIP)

    @pl.when(has_north)
    def _():
        arrival(1, got_rows.at[1, near_rows]).wait_recv()
        for index, at, count in spans:
            centre[index, last : last + count, :] = got_north[at : at + count, :]
        unpack_west(corners[2][...], side, last, 0, LIP)

    @pl.when(jnp.logical_not(at_seam))
    def _():
        take_east()

    @pl.when(on_top & (lon <= half))
    def _():
        take_fold()

    assemble()
    east_half = lane8 < n_parts * GROUP
    strip_at = jnp.where(east_half, slot_lane - (own - LIP), slot_lane - LIP)
    closed = jnp.where(fold_late, 1, 0)
    strip_lanes = (strip_at >= 0) & (strip_at < LIP) & (
        jnp.where(east_half, lon, -1) < n_lon - 1
    )
    last_part = lax.rem(slot_of, n_parts) == n_parts - 1
    north_lanes = strip_lanes & (jnp.where(last_part, closed, 0) == 0)
    band_lanes = jnp.where(middle, closed, 1) == 0

    seam_regions = [
        (MARGIN, MARGIN + part_rows - LIP, strip_lanes),
        (MARGIN + part_rows - LIP, MARGIN + part_rows, north_lanes),
        (north_at + BAND - 2 * LIP, north_at + BAND - LIP, band_lanes),
        (south_at + LIP, south_at + 2 * LIP, middle),
    ]
    march(seam_rows, seam_weights, seam_basis, seam_regions, add_dot, flush, False)

    patch_rows = group_rows + 2 * MARGIN
    far_tile_rows = max(patch_rows, 2 * BAND)
    far_targets = (far.at[0], far_basis.at[0], far_basis.at[STEPS + 1])

    def march_far(regions):
        prepare(far_tile_rows, far, far_shifted, far_weights, far_basis)
        march(far_tile_rows, far_weights, far_basis, regions, add_dot, flush, False)

    @pl.when(past_seam)
    def _():
        arrival(7, deep_strip).wait_recv()
        for g in range(n_groups):
            unpack_deep(deep_strip[...], first + g * group_rows, g, group_rows)

        @pl.when(has_south)
        def _():
            arrival(8, deep_south).wait_recv()
            unpack_deep(deep_south[...], first - LIP, n_groups - 1, LIP)

        @pl.when(has_north)
        def _():
            arrival(9, deep_north).wait_recv()
            unpack_deep(deep_north[...], last, 0, LIP)

        span_lanes = GROUP - 2 * LIP
        for index, target in enumerate(far_targets):
            for at in range(0, patch_rows, 8):
                value = None
                for g in range(n_groups):
                    low = PAD + g * group_rows - MARGIN + at
                    mixed = turned(
                        jnp.where(
                            lane8 < span_lanes,
                            centre[index, low : low + 8, :],
                            side[index, low : low + 8, :],
                        ),
                        g * GROUP + 2 * LIP,
                    )
                    value = mixed if g == 0 else jnp.where(slot_of >= g, mixed, value)
                target[8 + at : 16 + at, :] = value
        patch_lanes = (slot_lane >= LIP) & (slot_lane < 2 * LIP)
        upper = jnp.where(slot_of == n_groups - 1, jnp.where(on_top, 1, 0), 0) == 0
        march_far([
            (MARGIN, MARGIN + group_rows - LIP, patch_lanes),
            (MARGIN + group_rows - LIP, MARGIN + group_rows, patch_lanes & upper),
        ])

    @pl.when(fold_early)
    def _():
        edge_row = BAND - LIP
        for target in (far_centre, far_side):
            for index in (0, 1, 2):
                for at in range(0, BAND, 8):
                    target[index, at : at + 8, :] = nothing
        arrival(10, got_far).wait_recv()
        home = lon + half
        low = edge_row - 2 * LIP
        unpack_west(far_edges[0][...], far_side, low, n_groups - 1, 2 * LIP)
        unpack_east(far_edges[1][...], far_side, low, n_groups - 1, 2 * LIP)
        mirror = folded(home)
        for index, at, count in spans:
            low = edge_row - count - LIP
            far_centre[index, low : low + LIP, :] = far_rows[index * LIP : (index + 1) * LIP, :]
            for r in range(count):
                far_centre[index, edge_row - 1 - r : edge_row - r, :] = fold_all[
                    home, at + r : at + r + 1, :
                ]
            for source, target in zip(mirror, (far_centre, far_side)):
                target[index, edge_row : edge_row + count, :] = source[at : at + count, :]
        for index, target in enumerate(far_targets):
            for at in range(0, BAND, 8):
                inside, outside = far_centre[index, at : at + 8, :], far_side[index, at : at + 8, :]
                target[8 + at : 16 + at, :] = inside
                spot = 8 + BAND + at
                target[spot : spot + 8, :] = jnp.where(
                    lane8 < GROUP,
                    turned(jnp.where(lane8 >= width - own, inside, outside), own - width),
                    turned(jnp.where(lane8 < own, inside, outside), GROUP + LIP),
                )
        edge_at = jnp.where(slot_of == 0, slot_lane - (own - LIP), slot_lane - LIP)
        edge_lanes = (slot_of < 2) & (edge_at >= 0) & (edge_at < LIP)
        fold_at = BAND - 2 * LIP
        march_far([
            (fold_at, fold_at + LIP, middle),
            (fold_at + BAND, fold_at + BAND + LIP, edge_lanes),
        ])

    def finish_late():
        @pl.when(at_seam | fold_late)
        def _():
            @pl.when(at_seam)
            def _():
                take_east()

            @pl.when(fold_late)
            def _():
                take_fold()

            assemble()
            march(seam_rows, seam_weights, seam_basis, seam_regions, None, None, False)

    number = len(order_of())
    pending = []
    lane = lax.broadcasted_iota(jnp.int32, (8, width), 1)
    home = lane - lax.broadcasted_iota(jnp.int32, (8, width), 0)
    message = jnp.zeros((8, width), jnp.float32)
    for g in range(number // 8):
        grouped = fold_sublanes([dots[8 * g + s] for s in range(8)])
        message = jnp.where(home == 8 * g, jnp.sum(grouped, axis=1, keepdims=True), message)
    message = jnp.sum(message, axis=0, keepdims=True)
    if direct:
        slots, send_sem, recv_sem = moment_refs
        me = lat * n_lon + lon
        slots[me] = message
        copies = [
            pltpu.make_async_remote_copy(
                src_ref=slots.at[me], dst_ref=slots.at[me], send_sem=send_sem,
                recv_sem=recv_sem,
                device_id=(lax.rem(lat + a, n_lat), lax.rem(lon + b, n_lon)),
                device_id_type=MESH,
            )
            for a, b in everyone
        ]
        rounds = ((slots, n_lat * n_lon, copies, send_sem, recv_sem),)
    else:
        slots_lat, slots_lon, lat_send, lat_recv, lon_send, lon_recv = moment_refs
        rounds = (
            (slots_lat, n_lat, None, lat_send, lat_recv, lat, True),
            (slots_lon, n_lon, None, lon_send, lon_recv, lon, False),
        )
    for slots, size, copies, send_sem, recv_sem, *rest in rounds:
        if copies is None:
            me, along_lat = rest
            slots[me] = message
            copies = spread(slots.at[me], slots.at[me], send_sem, recv_sem, along_lat)
        for copy in copies:
            copy.start()
        if not pending:
            finish_late()
        others = slots.at[0 : size - 1]
        whole = pltpu.make_async_remote_copy(
            src_ref=others, dst_ref=others, send_sem=send_sem, recv_sem=recv_sem,
            device_id=(lat, lon), device_id_type=MESH,
        )
        whole.wait_recv()
        terms = [slots[index] for index in range(size)]
        while len(terms) > 1:
            odd = terms[len(terms) // 2 * 2 :]
            terms = [x + y for x, y in zip(terms[0::2], terms[1::2])] + odd
        message = terms[0]
        pending.append(whole)
    message = jnp.broadcast_to(message, (8, width))
    for g in range(number // 8):
        picked = jnp.sum(jnp.where(home == 8 * g, message, 0.0), axis=1, keepdims=True)
        moment_rows[8 * g : 8 * g + 8, :] = jnp.broadcast_to(picked, (8, width))
    moments = {}
    for kind in (("p", "p"), ("p", "r"), ("r", "r")):
        series = []
        for index in range(17 if kind == ("p", "p") else 16 if kind == ("p", "r") else 15):
            spot = order_of()[kind + (index,)]
            value = jnp.broadcast_to(moment_rows[spot : spot + 1, :], (8, width))
            series.append(value if index < 2 else 2.0 * value - series[index % 2])
        moments[kind] = series
    height_coords, residual_coords = coordinates(moments)
    wanted = (height_coords, residual_coords)

    def combined(fields, at):
        totals = [None, None]
        for chain, power in sorted(height_coords | residual_coords):
            slot = power + (0 if chain == "p" else STEPS + 1)
            field = fields[slot, 8 + at : 16 + at, :]
            for which, coords in enumerate(wanted):
                if (chain, power) in coords:
                    term = coords[(chain, power)] * field
                    totals[which] = term if totals[which] is None else totals[which] + term
        return totals

    for at in range(0, seam_rows, 8):
        for which, total in enumerate(combined(seam_basis, at)):
            patch[which, at : at + 8, :] = total
    row8 = lax.broadcasted_iota(jnp.int32, (8, width), 0)
    for at in range(0, rows, 8):
        q = at // part_rows
        for which, total in enumerate(combined(wide_basis, at)):
            for low, high, source in (
                (0, LIP, south_at + LIP),
                (rows - LIP, rows, north_at + BAND - LIP - rows),
            ):
                if low < at + 8 and high > at:
                    edge = patch[which, source + at : source + at + 8, :]
                    if low <= at and high >= at + 8:
                        total = edge
                    else:
                        total = jnp.where((row8 >= low - at) & (row8 < high - at), edge, total)
            spot = at - q * part_rows + MARGIN
            strip = patch[which, spot : spot + 8, :]
            total = jnp.where(lane8 < LIP, turned(strip, -(n_parts + q) * GROUP - LIP), total)
            total = jnp.where(
                lane8 >= width - LIP, turned(strip, width - own - q * GROUP), total
            )
            (out_height, out_residual)[which][at : at + 8, :] = total

    for copy in pending:
        copy.wait_send()
    departure(2, got_sides).wait_send()
    for condition, index, block in (
        (has_north, 0, got_rows.at[0]),
        (has_south, 1, got_rows.at[1]),
        (on_top, 3, fold_all.at[0 : n_lon - 1, full]),
        (at_seam, 4, deep_packed),
        (at_seam & has_north, 5, deep_south),
        (at_seam & has_south, 6, deep_north),
        (fold_late, 7, far_rows),
        (gives_west_edge, 8, far_edges[0]),
        (gives_east_edge, 9, far_edges[1]),
    ):
        @pl.when(condition)
        def _():
            departure(index, block).wait_send()


@functools.cache
def order_of():
    keys = [("p", "p", k) for k in range(2 * STEPS + 1)]
    keys += [("p", "r", k) for k in range(2 * STEPS)]
    keys += [("r", "r", k) for k in range(2 * STEPS - 1)]
    return {key: index for index, key in enumerate(keys)}


def hand_over(height, residual, out_height, out_residual):
    out_height[...] = height[...]
    out_residual[...] = residual[...]


def per_device(n_lat, n_lon, forcing, search_direction, ocean_depth, land_mask, fold_map):
    rows, width = forcing.shape
    tall = rows + 2 * PAD
    f32 = jnp.float32
    n_parts = width // GROUP // 2
    seam_rows = rows // n_parts + 2 * MARGIN + 2 * BAND

    def tile(count):
        return [
            pltpu.VMEM((planes, count + 16, width), f32)
            for planes in (2, 4, 8, 2 * STEPS + 1)
        ]

    edge = pltpu.VMEM((32, width), f32)
    group_rows = rows * GROUP // width
    dma = pltpu.SemaphoreType.DMA
    if n_lat * n_lon <= DIRECT_LIMIT:
        moment_refs = [pltpu.VMEM((n_lat * n_lon, 1, width), f32), dma, dma]
    else:
        moment_refs = [pltpu.VMEM((size, 1, width), f32) for size in (n_lat, n_lon)] + [dma] * 4
    block = pl.BlockSpec(memory_space=pltpu.VMEM)
    outs = pl.pallas_call(
        functools.partial(kernel, n_lat, n_lon),
        out_shape=[pltpu.VMEM((rows, width), f32)] * 2,
        in_specs=[pl.BlockSpec(memory_space=pl.ANY)] * 5,
        out_specs=[block] * 2,
        scratch_shapes=[
            pltpu.VMEM((3, rows, width), f32), pltpu.VMEM((rows, width), jnp.int32),
            pltpu.SMEM(fold_map.shape, jnp.int32),
            pltpu.VMEM((3, tall, width), f32), pltpu.VMEM((3, tall, width), f32),
            *tile(rows),
            *tile(seam_rows),
            *tile(max(group_rows + 2 * MARGIN, 2 * BAND)),
            pltpu.VMEM((2, seam_rows, width), f32),
            edge, edge, edge,
            pltpu.VMEM((2, group_rows, width), f32),
            pltpu.VMEM((2, 3 * LIP + 2 * STEPS, width), f32),
            pltpu.VMEM((2, group_rows, width), f32),
            pltpu.VMEM((n_lon, 32, width), f32),
            pltpu.VMEM((group_rows, width), f32),
            pltpu.VMEM((group_rows + 2 * LIP, width), f32),
            pltpu.VMEM((3 * LIP, width), f32),
            pltpu.VMEM((7 * LIP, width), f32),
            pltpu.VMEM((3, BAND, width), f32), pltpu.VMEM((3, BAND, width), f32),
            pltpu.VMEM((6 * STEPS, 8, width), f32),
            pltpu.VMEM((6 * STEPS, width), f32),
            dma((3,)), dma((10,)), dma((11,)),
            *moment_refs,
        ],
        compiler_params=pltpu.CompilerParams(collective_id=0, has_side_effects=True),
        name="tripole_cg",
    )(forcing, search_direction, ocean_depth, land_mask, fold_map)
    return pl.pallas_call(
        hand_over,
        out_shape=[jax.ShapeDtypeStruct((rows, width), f32)] * 2,
        in_specs=[block] * 2,
        out_specs=[block] * 2,
        name="hand_over",
    )(*(pltpu.with_memory_space_constraint(out, pltpu.VMEM) for out in outs))


def solution(mesh):
    cells = P("lat", "lon")
    return jax.shard_map(
        functools.partial(per_device, mesh.shape["lat"], mesh.shape["lon"]),
        mesh=mesh,
        in_specs=(cells, cells, cells, cells, P()),
        out_specs=(cells, cells),
        check_vma=False,
    )
```

```python
import functools

import jax
import jax.numpy as jnp
from jax import lax
from jax.experimental import pallas as pl
from jax.experimental.pallas import tpu as pltpu
from jax.sharding import PartitionSpec as P

STEPS = 8
REACH = 256
MESH = pl.DeviceIdType.MESH
PAD = 16
GROUP = 32
CHUNK = 16
LIP = STEPS + 1
MARGIN = 12
SLAB = 40
BAND = 32
DIRECT_LIMIT = 64

DIRECTIONS = ((1, 0), (-1, 0), (0, 1), (0, -1), (1, 1), (-1, -1), (1, -1), (-1, 1))
SLOT = {offset: index for index, offset in enumerate(DIRECTIONS)}


def halves(offset):
    return 0.5 if 0 in offset else 0.25


def chunks_of(low, high, size):
    return [(at, min(size, high - at)) for at in range(low, high, size)]


def turned(x, shift):
    shift = shift % x.shape[1]
    return x if shift == 0 else pltpu.roll(x, shift, 1)


def plus(left, right):
    result = dict(left)
    for key, value in right.items():
        result[key] = result[key] + value if key in result else value
    return result


def scaled(factor, vector):
    return {key: factor * value for key, value in vector.items()}


def apply_shift(vector):
    result = {}
    for (chain, power), value in vector.items():
        parts = [((chain, power), value)]
        if power == 0:
            parts.append(((chain, 1), value))
        else:
            half = 0.5 * value
            parts += [((chain, power + 1), half), ((chain, power - 1), half)]
        result = plus(result, {}) if not parts else result
        for key, part in parts:
            result = plus(result, {key: part})
    return result


def tree_sum(terms):
    terms = list(terms)
    while len(terms) > 1:
        odd = terms[len(terms) // 2 * 2 :]
        terms = [x + y for x, y in zip(terms[0::2], terms[1::2])] + odd
    return terms[0]


def against(coords, series):
    return tree_sum(value * series[key] for key, value in sorted(coords.items()))


def shifted_series(series, chain, reach):
    result = {}
    for k in range(reach + 1):
        beside = (
            series[(chain, 1)]
            if k == 0
            else 0.5 * (series[(chain, k + 1)] + series[(chain, k - 1)])
        )
        result[(chain, k)] = series[(chain, k)] + beside
    return result


def coordinates(moments):
    one = jnp.ones_like(moments[("p", "p")][0])
    direction_coords, residual_coords = {("p", 0): one}, {("r", 0): one}
    direction = {("p", k): value for k, value in enumerate(moments[("p", "p")])}
    direction |= {("r", k): value for k, value in enumerate(moments[("p", "r")])}
    residual = {("p", k): value for k, value in enumerate(moments[("p", "r")])}
    residual |= {("r", k): value for k, value in enumerate(moments[("r", "r")])}
    solution_coords = {}
    norm_now = residual[("r", 0)]
    for step in range(STEPS):
        reach = 2 * STEPS - 2 - step
        mapped = shifted_series(direction, "p", reach) | shifted_series(direction, "r", reach - 1)
        mapped_coords = apply_shift(direction_coords)
        step_length = norm_now / against(direction_coords, mapped)
        solution_coords = plus(solution_coords, scaled(step_length, direction_coords))
        residual_coords = plus(residual_coords, scaled(-step_length, mapped_coords))
        if step == STEPS - 1:
            break
        residual = {key: residual[key] - step_length * value for key, value in mapped.items()}
        shrink = 1.0 / norm_now
        norm_now = against(residual_coords, residual)
        turn = norm_now * shrink
        direction = {key: value + turn * direction[key] for key, value in residual.items()}
        direction_coords = plus(residual_coords, scaled(turn, direction_coords))
    return solution_coords, residual_coords


def fold_sublanes(parts):
    row = lax.broadcasted_iota(jnp.int32, parts[0].shape, 0)
    parts = list(parts)
    span = 4
    while span:
        low = (row & span) == 0
        half = len(parts) // 2
        parts = [
            jnp.where(low, first, second)
            + pltpu.roll(jnp.where(low, second, first), span, 0)
            if span == 4
            else jnp.where(low, first, second)
            + jnp.where(low, pltpu.roll(first, 8 - span, 0), pltpu.roll(second, span, 0))
            for first, second in zip(parts[:half], parts[half:])
        ]
        span //= 2
    return parts[0]


def kept(at, count, regions):
    row = lax.broadcasted_iota(jnp.int32, (8, regions[0][2].shape[1]), 0)
    masks = []
    for r in range(at, at + count, 8):
        mask = None
        for low, high, lanes in regions:
            if low >= r + 8 or high <= r:
                continue
            part = lanes
            if low > r or high < r + 8:
                part = lanes & (row >= low - r) & (row < high - r)
            mask = part if mask is None else mask | part
        masks.append(mask)
    return masks


def prepare(rows, depth_root, shifted, weights, basis):
    width = depth_root.shape[2]
    zero = jnp.zeros((8, width), jnp.float32)
    for at in (0, 8 + rows):
        span = pl.ds(at, 8)
        depth_root[0, span, :] = zero
        depth_root[1, span, :] = zero
        for slot in range(2 * STEPS + 1):
            if slot not in (STEPS, 2 * STEPS):
                basis[slot, span, :] = zero

    depth, root = depth_root.at[0], depth_root.at[1]
    for at, count in chunks_of(0, rows + 16, CHUNK):
        span = pl.ds(at, count)
        shifted[0, span, :] = turned(depth[span, :], -1)
        shifted[1, span, :] = turned(depth[span, :], 1)
    shifted_depth = {0: depth, 1: shifted.at[0], -1: shifted.at[1]}
    for at, count in chunks_of(8, 8 + rows, CHUNK):
        here = depth[at : at + count, :]
        sums = {0.5: None, 0.25: None}
        for a, b in DIRECTIONS:
            beside = shifted_depth[b][at + a : at + a + count, :]
            link = jnp.where(beside > 0.0, here + beside, 0.0)
            factor = halves((a, b))
            sums[factor] = link if sums[factor] is None else sums[factor] + link
        diagonal = here * (1.0 / (REACH * REACH)) + (0.5 * sums[0.5] + 0.25 * sums[0.25])
        value = lax.rsqrt(jnp.where(here > 0.0, diagonal, 1.0))
        span = pl.ds(at, count)
        root[span, :] = value
        shifted[2, span, :] = turned(value, -1)
        shifted[3, span, :] = turned(value, 1)
    shifted_root = {0: root, 1: shifted.at[2], -1: shifted.at[3]}
    for at, count in chunks_of(8, 8 + rows, CHUNK):
        for b in (-1, 0, 1):
            goal_depth = shifted_depth[-b][at : at + count, :]
            goal_root = shifted_root[-b][at : at + count, :]
            for a in (-1, 0, 1):
                if (a, b) == (0, 0):
                    continue
                from_depth = depth[at + a : at + a + count, :]
                from_root = root[at + a : at + a + count, :]
                link = jnp.where(
                    jnp.minimum(goal_depth, from_depth) > 0.0, goal_depth + from_depth, 0.0
                )
                weights[SLOT[(a, b)], at : at + count, :] = (
                    goal_root * (-2.0 * halves((a, b)))
                ) * (link * from_root)


def needed(rows, regions, reach):
    tiles = sorted({
        at
        for low, high, _ in regions
        for at in range(max(low - reach, 0) // 8 * 8, min(high + reach, rows), 8)
    })
    runs = []
    for at in tiles:
        if runs and runs[-1][0] + runs[-1][1] == at and runs[-1][1] < CHUNK:
            runs[-1][1] += 8
        else:
            runs.append([at, 8])
    return [(8 + at, count) for at, count in runs]


def march(rows, weights, basis, regions, add_dot, flush, new):
    def keep(at, count):
        return kept(at, count, regions)

    def masked(masks, value):
        return [
            None if mask is None else jnp.where(mask, value[8 * i : 8 * i + 8, :], 0.0)
            for i, mask in enumerate(masks)
        ]

    def dot(key, left, right):
        for i, piece in enumerate(left):
            if piece is not None:
                add_dot(key, piece, right[8 * i : 8 * i + 8, :])

    for at, count in needed(rows, regions, 0) if add_dot else []:
        p0 = basis[0, at : at + count, :]
        r0 = basis[STEPS + 1, at : at + count, :]
        masks = keep(at - 8, count)
        p0_kept, r0_kept = masked(masks, p0), masked(masks, r0)
        dot(("p", "p", 0), p0_kept, p0)
        dot(("r", "r", 0), r0_kept, r0)
        dot(("p", "r", 0), p0_kept, r0)

    for power in range(1, STEPS + 1):
        chains = [("p", 0)] + ([("r", STEPS + 1)] if power < STEPS else [])
        for at, count in needed(rows, regions, STEPS - power):
            fresh = {}
            held = {}
            factors = {ab: weights[SLOT[ab], at : at + count, :] for ab in DIRECTIONS}
            for name, origin in chains:
                slot = origin + power
                taken = {a: basis[slot - 1, at + a : at + a + count, :] for a in (-1, 0, 1)}
                held[name] = taken[0]
                columns = {}
                for b in (-1, 0, 1):
                    total = None
                    for a in (-1, 0, 1):
                        if (a, b) == (0, 0):
                            continue
                        term = factors[(a, b)] * taken[a]
                        total = term if total is None else total + term
                    columns[b] = total
                value = columns[0] + turned(columns[1], -1) + turned(columns[-1], 1)
                if power == 1:
                    value = 0.5 * value
                else:
                    value = value - basis[slot - 2, at : at + count, :]
                basis[slot, at : at + count, :] = value
                fresh[name] = value
            if not add_dot:
                continue
            masks = keep(at - 8, count)
            fresh_kept = {name: masked(masks, fresh[name]) for name, _ in chains}
            for name, _ in chains:
                dot((name, name, 2 * power), fresh_kept[name], fresh[name])
                dot((name, name, 2 * power - 1), fresh_kept[name], held[name])
            if power < STEPS:
                dot(("p", "r", 2 * power), fresh_kept["p"], fresh["r"])
                dot(("p", "r", 2 * power - 1), fresh_kept["p"], held["r"])
            else:
                dot(
                    ("p", "r", 2 * power - 1),
                    fresh_kept["p"],
                    basis[STEPS + power, at : at + count, :],
                )
        if add_dot:
            flush(new)


def kernel(
    n_lat, n_lon, forcing_hbm, search_hbm, depth_hbm, mask_hbm, fold_hbm,
    wide_basis, seam_basis, sums_out, loaded, mask_in, fold_map,
    centre, side, wide, wide_shifted, wide_weights, seam, seam_shifted,
    seam_weights, far, far_shifted, far_weights, far_basis, row_north, row_south,
    fold_rows, packed, got_rows, got_sides, fold_all, deep_packed, got_deep, deep_rows, got_far,
    far_centre, far_side, dots, load_sem, near_send, near_recv, *moment_refs,
):
    rows, width = forcing_hbm.shape
    lat, lon = lax.axis_index("lat"), lax.axis_index("lon")
    top = n_lat - 1
    north, south = lax.rem(lat + 1, n_lat), lax.rem(lat + n_lat - 1, n_lat)
    east, west = lax.rem(lon + 1, n_lon), lax.rem(lon + n_lon - 1, n_lon)
    has_north, has_south = lat < top, lat > 0
    group_rows = rows * GROUP // width
    n_groups = width // GROUP

    barrier = pltpu.get_barrier_semaphore()

    def greet(place):
        pl.semaphore_signal(barrier, inc=1, device_id=place, device_id_type=MESH)

    for source, target, index in (
        (mask_hbm, mask_in, 0), (depth_hbm, loaded.at[0], 1), (search_hbm, loaded.at[1], 1),
        (forcing_hbm, loaded.at[2], 1), (fold_hbm, fold_map, 2),
    ):
        pltpu.make_async_copy(source, target, load_sem.at[index]).start()
    depth_in, search, forcing = loaded.at[0], loaded.at[1], loaded.at[2]
    direct = n_lat * n_lon <= DIRECT_LIMIT
    everyone = [(a, b) for a in range(n_lat) for b in range(n_lon) if a or b]
    everyone.sort(key=lambda d: (d[1] or n_lon, d[0] or n_lat))
    if direct:
        for a, b in everyone:
            greet((lax.rem(lat + a, n_lat), lax.rem(lon + b, n_lon)))
        greeted = len(everyone)
    else:
        for d in range(1, n_lat):
            greet((lax.rem(lat + d, n_lat), lon))
        for d in range(1, n_lon):
            greet((lat, lax.rem(lon + d, n_lon)))
        for place in ((north, east), (north, west), (south, east), (south, west)):
            greet(place)
        greeted = n_lat - 1 + n_lon - 1 + 4

    pltpu.make_async_copy(mask_hbm, mask_in, load_sem.at[0]).wait()
    pltpu.make_async_copy(loaded, loaded, load_sem.at[1]).wait()
    pltpu.make_async_copy(fold_hbm, fold_map, load_sem.at[2]).wait()
    lane_group = lax.broadcasted_iota(jnp.int32, (group_rows, width), 1)
    west_edge = east_edge = None
    for g in range(n_groups):
        here = pl.ds(g * group_rows, group_rows)
        there = pl.ds(PAD + g * group_rows, group_rows)
        flag = mask_in[here, :].astype(jnp.float32)
        deep = depth_in[here, :] * flag
        moving = search[here, :] * flag
        left = forcing[here, :] * flag
        for index, value in enumerate((deep, moving, left)):
            centre[index, there, :] = value
        inner = pl.ds(8 + g * group_rows, group_rows)
        wide[0, inner, :] = deep
        wide_basis[0, inner, :] = moving
        wide_basis[STEPS + 1, inner, :] = left
        inside = lane_group - g * GROUP
        to_west = jnp.where(
            inside < 9,
            turned(deep, g * GROUP),
            jnp.where(inside < 17, turned(moving, g * GROUP + 9), turned(left, g * GROUP + 17)),
        )
        to_east = jnp.where(
            inside < 9,
            turned(deep, g * GROUP + 9),
            jnp.where(inside < 17, turned(moving, g * GROUP + 17), turned(left, g * GROUP + 25)),
        )
        west_edge = to_west if g == 0 else jnp.where(inside >= 0, to_west, west_edge)
        east_edge = to_east if g == 0 else jnp.where(inside >= 0, to_east, east_edge)
    packed[0] = west_edge
    packed[1] = east_edge
    first, last = PAD, PAD + rows
    spans = ((0, 0, LIP), (1, LIP, STEPS), (2, LIP + STEPS, STEPS))
    depth_of = LIP + 2 * STEPS
    for index, at, count in spans:
        row_south[at : at + count, :] = centre[index, first : first + count, :]
        row_north[at : at + count, :] = centre[index, last - count : last, :]

    @pl.when(lat == top)
    def _():
        for index, at, count in spans:
            for r in range(count):
                fold_rows[at + r : at + r + 1, :] = centre[index, last - 1 - r : last - r, :]
        fold_all[lon, 0:depth_of, :] = fold_rows[0:depth_of, :]

    pl.semaphore_wait(barrier, greeted)

    half = n_lon // 2
    at_seam, past_seam = lon == n_lon - 1, lon == 0
    on_top = lat == top
    fold_late, fold_early = on_top & (lon > half), on_top & (lon >= 1) & (lon < half)

    def near(gone, arrived, source, target, place):
        return pltpu.make_async_remote_copy(
            src_ref=source, dst_ref=target, send_sem=near_send.at[gone],
            recv_sem=near_recv.at[arrived], device_id=place, device_id_type=MESH,
        )

    def arrival(index, block):
        return near(0, index, block, block, (lat, lon))

    def departure(index, block):
        return near(index, 0, block, block, (lat, lon))

    tail, head = pl.ds(group_rows - LIP, LIP), pl.ds(0, LIP)
    tall_tail = pl.ds(group_rows - 2 * LIP, 2 * LIP)
    full = pl.ds(0, depth_of)
    near_rows = pl.ds(0, depth_of + LIP)
    got_south, got_north = got_rows.at[0, full], got_rows.at[1, full]
    got_west, got_east = got_sides.at[0], got_sides.at[1]
    corners = [got_rows.at[index // 2, pl.ds(depth_of + LIP * (index % 2), LIP)] for index in range(4)]
    deep_strip = got_deep.at[0:group_rows]
    deep_south = got_deep.at[group_rows : group_rows + LIP]
    deep_north = got_deep.at[group_rows + LIP : group_rows + 2 * LIP]
    far_rows = got_far.at[0 : 3 * LIP]
    far_edges = [got_far.at[at : at + 2 * LIP] for at in (3 * LIP, 5 * LIP)]
    northward = (
        near(0, 0, row_north.at[full], got_south, (north, lon)),
        near(0, 0, packed.at[1, tail], corners[0], (north, east)),
        near(0, 4, packed.at[0, tail], corners[1], (north, west)),
    )
    southward = (
        near(1, 1, row_south.at[full], got_north, (south, lon)),
        near(1, 1, packed.at[1, head], corners[2], (south, east)),
        near(1, 5, packed.at[0, head], corners[3], (south, west)),
    )
    to_east = near(2, 2, packed.at[1], got_west, (lat, east))
    to_west = near(2, 3, packed.at[0], got_east, (lat, west))
    deep_east = near(4, 7, deep_packed, deep_strip, (lat, east))
    deep_up = near(5, 8, deep_packed.at[tail], deep_south, (north, east))
    deep_down = near(6, 9, deep_packed.at[head], deep_north, (south, east))

    def across_half(step):
        return (lat, lax.rem(lon + step + n_lon, n_lon))

    far_away = near(7, 10, deep_rows, far_rows, across_half(-half))
    far_west_edge = near(8, 10, packed.at[1, tall_tail], far_edges[0], across_half(1 - half))
    far_east_edge = near(9, 10, packed.at[0, tall_tail], far_edges[1], across_half(-1 - half))
    gives_west_edge = on_top & (lon >= half) & (lon < n_lon - 1)
    gives_east_edge = on_top & ((lon > half + 1) | (lon == 0))

    def spread(source, slot, send_sem, recv_sem, along_lat):
        size = n_lat if along_lat else n_lon
        me = lat if along_lat else lon
        copies = []
        for d in range(1, size):
            peer = lax.rem(me + d, size)
            copies.append(
                pltpu.make_async_remote_copy(
                    src_ref=source, dst_ref=slot, send_sem=send_sem,
                    recv_sem=recv_sem,
                    device_id=(peer, lon) if along_lat else (lat, peer),
                    device_id_type=MESH,
                )
            )
        return copies

    across = spread(
        fold_rows.at[full], fold_all.at[lon, full], near_send.at[3], near_recv.at[6], False
    )

    to_west.start()
    to_east.start()

    @pl.when(has_north)
    def _():
        for copy in northward:
            copy.start()

    @pl.when(has_south)
    def _():
        for copy in southward:
            copy.start()

    @pl.when(at_seam)
    def _():
        for g in range(n_groups):
            here = pl.ds(PAD + g * group_rows, group_rows)
            inside = lane_group - g * GROUP
            value = jnp.where(
                inside < LIP,
                turned(centre[0, here, :], g * GROUP + 2 * LIP),
                jnp.where(
                    inside < 2 * LIP,
                    turned(centre[1, here, :], g * GROUP + 3 * LIP - 1),
                    turned(centre[2, here, :], g * GROUP + 4 * LIP - 1),
                ),
            )
            if g:
                value = jnp.where(inside >= 0, value, deep_packed[...])
            deep_packed[...] = value
        deep_east.start()

        @pl.when(has_north)
        def _():
            deep_up.start()

        @pl.when(has_south)
        def _():
            deep_down.start()

    @pl.when(on_top)
    def _():
        for index, top_row in enumerate((LIP, STEPS, STEPS)):
            low = last - top_row - LIP
            deep_rows[index * LIP : (index + 1) * LIP, :] = centre[index, low : low + LIP, :]
        for copy in reversed(across):
            copy.start()

    for condition, copy in (
        (fold_late, far_away),
        (gives_west_edge, far_west_edge),
        (gives_east_edge, far_east_edge),
    ):
        @pl.when(condition)
        def _():
            copy.start()

    dot_sums = {}

    def add_dot(key, left, right):
        product = left * right
        for r in range(0, product.shape[0], 8):
            piece = product[r : r + 8, :]
            dot_sums[key] = piece if key not in dot_sums else dot_sums[key] + piece

    def flush(new):
        for key in list(dot_sums):
            total = dot_sums.pop(key)
            spot = order_of()[key]
            dots[spot] = total if new else dots[spot] + total

    lane8 = lax.broadcasted_iota(jnp.int32, (8, width), 1)
    nothing = jnp.zeros((8, width), jnp.float32)

    prepare(rows, wide, wide_shifted, wide_weights, wide_basis)
    middle = (lane8 >= LIP) & (lane8 < width - LIP)

    march(
        rows, wide_weights, wide_basis, [(LIP, rows - LIP, middle)], add_dot, flush, True
    )

    part_spans = ((0, 0, LIP), (1, LIP, STEPS), (2, LIP + STEPS, STEPS))

    def unpack_west(got, target, start, g, count):
        lane = lax.broadcasted_iota(jnp.int32, (count, width), 1)
        for index, offset, cells in part_spans:
            value = turned(got, -g * GROUP - offset - cells)
            target[index, start : start + count, :] = jnp.where(lane >= width - cells, value, 0.0)

    def unpack_east(got, target, start, g, count):
        lane = lax.broadcasted_iota(jnp.int32, (count, width), 1)
        for index, offset, cells in part_spans:
            value = turned(got, -g * GROUP - offset)
            target[index, start : start + count, :] = jnp.where(
                lane < cells, value, target[index, start : start + count, :]
            )

    def unpack_deep(got, start, g, count):
        lane = lax.broadcasted_iota(jnp.int32, (count, width), 1)
        for index, cells in ((0, LIP), (1, STEPS), (2, STEPS)):
            low = width - cells - LIP
            value = turned(got, low - g * GROUP - index * LIP)
            side[index, start : start + count, :] = jnp.where(
                (lane >= low) & (lane < low + LIP), value, side[index, start : start + count, :]
            )

    for index in (0, 1, 2):
        for at in (0, 8, last, last + 8):
            centre[index, at : at + 8, :] = nothing
            side[index, at : at + 8, :] = nothing

    def take_east():
        arrival(3, got_east).wait_recv()
        for g in range(n_groups):
            unpack_east(got_east[...], side, first + g * group_rows, g, group_rows)

        @pl.when(has_south)
        def _():
            arrival(4, corners[1]).wait_recv()
            unpack_east(corners[1][...], side, first - LIP, n_groups - 1, LIP)

        @pl.when(has_north)
        def _():
            arrival(5, corners[3]).wait_recv()
            unpack_east(corners[3][...], side, last, 0, LIP)

    def folded(home):
        total = n_lon * width
        pivot = lax.rem(fold_map[0] - home * width + total, total)
        block, offset = pivot // width, lax.rem(pivot, width)
        lane = lax.broadcasted_iota(jnp.int32, (32, width), 1)
        index = lax.rem(offset - lane + width, width)

        def mirrored(which):
            rows_of = fold_all[lax.rem(block + which + n_lon, n_lon)]
            return jnp.take_along_axis(rows_of, index, axis=1, mode="promise_in_bounds")

        ahead, same, behind, beyond = (mirrored(which) for which in (1, 0, -1, -2))
        close = lane <= offset
        value = jnp.where(close, same, behind)
        halo = jnp.where(
            lane < width // 2, jnp.where(close, behind, beyond), jnp.where(close, ahead, same)
        )
        return value, halo

    def take_fold():
        arrival(6, fold_all.at[0 : n_lon - 1, full]).wait_recv()
        for source, target in zip(folded(lon), (centre, side)):
            for index, at, count in spans:
                target[index, last : last + count, :] = source[at : at + count, :]

    n_parts = width // GROUP // 2
    part_rows = rows // n_parts
    strip_rows = part_rows + 2 * MARGIN
    seam_rows = strip_rows + 2 * BAND
    north_at, south_at = strip_rows, strip_rows + BAND
    own = GROUP - LIP
    slot_of = lane8 // GROUP
    slot_lane = lane8 - slot_of * GROUP

    def assemble():
        targets = (seam.at[0], seam_basis.at[0], seam_basis.at[STEPS + 1])
        for index, target in enumerate(targets):
            for at in range(0, strip_rows, 8):
                value = None
                for q in range(n_parts):
                    low = PAD + q * part_rows - MARGIN + at
                    inside, outside = centre[index, low : low + 8, :], side[index, low : low + 8, :]
                    east_slot = turned(
                        jnp.where(lane8 >= width - own, inside, outside),
                        q * GROUP - (width - own),
                    )
                    west_slot = turned(
                        jnp.where(lane8 < own, inside, outside), (n_parts + q) * GROUP + LIP
                    )
                    mixed = jnp.where(lane8 < n_parts * GROUP, east_slot, west_slot)
                    value = mixed if q == 0 else jnp.where(
                        lax.rem(slot_of, n_parts) >= q, mixed, value
                    )
                target[8 + at : 16 + at, :] = value
            for at in range(0, BAND, 8):
                low = last + LIP - BAND + at
                target[8 + north_at + at : 16 + north_at + at, :] = centre[index, low : low + 8, :]
                low = first - LIP + at
                target[8 + south_at + at : 16 + south_at + at, :] = centre[index, low : low + 8, :]
        prepare(seam_rows, seam, seam_shifted, seam_weights, seam_basis)

    arrival(2, got_west).wait_recv()
    for g in range(n_groups):
        unpack_west(got_west[...], side, first + g * group_rows, g, group_rows)

    @pl.when(has_south)
    def _():
        arrival(0, got_rows.at[0, near_rows]).wait_recv()
        for index, at, count in spans:
            centre[index, first - count : first, :] = got_south[at : at + count, :]
        unpack_west(corners[0][...], side, first - LIP, n_groups - 1, LIP)

    @pl.when(has_north)
    def _():
        arrival(1, got_rows.at[1, near_rows]).wait_recv()
        for index, at, count in spans:
            centre[index, last : last + count, :] = got_north[at : at + count, :]
        unpack_west(corners[2][...], side, last, 0, LIP)

    @pl.when(jnp.logical_not(at_seam))
    def _():
        take_east()

    @pl.when(on_top & (lon <= half))
    def _():
        take_fold()

    assemble()
    east_half = lane8 < n_parts * GROUP
    strip_at = jnp.where(east_half, slot_lane - (own - LIP), slot_lane - LIP)
    closed = jnp.where(fold_late, 1, 0)
    strip_lanes = (strip_at >= 0) & (strip_at < LIP) & (
        jnp.where(east_half, lon, -1) < n_lon - 1
    )
    last_part = lax.rem(slot_of, n_parts) == n_parts - 1
    north_lanes = strip_lanes & (jnp.where(last_part, closed, 0) == 0)
    band_lanes = jnp.where(middle, closed, 1) == 0

    seam_regions = [
        (MARGIN, MARGIN + part_rows - LIP, strip_lanes),
        (MARGIN + part_rows - LIP, MARGIN + part_rows, north_lanes),
        (north_at + BAND - 2 * LIP, north_at + BAND - LIP, band_lanes),
        (south_at + LIP, south_at + 2 * LIP, middle),
    ]
    march(seam_rows, seam_weights, seam_basis, seam_regions, add_dot, flush, False)

    patch_rows = group_rows + 2 * MARGIN
    far_tile_rows = max(patch_rows, 2 * BAND)
    far_targets = (far.at[0], far_basis.at[0], far_basis.at[STEPS + 1])

    def march_far(regions):
        prepare(far_tile_rows, far, far_shifted, far_weights, far_basis)
        march(far_tile_rows, far_weights, far_basis, regions, add_dot, flush, False)

    @pl.when(past_seam)
    def _():
        arrival(7, deep_strip).wait_recv()
        for g in range(n_groups):
            unpack_deep(deep_strip[...], first + g * group_rows, g, group_rows)

        @pl.when(has_south)
        def _():
            arrival(8, deep_south).wait_recv()
            unpack_deep(deep_south[...], first - LIP, n_groups - 1, LIP)

        @pl.when(has_north)
        def _():
            arrival(9, deep_north).wait_recv()
            unpack_deep(deep_north[...], last, 0, LIP)

        span_lanes = GROUP - 2 * LIP
        for index, target in enumerate(far_targets):
            for at in range(0, patch_rows, 8):
                value = None
                for g in range(n_groups):
                    low = PAD + g * group_rows - MARGIN + at
                    mixed = turned(
                        jnp.where(
                            lane8 < span_lanes,
                            centre[index, low : low + 8, :],
                            side[index, low : low + 8, :],
                        ),
                        g * GROUP + 2 * LIP,
                    )
                    value = mixed if g == 0 else jnp.where(slot_of >= g, mixed, value)
                target[8 + at : 16 + at, :] = value
        patch_lanes = (slot_lane >= LIP) & (slot_lane < 2 * LIP)
        upper = jnp.where(slot_of == n_groups - 1, jnp.where(on_top, 1, 0), 0) == 0
        march_far([
            (MARGIN, MARGIN + group_rows - LIP, patch_lanes),
            (MARGIN + group_rows - LIP, MARGIN + group_rows, patch_lanes & upper),
        ])

    @pl.when(fold_early)
    def _():
        edge_row = BAND - LIP
        for target in (far_centre, far_side):
            for index in (0, 1, 2):
                for at in range(0, BAND, 8):
                    target[index, at : at + 8, :] = nothing
        arrival(10, got_far).wait_recv()
        home = lon + half
        low = edge_row - 2 * LIP
        unpack_west(far_edges[0][...], far_side, low, n_groups - 1, 2 * LIP)
        unpack_east(far_edges[1][...], far_side, low, n_groups - 1, 2 * LIP)
        mirror = folded(home)
        for index, at, count in spans:
            low = edge_row - count - LIP
            far_centre[index, low : low + LIP, :] = far_rows[index * LIP : (index + 1) * LIP, :]
            for r in range(count):
                far_centre[index, edge_row - 1 - r : edge_row - r, :] = fold_all[
                    home, at + r : at + r + 1, :
                ]
            for source, target in zip(mirror, (far_centre, far_side)):
                target[index, edge_row : edge_row + count, :] = source[at : at + count, :]
        for index, target in enumerate(far_targets):
            for at in range(0, BAND, 8):
                inside, outside = far_centre[index, at : at + 8, :], far_side[index, at : at + 8, :]
                target[8 + at : 16 + at, :] = inside
                spot = 8 + BAND + at
                target[spot : spot + 8, :] = jnp.where(
                    lane8 < GROUP,
                    turned(jnp.where(lane8 >= width - own, inside, outside), own - width),
                    turned(jnp.where(lane8 < own, inside, outside), GROUP + LIP),
                )
        edge_at = jnp.where(slot_of == 0, slot_lane - (own - LIP), slot_lane - LIP)
        edge_lanes = (slot_of < 2) & (edge_at >= 0) & (edge_at < LIP)
        fold_at = BAND - 2 * LIP
        march_far([
            (fold_at, fold_at + LIP, middle),
            (fold_at + BAND, fold_at + BAND + LIP, edge_lanes),
        ])

    def finish_late():
        @pl.when(at_seam | fold_late)
        def _():
            @pl.when(at_seam)
            def _():
                take_east()

            @pl.when(fold_late)
            def _():
                take_fold()

            assemble()
            march(seam_rows, seam_weights, seam_basis, seam_regions, None, None, False)

    number = len(order_of())
    pending = []
    lane = lax.broadcasted_iota(jnp.int32, (8, width), 1)
    home = lane - lax.broadcasted_iota(jnp.int32, (8, width), 0)
    message = jnp.zeros((8, width), jnp.float32)
    for g in range(number // 8):
        grouped = fold_sublanes([dots[8 * g + s] for s in range(8)])
        message = jnp.where(home == 8 * g, jnp.sum(grouped, axis=1, keepdims=True), message)
    message = jnp.sum(message, axis=0, keepdims=True)
    if direct:
        slots, send_sem, recv_sem = moment_refs
        me = lat * n_lon + lon
        slots[me] = message
        copies = [
            pltpu.make_async_remote_copy(
                src_ref=slots.at[me], dst_ref=slots.at[me], send_sem=send_sem,
                recv_sem=recv_sem,
                device_id=(lax.rem(lat + a, n_lat), lax.rem(lon + b, n_lon)),
                device_id_type=MESH,
            )
            for a, b in everyone
        ]
        rounds = ((slots, n_lat * n_lon, copies, send_sem, recv_sem),)
    else:
        slots_lat, slots_lon, lat_send, lat_recv, lon_send, lon_recv = moment_refs
        rounds = (
            (slots_lat, n_lat, None, lat_send, lat_recv, lat, True),
            (slots_lon, n_lon, None, lon_send, lon_recv, lon, False),
        )
    for slots, size, copies, send_sem, recv_sem, *rest in rounds:
        if copies is None:
            me, along_lat = rest
            slots[me] = message
            copies = spread(slots.at[me], slots.at[me], send_sem, recv_sem, along_lat)
        for copy in copies:
            copy.start()
        if not pending:
            finish_late()
        others = slots.at[0 : size - 1]
        whole = pltpu.make_async_remote_copy(
            src_ref=others, dst_ref=others, send_sem=send_sem, recv_sem=recv_sem,
            device_id=(lat, lon), device_id_type=MESH,
        )
        whole.wait_recv()
        terms = [slots[index] for index in range(size)]
        while len(terms) > 1:
            odd = terms[len(terms) // 2 * 2 :]
            terms = [x + y for x, y in zip(terms[0::2], terms[1::2])] + odd
        message = terms[0]
        pending.append(whole)
    sums_out[...] = jnp.broadcast_to(message, (8, width))
    for copy in pending:
        copy.wait_send()
    departure(2, got_sides).wait_send()
    for condition, index, block in (
        (has_north, 0, got_rows.at[0]),
        (has_south, 1, got_rows.at[1]),
        (on_top, 3, fold_all.at[0 : n_lon - 1, full]),
        (at_seam, 4, deep_packed),
        (at_seam & has_north, 5, deep_south),
        (at_seam & has_south, 6, deep_north),
        (fold_late, 7, far_rows),
        (gives_west_edge, 8, far_edges[0]),
        (gives_east_edge, 9, far_edges[1]),
    ):
        @pl.when(condition)
        def _():
            departure(index, block).wait_send()


@functools.cache
def order_of():
    keys = [("p", "p", k) for k in range(2 * STEPS + 1)]
    keys += [("p", "r", k) for k in range(2 * STEPS)]
    keys += [("r", "r", k) for k in range(2 * STEPS - 1)]
    return {key: index for index, key in enumerate(keys)}


def finish(
    sums, wide_basis, seam_basis, out_height, out_residual, moment_rows, patch, results, out_sem
):
    rows, width = out_height.shape
    number = len(order_of())
    n_parts = width // GROUP // 2
    part_rows = rows // n_parts
    north_at = part_rows + 2 * MARGIN
    south_at = north_at + BAND
    seam_rows = south_at + BAND
    own = GROUP - LIP
    lane8 = lax.broadcasted_iota(jnp.int32, (8, width), 1)
    home = lane8 - lax.broadcasted_iota(jnp.int32, (8, width), 0)
    message = sums[...]
    for g in range(number // 8):
        picked = jnp.sum(jnp.where(home == 8 * g, message, 0.0), axis=1, keepdims=True)
        moment_rows[8 * g : 8 * g + 8, :] = jnp.broadcast_to(picked, (8, width))
    moments = {}
    for kind in (("p", "p"), ("p", "r"), ("r", "r")):
        series = []
        for index in range(17 if kind == ("p", "p") else 16 if kind == ("p", "r") else 15):
            spot = order_of()[kind + (index,)]
            value = jnp.broadcast_to(moment_rows[spot : spot + 1, :], (8, width))
            series.append(value if index < 2 else 2.0 * value - series[index % 2])
        moments[kind] = series
    height_coords, residual_coords = coordinates(moments)
    outs = (out_height, out_residual)
    wanted = (height_coords, residual_coords)

    def combined(fields, at):
        totals = [None, None]
        for chain, power in sorted(height_coords | residual_coords):
            slot = power + (0 if chain == "p" else STEPS + 1)
            field = fields[slot, 8 + at : 16 + at, :]
            for which, coords in enumerate(wanted):
                if (chain, power) in coords:
                    term = coords[(chain, power)] * field
                    totals[which] = term if totals[which] is None else totals[which] + term
        return totals

    for at in range(0, seam_rows, 8):
        for which, total in enumerate(combined(seam_basis, at)):
            patch[which, at : at + 8, :] = total
    row8 = lax.broadcasted_iota(jnp.int32, (8, width), 0)
    for at in range(0, rows, 8):
        q = at // part_rows
        for which, total in enumerate(combined(wide_basis, at)):
            for low, high, source in (
                (0, LIP, south_at + LIP),
                (rows - LIP, rows, north_at + BAND - LIP - rows),
            ):
                if low < at + 8 and high > at:
                    edge = patch[which, source + at : source + at + 8, :]
                    if low <= at and high >= at + 8:
                        total = edge
                    else:
                        total = jnp.where((row8 >= low - at) & (row8 < high - at), edge, total)
            spot = at - q * part_rows + MARGIN
            strip = patch[which, spot : spot + 8, :]
            total = jnp.where(lane8 < LIP, turned(strip, -(n_parts + q) * GROUP - LIP), total)
            total = jnp.where(
                lane8 >= width - LIP, turned(strip, width - own - q * GROUP), total
            )
            results[which, at : at + 8, :] = total
        if (at + 8) % SLAB == 0 or at + 8 == rows:
            low = at // SLAB * SLAB
            span = slice(low, at + 8)
            for which, out in enumerate(outs):
                pltpu.make_async_copy(
                    results.at[which, span], out.at[span], out_sem.at[which]
                ).start()
    for which, out in enumerate(outs):
        pltpu.make_async_copy(results.at[which], out, out_sem.at[which]).wait()


def per_device(n_lat, n_lon, forcing, search_direction, ocean_depth, land_mask, fold_map):
    rows, width = forcing.shape
    tall = rows + 2 * PAD
    f32 = jnp.float32
    n_parts = width // GROUP // 2
    seam_rows = rows // n_parts + 2 * MARGIN + 2 * BAND

    def tile(count):
        return [
            pltpu.VMEM((planes, count + 16, width), f32)
            for planes in (2, 4, 8, 2 * STEPS + 1)
        ]

    edge = pltpu.VMEM((32, width), f32)
    group_rows = rows * GROUP // width
    dma = pltpu.SemaphoreType.DMA
    if n_lat * n_lon <= DIRECT_LIMIT:
        moment_refs = [pltpu.VMEM((n_lat * n_lon, 1, width), f32), dma, dma]
    else:
        moment_refs = [pltpu.VMEM((size, 1, width), f32) for size in (n_lat, n_lon)] + [dma] * 4
    block = pl.BlockSpec(memory_space=pltpu.VMEM)
    outs = pl.pallas_call(
        functools.partial(kernel, n_lat, n_lon),
        out_shape=[
            tile(rows)[-1], tile(seam_rows)[-1], pltpu.VMEM((8, width), f32)
        ],
        in_specs=[pl.BlockSpec(memory_space=pl.ANY)] * 5,
        out_specs=[block] * 3,
        scratch_shapes=[
            pltpu.VMEM((3, rows, width), f32), pltpu.VMEM((rows, width), jnp.int32),
            pltpu.SMEM(fold_map.shape, jnp.int32),
            pltpu.VMEM((3, tall, width), f32), pltpu.VMEM((3, tall, width), f32),
            *tile(rows)[:-1],
            *tile(seam_rows)[:-1],
            *tile(max(group_rows + 2 * MARGIN, 2 * BAND)),
            edge, edge, edge,
            pltpu.VMEM((2, group_rows, width), f32),
            pltpu.VMEM((2, 3 * LIP + 2 * STEPS, width), f32),
            pltpu.VMEM((2, group_rows, width), f32),
            pltpu.VMEM((n_lon, 32, width), f32),
            pltpu.VMEM((group_rows, width), f32),
            pltpu.VMEM((group_rows + 2 * LIP, width), f32),
            pltpu.VMEM((3 * LIP, width), f32),
            pltpu.VMEM((7 * LIP, width), f32),
            pltpu.VMEM((3, BAND, width), f32), pltpu.VMEM((3, BAND, width), f32),
            pltpu.VMEM((6 * STEPS, 8, width), f32),
            dma((3,)), dma((10,)), dma((11,)),
            *moment_refs,
        ],
        compiler_params=pltpu.CompilerParams(collective_id=0, has_side_effects=True),
        name="tripole_cg",
    )(forcing, search_direction, ocean_depth, land_mask, fold_map)
    wide_basis, seam_basis, sums = (
        pltpu.with_memory_space_constraint(out, pltpu.VMEM) for out in outs
    )
    return pl.pallas_call(
        finish,
        out_shape=[jax.ShapeDtypeStruct((rows, width), f32)] * 2,
        in_specs=[block] * 3,
        out_specs=[pl.BlockSpec(memory_space=pl.ANY)] * 2,
        scratch_shapes=[
            pltpu.VMEM((6 * STEPS, width), f32),
            pltpu.VMEM((2, seam_rows, width), f32),
            pltpu.VMEM((2, rows, width), f32),
            dma((2,)),
        ],
        name="finish",
    )(sums, wide_basis, seam_basis)


def solution(mesh):
    cells = P("lat", "lon")
    return jax.shard_map(
        functools.partial(per_device, mesh.shape["lat"], mesh.shape["lon"]),
        mesh=mesh,
        in_specs=(cells, cells, cells, cells, P()),
        out_specs=(cells, cells),
        check_vma=False,
    )
```

```python
import functools

import jax
import jax.numpy as jnp
from jax import lax
from jax.experimental import pallas as pl
from jax.experimental.pallas import tpu as pltpu
from jax.sharding import PartitionSpec as P

STEPS = 8
REACH = 256
MESH = pl.DeviceIdType.MESH
PAD = 16
GROUP = 32
CHUNK = 16
LIP = STEPS + 1
MARGIN = 12
SLAB = 40
BAND = 32
DIRECT_LIMIT = 64

DIRECTIONS = ((1, 0), (-1, 0), (0, 1), (0, -1), (1, 1), (-1, -1), (1, -1), (-1, 1))
SLOT = {offset: index for index, offset in enumerate(DIRECTIONS)}


def halves(offset):
    return 0.5 if 0 in offset else 0.25


def chunks_of(low, high, size):
    return [(at, min(size, high - at)) for at in range(low, high, size)]


def turned(x, shift):
    shift = shift % x.shape[1]
    return x if shift == 0 else pltpu.roll(x, shift, 1)


def plus(left, right):
    result = dict(left)
    for key, value in right.items():
        result[key] = result[key] + value if key in result else value
    return result


def scaled(factor, vector):
    return {key: factor * value for key, value in vector.items()}


def apply_shift(vector):
    result = {}
    for (chain, power), value in vector.items():
        parts = [((chain, power), value)]
        if power == 0:
            parts.append(((chain, 1), value))
        else:
            half = 0.5 * value
            parts += [((chain, power + 1), half), ((chain, power - 1), half)]
        result = plus(result, {}) if not parts else result
        for key, part in parts:
            result = plus(result, {key: part})
    return result


def tree_sum(terms):
    terms = list(terms)
    while len(terms) > 1:
        odd = terms[len(terms) // 2 * 2 :]
        terms = [x + y for x, y in zip(terms[0::2], terms[1::2])] + odd
    return terms[0]


def against(coords, series):
    return tree_sum(value * series[key] for key, value in sorted(coords.items()))


def shifted_series(series, chain, reach):
    result = {}
    for k in range(reach + 1):
        beside = (
            series[(chain, 1)]
            if k == 0
            else 0.5 * (series[(chain, k + 1)] + series[(chain, k - 1)])
        )
        result[(chain, k)] = series[(chain, k)] + beside
    return result


def coordinates(moments):
    one = jnp.ones_like(moments[("p", "p")][0])
    direction_coords, residual_coords = {("p", 0): one}, {("r", 0): one}
    direction = {("p", k): value for k, value in enumerate(moments[("p", "p")])}
    direction |= {("r", k): value for k, value in enumerate(moments[("p", "r")])}
    residual = {("p", k): value for k, value in enumerate(moments[("p", "r")])}
    residual |= {("r", k): value for k, value in enumerate(moments[("r", "r")])}
    solution_coords = {}
    norm_now = residual[("r", 0)]
    for step in range(STEPS):
        reach = 2 * STEPS - 2 - step
        mapped = shifted_series(direction, "p", reach) | shifted_series(direction, "r", reach - 1)
        mapped_coords = apply_shift(direction_coords)
        step_length = norm_now / against(direction_coords, mapped)
        solution_coords = plus(solution_coords, scaled(step_length, direction_coords))
        residual_coords = plus(residual_coords, scaled(-step_length, mapped_coords))
        if step == STEPS - 1:
            break
        residual = {key: residual[key] - step_length * value for key, value in mapped.items()}
        shrink = 1.0 / norm_now
        norm_now = against(residual_coords, residual)
        turn = norm_now * shrink
        direction = {key: value + turn * direction[key] for key, value in residual.items()}
        direction_coords = plus(residual_coords, scaled(turn, direction_coords))
    return solution_coords, residual_coords


def fold_sublanes(parts):
    row = lax.broadcasted_iota(jnp.int32, parts[0].shape, 0)
    parts = list(parts)
    span = 4
    while span:
        low = (row & span) == 0
        half = len(parts) // 2
        parts = [
            jnp.where(low, first, second)
            + pltpu.roll(jnp.where(low, second, first), span, 0)
            if span == 4
            else jnp.where(low, first, second)
            + jnp.where(low, pltpu.roll(first, 8 - span, 0), pltpu.roll(second, span, 0))
            for first, second in zip(parts[:half], parts[half:])
        ]
        span //= 2
    return parts[0]


def kept(at, count, regions):
    row = lax.broadcasted_iota(jnp.int32, (8, regions[0][2].shape[1]), 0)
    masks = []
    for r in range(at, at + count, 8):
        mask = None
        for low, high, lanes in regions:
            if low >= r + 8 or high <= r:
                continue
            part = lanes
            if low > r or high < r + 8:
                part = lanes & (row >= low - r) & (row < high - r)
            mask = part if mask is None else mask | part
        masks.append(mask)
    return masks


def gathered(around):
    beside = around[-1] + around[1]
    edge = around[0] + 0.5 * beside
    return beside + (turned(edge, -1) + turned(edge, 1))


def rows_near(ref, at, count):
    return {a: ref[at + a : at + a + count, :] for a in (-1, 0, 1)}


def clear(rows, planes, deep, basis):
    width = planes.shape[2]
    zero = jnp.zeros((8, width), jnp.float32)
    for at in (0, 8 + rows):
        planes[0, at : at + 8, :] = zero
    for at in range(0, rows + 16, 8):
        for slot in range(4):
            deep[slot, at : at + 8, :] = zero
        for slot in range(2 * STEPS + 1):
            basis[slot, at : at + 8, :] = zero


def prepare(rows, planes, deep, basis, regions):
    depth = planes.at[0]
    for at, count in chunks_of(8, 8 + rows, CHUNK):
        span = pl.ds(at, count)
        around = rows_near(depth, at, count)
        here = around[0]
        is_wet = here > 0.0
        wet = {a: jnp.where(value > 0.0, 1.0, 0.0) for a, value in around.items()}
        links = 0.5 * (here * gathered(wet) + gathered(around))
        diagonal = jnp.where(is_wet, here * (1.0 / (REACH * REACH)) + links, 1.0)
        root = lax.rsqrt(diagonal)
        planes[3, span, :] = turned(here, 1)
        planes[4, span, :] = turned(here, -1)
        planes[1, span, :] = jnp.where(is_wet, -(root * root), 0.0)
        basis[2 * STEPS + 1, span, :] = diagonal * root
        for i, mask in enumerate(kept(at - 8, count, regions)):
            if mask is not None:
                planes[2, at + 8 * i : at + 8 * i + 8, :] = jnp.where(
                    mask, diagonal[8 * i : 8 * i + 8, :], 0.0
                )
        for chain, slot in enumerate((0, STEPS + 1)):
            value = root * basis[slot, span, :]
            basis[slot, span, :] = value
            deep[chain, span, :] = here * value


def needed(rows, regions, reach):
    tiles = sorted({
        at
        for low, high, _ in regions
        for at in range(max(low - reach, 0) // 8 * 8, min(high + reach, rows), 8)
    })
    runs = []
    for at in tiles:
        if runs and runs[-1][0] + runs[-1][1] == at and runs[-1][1] < CHUNK:
            runs[-1][1] += 8
        else:
            runs.append([at, 8])
    return [(8 + at, count) for at, count in runs]


def march(rows, planes, deep, basis, regions, add_dot, flush, new):
    def weighted(at, masks, value):
        return [
            None
            if mask is None
            else planes[2, at + 8 * i : at + 8 * i + 8, :] * value[8 * i : 8 * i + 8, :]
            for i, mask in enumerate(masks)
        ]

    def dot(key, left, right):
        for i, piece in enumerate(left):
            if piece is not None:
                add_dot(key, piece, right[8 * i : 8 * i + 8, :])

    for at, count in needed(rows, regions, 0) if add_dot else []:
        p0 = basis[0, at : at + count, :]
        r0 = basis[STEPS + 1, at : at + count, :]
        masks = kept(at - 8, count, regions)
        p0_kept, r0_kept = weighted(at, masks, p0), weighted(at, masks, r0)
        dot(("p", "p", 0), p0_kept, p0)
        dot(("r", "r", 0), r0_kept, r0)
        dot(("p", "r", 0), p0_kept, r0)

    for power in range(1, STEPS + 1):
        chains = [("p", 0)] + ([("r", STEPS + 1)] if power < STEPS else [])
        for at, count in needed(rows, regions, STEPS - power):
            fresh = {}
            held = {}
            depth, factor, west_depth, east_depth = (
                planes[plane, at : at + count, :] for plane in (0, 1, 3, 4)
            )
            for chain, (name, origin) in enumerate(chains):
                slot = origin + power
                before, after = (power + 1) % 2 * 2 + chain, power % 2 * 2 + chain
                taken = rows_near(basis.at[slot - 1], at, count)
                held[name] = taken[0]
                heavy = rows_near(deep.at[before], at, count)
                beside, beside_heavy = taken[-1] + taken[1], heavy[-1] + heavy[1]
                edge = taken[0] + 0.5 * beside
                edge_heavy = heavy[0] + 0.5 * beside_heavy
                sums = (depth * beside + beside_heavy) + (
                    turned(west_depth * edge + edge_heavy, -1)
                    + turned(east_depth * edge + edge_heavy, 1)
                )
                if power == 1:
                    value = (0.5 * factor) * sums
                else:
                    value = factor * sums - basis[slot - 2, at : at + count, :]
                basis[slot, at : at + count, :] = value
                if power < STEPS:
                    deep[after, at : at + count, :] = depth * value
                fresh[name] = value
            if not add_dot:
                continue
            masks = kept(at - 8, count, regions)
            fresh_kept = {name: weighted(at, masks, fresh[name]) for name, _ in chains}
            for name, _ in chains:
                dot((name, name, 2 * power), fresh_kept[name], fresh[name])
                dot((name, name, 2 * power - 1), fresh_kept[name], held[name])
            if power < STEPS:
                dot(("p", "r", 2 * power), fresh_kept["p"], fresh["r"])
                dot(("p", "r", 2 * power - 1), fresh_kept["p"], held["r"])
            else:
                dot(
                    ("p", "r", 2 * power - 1),
                    fresh_kept["p"],
                    basis[STEPS + power, at : at + count, :],
                )
        if add_dot:
            flush(new)


def kernel(
    n_lat, n_lon, forcing_hbm, search_hbm, depth_hbm, mask_hbm, fold_hbm,
    wide_basis, seam_basis, sums_out, loaded, mask_in, fold_map,
    centre, side, wide, wide_deep, seam, seam_deep, far, far_deep, far_basis, row_north, row_south,
    fold_rows, packed, got_rows, got_sides, fold_all, deep_packed, got_deep, deep_rows, got_far,
    far_centre, far_side, dots, load_sem, near_send, near_recv, *moment_refs,
):
    rows, width = forcing_hbm.shape
    lat, lon = lax.axis_index("lat"), lax.axis_index("lon")
    top = n_lat - 1
    north, south = lax.rem(lat + 1, n_lat), lax.rem(lat + n_lat - 1, n_lat)
    east, west = lax.rem(lon + 1, n_lon), lax.rem(lon + n_lon - 1, n_lon)
    has_north, has_south = lat < top, lat > 0
    group_rows = rows * GROUP // width
    n_groups = width // GROUP

    barrier = pltpu.get_barrier_semaphore()

    def greet(place):
        pl.semaphore_signal(barrier, inc=1, device_id=place, device_id_type=MESH)

    for source, target, index in (
        (mask_hbm, mask_in, 0), (depth_hbm, loaded.at[0], 1), (search_hbm, loaded.at[1], 1),
        (forcing_hbm, loaded.at[2], 1), (fold_hbm, fold_map, 2),
    ):
        pltpu.make_async_copy(source, target, load_sem.at[index]).start()
    depth_in, search, forcing = loaded.at[0], loaded.at[1], loaded.at[2]
    direct = n_lat * n_lon <= DIRECT_LIMIT
    everyone = [(a, b) for a in range(n_lat) for b in range(n_lon) if a or b]
    everyone.sort(key=lambda d: (d[1] or n_lon, d[0] or n_lat))
    if direct:
        for a, b in everyone:
            greet((lax.rem(lat + a, n_lat), lax.rem(lon + b, n_lon)))
        greeted = len(everyone)
    else:
        for d in range(1, n_lat):
            greet((lax.rem(lat + d, n_lat), lon))
        for d in range(1, n_lon):
            greet((lat, lax.rem(lon + d, n_lon)))
        for place in ((north, east), (north, west), (south, east), (south, west)):
            greet(place)
        greeted = n_lat - 1 + n_lon - 1 + 4

    n_parts = width // GROUP // 2
    part_rows = rows // n_parts
    strip_rows = part_rows + 2 * MARGIN
    seam_rows = strip_rows + 2 * BAND
    patch_rows = group_rows + 2 * MARGIN
    far_tile_rows = max(patch_rows, 2 * BAND)
    clear(rows, wide, wide_deep, wide_basis)
    clear(seam_rows, seam, seam_deep, seam_basis)
    clear(far_tile_rows, far, far_deep, far_basis)
    pltpu.make_async_copy(mask_hbm, mask_in, load_sem.at[0]).wait()
    pltpu.make_async_copy(loaded, loaded, load_sem.at[1]).wait()
    pltpu.make_async_copy(fold_hbm, fold_map, load_sem.at[2]).wait()
    lane_group = lax.broadcasted_iota(jnp.int32, (group_rows, width), 1)
    west_edge = east_edge = None
    for g in range(n_groups):
        here = pl.ds(g * group_rows, group_rows)
        there = pl.ds(PAD + g * group_rows, group_rows)
        flag = mask_in[here, :].astype(jnp.float32)
        deep = depth_in[here, :] * flag
        moving = search[here, :] * flag
        left = forcing[here, :] * flag
        for index, value in enumerate((deep, moving, left)):
            centre[index, there, :] = value
        inner = pl.ds(8 + g * group_rows, group_rows)
        wide[0, inner, :] = deep
        wide_basis[0, inner, :] = moving
        wide_basis[STEPS + 1, inner, :] = left
        inside = lane_group - g * GROUP
        to_west = jnp.where(
            inside < 9,
            turned(deep, g * GROUP),
            jnp.where(inside < 17, turned(moving, g * GROUP + 9), turned(left, g * GROUP + 17)),
        )
        to_east = jnp.where(
            inside < 9,
            turned(deep, g * GROUP + 9),
            jnp.where(inside < 17, turned(moving, g * GROUP + 17), turned(left, g * GROUP + 25)),
        )
        west_edge = to_west if g == 0 else jnp.where(inside >= 0, to_west, west_edge)
        east_edge = to_east if g == 0 else jnp.where(inside >= 0, to_east, east_edge)
    packed[0] = west_edge
    packed[1] = east_edge
    first, last = PAD, PAD + rows
    spans = ((0, 0, LIP), (1, LIP, STEPS), (2, LIP + STEPS, STEPS))
    depth_of = LIP + 2 * STEPS
    for index, at, count in spans:
        row_south[at : at + count, :] = centre[index, first : first + count, :]
        row_north[at : at + count, :] = centre[index, last - count : last, :]

    @pl.when(lat == top)
    def _():
        for index, at, count in spans:
            for r in range(count):
                fold_rows[at + r : at + r + 1, :] = centre[index, last - 1 - r : last - r, :]
        fold_all[lon, 0:depth_of, :] = fold_rows[0:depth_of, :]

    pl.semaphore_wait(barrier, greeted)

    half = n_lon // 2
    at_seam, past_seam = lon == n_lon - 1, lon == 0
    on_top = lat == top
    fold_late, fold_early = on_top & (lon > half), on_top & (lon >= 1) & (lon < half)

    def near(gone, arrived, source, target, place):
        return pltpu.make_async_remote_copy(
            src_ref=source, dst_ref=target, send_sem=near_send.at[gone],
            recv_sem=near_recv.at[arrived], device_id=place, device_id_type=MESH,
        )

    def arrival(index, block):
        return near(0, index, block, block, (lat, lon))

    def departure(index, block):
        return near(index, 0, block, block, (lat, lon))

    tail, head = pl.ds(group_rows - LIP, LIP), pl.ds(0, LIP)
    tall_tail = pl.ds(group_rows - 2 * LIP, 2 * LIP)
    full = pl.ds(0, depth_of)
    near_rows = pl.ds(0, depth_of + LIP)
    got_south, got_north = got_rows.at[0, full], got_rows.at[1, full]
    got_west, got_east = got_sides.at[0], got_sides.at[1]
    corners = [got_rows.at[index // 2, pl.ds(depth_of + LIP * (index % 2), LIP)] for index in range(4)]
    deep_strip = got_deep.at[0:group_rows]
    deep_south = got_deep.at[group_rows : group_rows + LIP]
    deep_north = got_deep.at[group_rows + LIP : group_rows + 2 * LIP]
    far_rows = got_far.at[0 : 3 * LIP]
    far_edges = [got_far.at[at : at + 2 * LIP] for at in (3 * LIP, 5 * LIP)]
    northward = (
        near(0, 0, row_north.at[full], got_south, (north, lon)),
        near(0, 0, packed.at[1, tail], corners[0], (north, east)),
        near(0, 4, packed.at[0, tail], corners[1], (north, west)),
    )
    southward = (
        near(1, 1, row_south.at[full], got_north, (south, lon)),
        near(1, 1, packed.at[1, head], corners[2], (south, east)),
        near(1, 5, packed.at[0, head], corners[3], (south, west)),
    )
    to_east = near(2, 2, packed.at[1], got_west, (lat, east))
    to_west = near(2, 3, packed.at[0], got_east, (lat, west))
    deep_east = near(4, 7, deep_packed, deep_strip, (lat, east))
    deep_up = near(5, 8, deep_packed.at[tail], deep_south, (north, east))
    deep_down = near(6, 9, deep_packed.at[head], deep_north, (south, east))

    def across_half(step):
        return (lat, lax.rem(lon + step + n_lon, n_lon))

    far_away = near(7, 10, deep_rows, far_rows, across_half(-half))
    far_west_edge = near(8, 10, packed.at[1, tall_tail], far_edges[0], across_half(1 - half))
    far_east_edge = near(9, 10, packed.at[0, tall_tail], far_edges[1], across_half(-1 - half))
    gives_west_edge = on_top & (lon >= half) & (lon < n_lon - 1)
    gives_east_edge = on_top & ((lon > half + 1) | (lon == 0))

    def spread(source, slot, send_sem, recv_sem, along_lat):
        size = n_lat if along_lat else n_lon
        me = lat if along_lat else lon
        copies = []
        for d in range(1, size):
            peer = lax.rem(me + d, size)
            copies.append(
                pltpu.make_async_remote_copy(
                    src_ref=source, dst_ref=slot, send_sem=send_sem,
                    recv_sem=recv_sem,
                    device_id=(peer, lon) if along_lat else (lat, peer),
                    device_id_type=MESH,
                )
            )
        return copies

    across = spread(
        fold_rows.at[full], fold_all.at[lon, full], near_send.at[3], near_recv.at[6], False
    )

    to_west.start()
    to_east.start()

    @pl.when(has_north)
    def _():
        for copy in northward:
            copy.start()

    @pl.when(has_south)
    def _():
        for copy in southward:
            copy.start()

    @pl.when(at_seam)
    def _():
        for g in range(n_groups):
            here = pl.ds(PAD + g * group_rows, group_rows)
            inside = lane_group - g * GROUP
            value = jnp.where(
                inside < LIP,
                turned(centre[0, here, :], g * GROUP + 2 * LIP),
                jnp.where(
                    inside < 2 * LIP,
                    turned(centre[1, here, :], g * GROUP + 3 * LIP - 1),
                    turned(centre[2, here, :], g * GROUP + 4 * LIP - 1),
                ),
            )
            if g:
                value = jnp.where(inside >= 0, value, deep_packed[...])
            deep_packed[...] = value
        deep_east.start()

        @pl.when(has_north)
        def _():
            deep_up.start()

        @pl.when(has_south)
        def _():
            deep_down.start()

    @pl.when(on_top)
    def _():
        for index, top_row in enumerate((LIP, STEPS, STEPS)):
            low = last - top_row - LIP
            deep_rows[index * LIP : (index + 1) * LIP, :] = centre[index, low : low + LIP, :]
        for copy in reversed(across):
            copy.start()

    for condition, copy in (
        (fold_late, far_away),
        (gives_west_edge, far_west_edge),
        (gives_east_edge, far_east_edge),
    ):
        @pl.when(condition)
        def _():
            copy.start()

    dot_sums = {}

    def add_dot(key, left, right):
        product = left * right
        for r in range(0, product.shape[0], 8):
            piece = product[r : r + 8, :]
            dot_sums[key] = piece if key not in dot_sums else dot_sums[key] + piece

    def flush(new):
        for key in list(dot_sums):
            total = dot_sums.pop(key)
            spot = order_of()[key]
            dots[spot] = total if new else dots[spot] + total

    lane8 = lax.broadcasted_iota(jnp.int32, (8, width), 1)
    nothing = jnp.zeros((8, width), jnp.float32)

    middle = (lane8 >= LIP) & (lane8 < width - LIP)

    wide_regions = [(LIP, rows - LIP, middle)]
    prepare(rows, wide, wide_deep, wide_basis, wide_regions)
    march(rows, wide, wide_deep, wide_basis, wide_regions, add_dot, flush, True)

    part_spans = ((0, 0, LIP), (1, LIP, STEPS), (2, LIP + STEPS, STEPS))

    def unpack_west(got, target, start, g, count):
        lane = lax.broadcasted_iota(jnp.int32, (count, width), 1)
        for index, offset, cells in part_spans:
            value = turned(got, -g * GROUP - offset - cells)
            target[index, start : start + count, :] = jnp.where(lane >= width - cells, value, 0.0)

    def unpack_east(got, target, start, g, count):
        lane = lax.broadcasted_iota(jnp.int32, (count, width), 1)
        for index, offset, cells in part_spans:
            value = turned(got, -g * GROUP - offset)
            target[index, start : start + count, :] = jnp.where(
                lane < cells, value, target[index, start : start + count, :]
            )

    def unpack_deep(got, start, g, count):
        lane = lax.broadcasted_iota(jnp.int32, (count, width), 1)
        for index, cells in ((0, LIP), (1, STEPS), (2, STEPS)):
            low = width - cells - LIP
            value = turned(got, low - g * GROUP - index * LIP)
            side[index, start : start + count, :] = jnp.where(
                (lane >= low) & (lane < low + LIP), value, side[index, start : start + count, :]
            )

    for index in (0, 1, 2):
        for at in (0, 8, last, last + 8):
            centre[index, at : at + 8, :] = nothing
            side[index, at : at + 8, :] = nothing

    def take_east():
        arrival(3, got_east).wait_recv()
        for g in range(n_groups):
            unpack_east(got_east[...], side, first + g * group_rows, g, group_rows)

        @pl.when(has_south)
        def _():
            arrival(4, corners[1]).wait_recv()
            unpack_east(corners[1][...], side, first - LIP, n_groups - 1, LIP)

        @pl.when(has_north)
        def _():
            arrival(5, corners[3]).wait_recv()
            unpack_east(corners[3][...], side, last, 0, LIP)

    def folded(home):
        total = n_lon * width
        pivot = lax.rem(fold_map[0] - home * width + total, total)
        block, offset = pivot // width, lax.rem(pivot, width)
        lane = lax.broadcasted_iota(jnp.int32, (32, width), 1)
        index = lax.rem(offset - lane + width, width)

        def mirrored(which):
            rows_of = fold_all[lax.rem(block + which + n_lon, n_lon)]
            return jnp.take_along_axis(rows_of, index, axis=1, mode="promise_in_bounds")

        ahead, same, behind, beyond = (mirrored(which) for which in (1, 0, -1, -2))
        close = lane <= offset
        value = jnp.where(close, same, behind)
        halo = jnp.where(
            lane < width // 2, jnp.where(close, behind, beyond), jnp.where(close, ahead, same)
        )
        return value, halo

    def take_fold():
        arrival(6, fold_all.at[0 : n_lon - 1, full]).wait_recv()
        for source, target in zip(folded(lon), (centre, side)):
            for index, at, count in spans:
                target[index, last : last + count, :] = source[at : at + count, :]

    north_at, south_at = strip_rows, strip_rows + BAND
    own = GROUP - LIP
    slot_of = lane8 // GROUP
    slot_lane = lane8 - slot_of * GROUP

    east_half = lane8 < n_parts * GROUP
    strip_at = jnp.where(east_half, slot_lane - (own - LIP), slot_lane - LIP)
    closed = jnp.where(fold_late, 1, 0)
    strip_lanes = (strip_at >= 0) & (strip_at < LIP) & (
        jnp.where(east_half, lon, -1) < n_lon - 1
    )
    last_part = lax.rem(slot_of, n_parts) == n_parts - 1
    north_lanes = strip_lanes & (jnp.where(last_part, closed, 0) == 0)
    band_lanes = jnp.where(middle, closed, 1) == 0

    seam_regions = [
        (MARGIN, MARGIN + part_rows - LIP, strip_lanes),
        (MARGIN + part_rows - LIP, MARGIN + part_rows, north_lanes),
        (north_at + BAND - 2 * LIP, north_at + BAND - LIP, band_lanes),
        (south_at + LIP, south_at + 2 * LIP, middle),
    ]
    def assemble():
        targets = (seam.at[0], seam_basis.at[0], seam_basis.at[STEPS + 1])
        for index, target in enumerate(targets):
            for at in range(0, strip_rows, 8):
                value = None
                for q in range(n_parts):
                    low = PAD + q * part_rows - MARGIN + at
                    inside, outside = centre[index, low : low + 8, :], side[index, low : low + 8, :]
                    east_slot = turned(
                        jnp.where(lane8 >= width - own, inside, outside),
                        q * GROUP - (width - own),
                    )
                    west_slot = turned(
                        jnp.where(lane8 < own, inside, outside), (n_parts + q) * GROUP + LIP
                    )
                    mixed = jnp.where(lane8 < n_parts * GROUP, east_slot, west_slot)
                    value = mixed if q == 0 else jnp.where(
                        lax.rem(slot_of, n_parts) >= q, mixed, value
                    )
                target[8 + at : 16 + at, :] = value
            for at in range(0, BAND, 8):
                low = last + LIP - BAND + at
                target[8 + north_at + at : 16 + north_at + at, :] = centre[index, low : low + 8, :]
                low = first - LIP + at
                target[8 + south_at + at : 16 + south_at + at, :] = centre[index, low : low + 8, :]
        prepare(seam_rows, seam, seam_deep, seam_basis, seam_regions)

    arrival(2, got_west).wait_recv()
    for g in range(n_groups):
        unpack_west(got_west[...], side, first + g * group_rows, g, group_rows)

    @pl.when(has_south)
    def _():
        arrival(0, got_rows.at[0, near_rows]).wait_recv()
        for index, at, count in spans:
            centre[index, first - count : first, :] = got_south[at : at + count, :]
        unpack_west(corners[0][...], side, first - LIP, n_groups - 1, LIP)

    @pl.when(has_north)
    def _():
        arrival(1, got_rows.at[1, near_rows]).wait_recv()
        for index, at, count in spans:
            centre[index, last : last + count, :] = got_north[at : at + count, :]
        unpack_west(corners[2][...], side, last, 0, LIP)

    @pl.when(jnp.logical_not(at_seam))
    def _():
        take_east()

    @pl.when(on_top & (lon <= half))
    def _():
        take_fold()

    assemble()
    march(seam_rows, seam, seam_deep, seam_basis, seam_regions, add_dot, flush, False)

    far_targets = (far.at[0], far_basis.at[0], far_basis.at[STEPS + 1])

    def march_far(regions):
        prepare(far_tile_rows, far, far_deep, far_basis, regions)
        march(far_tile_rows, far, far_deep, far_basis, regions, add_dot, flush, False)

    @pl.when(past_seam)
    def _():
        arrival(7, deep_strip).wait_recv()
        for g in range(n_groups):
            unpack_deep(deep_strip[...], first + g * group_rows, g, group_rows)

        @pl.when(has_south)
        def _():
            arrival(8, deep_south).wait_recv()
            unpack_deep(deep_south[...], first - LIP, n_groups - 1, LIP)

        @pl.when(has_north)
        def _():
            arrival(9, deep_north).wait_recv()
            unpack_deep(deep_north[...], last, 0, LIP)

        span_lanes = GROUP - 2 * LIP
        for index, target in enumerate(far_targets):
            for at in range(0, patch_rows, 8):
                value = None
                for g in range(n_groups):
                    low = PAD + g * group_rows - MARGIN + at
                    mixed = turned(
                        jnp.where(
                            lane8 < span_lanes,
                            centre[index, low : low + 8, :],
                            side[index, low : low + 8, :],
                        ),
                        g * GROUP + 2 * LIP,
                    )
                    value = mixed if g == 0 else jnp.where(slot_of >= g, mixed, value)
                target[8 + at : 16 + at, :] = value
        patch_lanes = (slot_lane >= LIP) & (slot_lane < 2 * LIP)
        upper = jnp.where(slot_of == n_groups - 1, jnp.where(on_top, 1, 0), 0) == 0
        march_far([
            (MARGIN, MARGIN + group_rows - LIP, patch_lanes),
            (MARGIN + group_rows - LIP, MARGIN + group_rows, patch_lanes & upper),
        ])

    @pl.when(fold_early)
    def _():
        edge_row = BAND - LIP
        for target in (far_centre, far_side):
            for index in (0, 1, 2):
                for at in range(0, BAND, 8):
                    target[index, at : at + 8, :] = nothing
        arrival(10, got_far).wait_recv()
        home = lon + half
        low = edge_row - 2 * LIP
        unpack_west(far_edges[0][...], far_side, low, n_groups - 1, 2 * LIP)
        unpack_east(far_edges[1][...], far_side, low, n_groups - 1, 2 * LIP)
        mirror = folded(home)
        for index, at, count in spans:
            low = edge_row - count - LIP
            far_centre[index, low : low + LIP, :] = far_rows[index * LIP : (index + 1) * LIP, :]
            for r in range(count):
                far_centre[index, edge_row - 1 - r : edge_row - r, :] = fold_all[
                    home, at + r : at + r + 1, :
                ]
            for source, target in zip(mirror, (far_centre, far_side)):
                target[index, edge_row : edge_row + count, :] = source[at : at + count, :]
        for index, target in enumerate(far_targets):
            for at in range(0, BAND, 8):
                inside, outside = far_centre[index, at : at + 8, :], far_side[index, at : at + 8, :]
                target[8 + at : 16 + at, :] = inside
                spot = 8 + BAND + at
                target[spot : spot + 8, :] = jnp.where(
                    lane8 < GROUP,
                    turned(jnp.where(lane8 >= width - own, inside, outside), own - width),
                    turned(jnp.where(lane8 < own, inside, outside), GROUP + LIP),
                )
        edge_at = jnp.where(slot_of == 0, slot_lane - (own - LIP), slot_lane - LIP)
        edge_lanes = (slot_of < 2) & (edge_at >= 0) & (edge_at < LIP)
        fold_at = BAND - 2 * LIP
        march_far([
            (fold_at, fold_at + LIP, middle),
            (fold_at + BAND, fold_at + BAND + LIP, edge_lanes),
        ])

    def finish_late():
        @pl.when(at_seam | fold_late)
        def _():
            @pl.when(at_seam)
            def _():
                take_east()

            @pl.when(fold_late)
            def _():
                take_fold()

            assemble()
            march(seam_rows, seam, seam_deep, seam_basis, seam_regions, None, None, False)

    number = len(order_of())
    pending = []
    lane = lax.broadcasted_iota(jnp.int32, (8, width), 1)
    home = lane - lax.broadcasted_iota(jnp.int32, (8, width), 0)
    message = jnp.zeros((8, width), jnp.float32)
    for g in range(number // 8):
        grouped = fold_sublanes([dots[8 * g + s] for s in range(8)])
        message = jnp.where(home == 8 * g, jnp.sum(grouped, axis=1, keepdims=True), message)
    message = jnp.sum(message, axis=0, keepdims=True)
    if direct:
        slots, send_sem, recv_sem = moment_refs
        me = lat * n_lon + lon
        slots[me] = message
        copies = [
            pltpu.make_async_remote_copy(
                src_ref=slots.at[me], dst_ref=slots.at[me], send_sem=send_sem,
                recv_sem=recv_sem,
                device_id=(lax.rem(lat + a, n_lat), lax.rem(lon + b, n_lon)),
                device_id_type=MESH,
            )
            for a, b in everyone
        ]
        rounds = ((slots, n_lat * n_lon, copies, send_sem, recv_sem),)
    else:
        slots_lat, slots_lon, lat_send, lat_recv, lon_send, lon_recv = moment_refs
        rounds = (
            (slots_lat, n_lat, None, lat_send, lat_recv, lat, True),
            (slots_lon, n_lon, None, lon_send, lon_recv, lon, False),
        )
    for slots, size, copies, send_sem, recv_sem, *rest in rounds:
        if copies is None:
            me, along_lat = rest
            slots[me] = message
            copies = spread(slots.at[me], slots.at[me], send_sem, recv_sem, along_lat)
        for copy in copies:
            copy.start()
        if not pending:
            finish_late()
        others = slots.at[0 : size - 1]
        whole = pltpu.make_async_remote_copy(
            src_ref=others, dst_ref=others, send_sem=send_sem, recv_sem=recv_sem,
            device_id=(lat, lon), device_id_type=MESH,
        )
        whole.wait_recv()
        terms = [slots[index] for index in range(size)]
        while len(terms) > 1:
            odd = terms[len(terms) // 2 * 2 :]
            terms = [x + y for x, y in zip(terms[0::2], terms[1::2])] + odd
        message = terms[0]
        pending.append(whole)
    sums_out[...] = jnp.broadcast_to(message, (8, width))
    for copy in pending:
        copy.wait_send()
    departure(2, got_sides).wait_send()
    for condition, index, block in (
        (has_north, 0, got_rows.at[0]),
        (has_south, 1, got_rows.at[1]),
        (on_top, 3, fold_all.at[0 : n_lon - 1, full]),
        (at_seam, 4, deep_packed),
        (at_seam & has_north, 5, deep_south),
        (at_seam & has_south, 6, deep_north),
        (fold_late, 7, far_rows),
        (gives_west_edge, 8, far_edges[0]),
        (gives_east_edge, 9, far_edges[1]),
    ):
        @pl.when(condition)
        def _():
            departure(index, block).wait_send()


@functools.cache
def order_of():
    keys = [("p", "p", k) for k in range(2 * STEPS + 1)]
    keys += [("p", "r", k) for k in range(2 * STEPS)]
    keys += [("r", "r", k) for k in range(2 * STEPS - 1)]
    return {key: index for index, key in enumerate(keys)}


def finish(
    sums, wide_basis, seam_basis, out_height, out_residual, moment_rows, patch, results, out_sem
):
    rows, width = out_height.shape
    number = len(order_of())
    n_parts = width // GROUP // 2
    part_rows = rows // n_parts
    north_at = part_rows + 2 * MARGIN
    south_at = north_at + BAND
    seam_rows = south_at + BAND
    own = GROUP - LIP
    lane8 = lax.broadcasted_iota(jnp.int32, (8, width), 1)
    home = lane8 - lax.broadcasted_iota(jnp.int32, (8, width), 0)
    message = sums[...]
    for g in range(number // 8):
        picked = jnp.sum(jnp.where(home == 8 * g, message, 0.0), axis=1, keepdims=True)
        moment_rows[8 * g : 8 * g + 8, :] = jnp.broadcast_to(picked, (8, width))
    moments = {}
    for kind in (("p", "p"), ("p", "r"), ("r", "r")):
        series = []
        for index in range(17 if kind == ("p", "p") else 16 if kind == ("p", "r") else 15):
            spot = order_of()[kind + (index,)]
            value = jnp.broadcast_to(moment_rows[spot : spot + 1, :], (8, width))
            series.append(value if index < 2 else 2.0 * value - series[index % 2])
        moments[kind] = series
    height_coords, residual_coords = coordinates(moments)
    outs = (out_height, out_residual)
    wanted = (height_coords, residual_coords)

    def combined(fields, at):
        totals = [None, None]
        for chain, power in sorted(height_coords | residual_coords):
            slot = power + (0 if chain == "p" else STEPS + 1)
            field = fields[slot, 8 + at : 16 + at, :]
            for which, coords in enumerate(wanted):
                if (chain, power) in coords:
                    term = coords[(chain, power)] * field
                    totals[which] = term if totals[which] is None else totals[which] + term
        stretch = fields[2 * STEPS + 1, 8 + at : 16 + at, :]
        return [stretch * total for total in totals]

    kept_rows = ((MARGIN, part_rows), (north_at + BAND - 2 * LIP, LIP), (south_at + LIP, LIP))
    for start, count in needed(seam_rows, [(low, low + size, None) for low, size in kept_rows], 0):
        for at in range(start - 8, start - 8 + count, 8):
            for which, total in enumerate(combined(seam_basis, at)):
                patch[which, at : at + 8, :] = total
    row8 = lax.broadcasted_iota(jnp.int32, (8, width), 0)
    for at in range(0, rows, 8):
        q = at // part_rows
        for which, total in enumerate(combined(wide_basis, at)):
            for low, high, source in (
                (0, LIP, south_at + LIP),
                (rows - LIP, rows, north_at + BAND - LIP - rows),
            ):
                if low < at + 8 and high > at:
                    edge = patch[which, source + at : source + at + 8, :]
                    if low <= at and high >= at + 8:
                        total = edge
                    else:
                        total = jnp.where((row8 >= low - at) & (row8 < high - at), edge, total)
            spot = at - q * part_rows + MARGIN
            strip = patch[which, spot : spot + 8, :]
            total = jnp.where(lane8 < LIP, turned(strip, -(n_parts + q) * GROUP - LIP), total)
            total = jnp.where(
                lane8 >= width - LIP, turned(strip, width - own - q * GROUP), total
            )
            results[which, at : at + 8, :] = total
        if (at + 8) % SLAB == 0 or at + 8 == rows:
            low = at // SLAB * SLAB
            span = slice(low, at + 8)
            for which, out in enumerate(outs):
                pltpu.make_async_copy(
                    results.at[which, span], out.at[span], out_sem.at[which]
                ).start()
    for which, out in enumerate(outs):
        pltpu.make_async_copy(results.at[which], out, out_sem.at[which]).wait()


def per_device(n_lat, n_lon, forcing, search_direction, ocean_depth, land_mask, fold_map):
    rows, width = forcing.shape
    tall = rows + 2 * PAD
    f32 = jnp.float32
    n_parts = width // GROUP // 2
    seam_rows = rows // n_parts + 2 * MARGIN + 2 * BAND

    def tile(count):
        return [
            pltpu.VMEM((planes, count + 16, width), f32)
            for planes in (5, 4, 2 * STEPS + 2)
        ]

    edge = pltpu.VMEM((32, width), f32)
    group_rows = rows * GROUP // width
    dma = pltpu.SemaphoreType.DMA
    if n_lat * n_lon <= DIRECT_LIMIT:
        moment_refs = [pltpu.VMEM((n_lat * n_lon, 1, width), f32), dma, dma]
    else:
        moment_refs = [pltpu.VMEM((size, 1, width), f32) for size in (n_lat, n_lon)] + [dma] * 4
    block = pl.BlockSpec(memory_space=pltpu.VMEM)
    outs = pl.pallas_call(
        functools.partial(kernel, n_lat, n_lon),
        out_shape=[
            tile(rows)[-1], tile(seam_rows)[-1], pltpu.VMEM((8, width), f32)
        ],
        in_specs=[pl.BlockSpec(memory_space=pl.ANY)] * 5,
        out_specs=[block] * 3,
        scratch_shapes=[
            pltpu.VMEM((3, rows, width), f32), pltpu.VMEM((rows, width), jnp.int32),
            pltpu.SMEM(fold_map.shape, jnp.int32),
            pltpu.VMEM((3, tall, width), f32), pltpu.VMEM((3, tall, width), f32),
            *tile(rows)[:-1],
            *tile(seam_rows)[:-1],
            *tile(max(group_rows + 2 * MARGIN, 2 * BAND)),
            edge, edge, edge,
            pltpu.VMEM((2, group_rows, width), f32),
            pltpu.VMEM((2, 3 * LIP + 2 * STEPS, width), f32),
            pltpu.VMEM((2, group_rows, width), f32),
            pltpu.VMEM((n_lon, 32, width), f32),
            pltpu.VMEM((group_rows, width), f32),
            pltpu.VMEM((group_rows + 2 * LIP, width), f32),
            pltpu.VMEM((3 * LIP, width), f32),
            pltpu.VMEM((7 * LIP, width), f32),
            pltpu.VMEM((3, BAND, width), f32), pltpu.VMEM((3, BAND, width), f32),
            pltpu.VMEM((6 * STEPS, 8, width), f32),
            dma((3,)), dma((10,)), dma((11,)),
            *moment_refs,
        ],
        compiler_params=pltpu.CompilerParams(collective_id=0, has_side_effects=True),
        name="tripole_cg",
    )(forcing, search_direction, ocean_depth, land_mask, fold_map)
    wide_basis, seam_basis, sums = (
        pltpu.with_memory_space_constraint(out, pltpu.VMEM) for out in outs
    )
    return pl.pallas_call(
        finish,
        out_shape=[jax.ShapeDtypeStruct((rows, width), f32)] * 2,
        in_specs=[block] * 3,
        out_specs=[pl.BlockSpec(memory_space=pl.ANY)] * 2,
        scratch_shapes=[
            pltpu.VMEM((6 * STEPS, width), f32),
            pltpu.VMEM((2, seam_rows, width), f32),
            pltpu.VMEM((2, rows, width), f32),
            dma((2,)),
        ],
        name="finish",
    )(sums, wide_basis, seam_basis)


def solution(mesh):
    cells = P("lat", "lon")
    return jax.shard_map(
        functools.partial(per_device, mesh.shape["lat"], mesh.shape["lon"]),
        mesh=mesh,
        in_specs=(cells, cells, cells, cells, P()),
        out_specs=(cells, cells),
        check_vma=False,
    )
```

```python
import functools

import jax
import jax.numpy as jnp
from jax import lax
from jax.experimental import pallas as pl
from jax.experimental.pallas import tpu as pltpu
from jax.sharding import PartitionSpec as P

STEPS = 8
REACH = 256
MESH = pl.DeviceIdType.MESH
PAD = 16
GROUP = 32
CHUNK = 16
LIP = STEPS + 1
MARGIN = 12
SLAB = 40
BAND = 32
DIRECT_LIMIT = 64

DIRECTIONS = ((1, 0), (-1, 0), (0, 1), (0, -1), (1, 1), (-1, -1), (1, -1), (-1, 1))
SLOT = {offset: index for index, offset in enumerate(DIRECTIONS)}


def halves(offset):
    return 0.5 if 0 in offset else 0.25


def chunks_of(low, high, size):
    return [(at, min(size, high - at)) for at in range(low, high, size)]


def turned(x, shift):
    shift = shift % x.shape[1]
    return x if shift == 0 else pltpu.roll(x, shift, 1)


def plus(left, right):
    result = dict(left)
    for key, value in right.items():
        result[key] = result[key] + value if key in result else value
    return result


def scaled(factor, vector):
    return {key: factor * value for key, value in vector.items()}


def apply_shift(vector):
    result = {}
    for (chain, power), value in vector.items():
        parts = [((chain, power), value)]
        if power == 0:
            parts.append(((chain, 1), value))
        else:
            half = 0.5 * value
            parts += [((chain, power + 1), half), ((chain, power - 1), half)]
        result = plus(result, {}) if not parts else result
        for key, part in parts:
            result = plus(result, {key: part})
    return result


def tree_sum(terms):
    terms = list(terms)
    while len(terms) > 1:
        odd = terms[len(terms) // 2 * 2 :]
        terms = [x + y for x, y in zip(terms[0::2], terms[1::2])] + odd
    return terms[0]


def against(coords, series):
    return tree_sum(value * series[key] for key, value in sorted(coords.items()))


def shifted_series(series, chain, reach):
    result = {}
    for k in range(reach + 1):
        beside = (
            series[(chain, 1)]
            if k == 0
            else 0.5 * (series[(chain, k + 1)] + series[(chain, k - 1)])
        )
        result[(chain, k)] = series[(chain, k)] + beside
    return result


def coordinates(moments):
    one = jnp.ones_like(moments[("p", "p")][0])
    direction_coords, residual_coords = {("p", 0): one}, {("r", 0): one}
    direction = {("p", k): value for k, value in enumerate(moments[("p", "p")])}
    direction |= {("r", k): value for k, value in enumerate(moments[("p", "r")])}
    residual = {("p", k): value for k, value in enumerate(moments[("p", "r")])}
    residual |= {("r", k): value for k, value in enumerate(moments[("r", "r")])}
    solution_coords = {}
    norm_now = residual[("r", 0)]
    for step in range(STEPS):
        reach = 2 * STEPS - 2 - step
        mapped = shifted_series(direction, "p", reach) | shifted_series(direction, "r", reach - 1)
        mapped_coords = apply_shift(direction_coords)
        step_length = norm_now / against(direction_coords, mapped)
        solution_coords = plus(solution_coords, scaled(step_length, direction_coords))
        residual_coords = plus(residual_coords, scaled(-step_length, mapped_coords))
        if step == STEPS - 1:
            break
        residual = {key: residual[key] - step_length * value for key, value in mapped.items()}
        shrink = 1.0 / norm_now
        norm_now = against(residual_coords, residual)
        turn = norm_now * shrink
        direction = {key: value + turn * direction[key] for key, value in residual.items()}
        direction_coords = plus(residual_coords, scaled(turn, direction_coords))
    return solution_coords, residual_coords


def fold_sublanes(parts):
    row = lax.broadcasted_iota(jnp.int32, parts[0].shape, 0)
    parts = list(parts)
    span = 4
    while span:
        low = (row & span) == 0
        half = len(parts) // 2
        parts = [
            jnp.where(low, first, second)
            + pltpu.roll(jnp.where(low, second, first), span, 0)
            if span == 4
            else jnp.where(low, first, second)
            + jnp.where(low, pltpu.roll(first, 8 - span, 0), pltpu.roll(second, span, 0))
            for first, second in zip(parts[:half], parts[half:])
        ]
        span //= 2
    return parts[0]


def kept(at, count, regions):
    row = lax.broadcasted_iota(jnp.int32, (8, regions[0][2].shape[1]), 0)
    masks = []
    for r in range(at, at + count, 8):
        mask = None
        for low, high, lanes in regions:
            if low >= r + 8 or high <= r:
                continue
            part = lanes
            if low > r or high < r + 8:
                part = lanes & (row >= low - r) & (row < high - r)
            mask = part if mask is None else mask | part
        masks.append(mask)
    return masks


def gathered(around):
    beside = around[-1] + around[1]
    edge = around[0] + 0.5 * beside
    return beside + (turned(edge, -1) + turned(edge, 1))


def rows_near(ref, at, count):
    return {a: ref[at + a : at + a + count, :] for a in (-1, 0, 1)}


def clear(rows, planes, deep, basis):
    width = planes.shape[2]
    zero = jnp.zeros((8, width), jnp.float32)
    for at in (0, 8 + rows):
        planes[0, at : at + 8, :] = zero
    for at in range(0, rows + 16, 8):
        for slot in range(4):
            deep[slot, at : at + 8, :] = zero
        for slot in range(2 * STEPS + 1):
            basis[slot, at : at + 8, :] = zero


def prepare(rows, planes, deep, basis, regions):
    depth = planes.at[0]
    for at, count in chunks_of(8, 8 + rows, CHUNK):
        span = pl.ds(at, count)
        around = rows_near(depth, at, count)
        here = around[0]
        is_wet = here > 0.0
        wet = {a: jnp.where(value > 0.0, 1.0, 0.0) for a, value in around.items()}
        links = 0.5 * (here * gathered(wet) + gathered(around))
        diagonal = jnp.where(is_wet, here * (1.0 / (REACH * REACH)) + links, 1.0)
        root = lax.rsqrt(diagonal)
        planes[3, span, :] = turned(here, 1)
        planes[4, span, :] = turned(here, -1)
        planes[1, span, :] = jnp.where(is_wet, -(root * root), 0.0)
        basis[2 * STEPS + 1, span, :] = diagonal * root
        for i, mask in enumerate(kept(at - 8, count, regions)):
            if mask is not None:
                planes[2, at + 8 * i : at + 8 * i + 8, :] = jnp.where(
                    mask, diagonal[8 * i : 8 * i + 8, :], 0.0
                )
        for chain, slot in enumerate((0, STEPS + 1)):
            value = root * basis[slot, span, :]
            basis[slot, span, :] = value
            deep[chain, span, :] = here * value


def needed(rows, regions, reach):
    tiles = sorted({
        at
        for low, high, _ in regions
        for at in range(max(low - reach, 0) // 8 * 8, min(high + reach, rows), 8)
    })
    runs = []
    for at in tiles:
        if runs and runs[-1][0] + runs[-1][1] == at and runs[-1][1] < CHUNK:
            runs[-1][1] += 8
        else:
            runs.append([at, 8])
    return [(8 + at, count) for at, count in runs]


def march(rows, planes, deep, basis, regions, add_dot, flush, new):
    def weighted(at, masks, value):
        return [
            None
            if mask is None
            else planes[2, at + 8 * i : at + 8 * i + 8, :] * value[8 * i : 8 * i + 8, :]
            for i, mask in enumerate(masks)
        ]

    def dot(key, left, right):
        for i, piece in enumerate(left):
            if piece is not None:
                add_dot(key, piece, right[8 * i : 8 * i + 8, :])

    for at, count in needed(rows, regions, 0) if add_dot else []:
        p0 = basis[0, at : at + count, :]
        r0 = basis[STEPS + 1, at : at + count, :]
        masks = kept(at - 8, count, regions)
        p0_kept, r0_kept = weighted(at, masks, p0), weighted(at, masks, r0)
        dot(("p", "p", 0), p0_kept, p0)
        dot(("r", "r", 0), r0_kept, r0)
        dot(("p", "r", 0), p0_kept, r0)

    for power in range(1, STEPS + 1):
        chains = [("p", 0)] + ([("r", STEPS + 1)] if power < STEPS else [])
        for at, count in needed(rows, regions, STEPS - power):
            fresh = {}
            held = {}
            depth, factor, west_depth, east_depth = (
                planes[plane, at : at + count, :] for plane in (0, 1, 3, 4)
            )
            for chain, (name, origin) in enumerate(chains):
                slot = origin + power
                before, after = (power + 1) % 2 * 2 + chain, power % 2 * 2 + chain
                taken = rows_near(basis.at[slot - 1], at, count)
                held[name] = taken[0]
                heavy = rows_near(deep.at[before], at, count)
                beside, beside_heavy = taken[-1] + taken[1], heavy[-1] + heavy[1]
                edge = taken[0] + 0.5 * beside
                edge_heavy = heavy[0] + 0.5 * beside_heavy
                sums = (depth * beside + beside_heavy) + (
                    turned(west_depth * edge + edge_heavy, -1)
                    + turned(east_depth * edge + edge_heavy, 1)
                )
                if power == 1:
                    value = (0.5 * factor) * sums
                else:
                    value = factor * sums - basis[slot - 2, at : at + count, :]
                basis[slot, at : at + count, :] = value
                if power < STEPS:
                    deep[after, at : at + count, :] = depth * value
                fresh[name] = value
            if not add_dot:
                continue
            masks = kept(at - 8, count, regions)
            fresh_kept = {name: weighted(at, masks, fresh[name]) for name, _ in chains}
            for name, _ in chains:
                dot((name, name, 2 * power), fresh_kept[name], fresh[name])
                dot((name, name, 2 * power - 1), fresh_kept[name], held[name])
            if power < STEPS:
                dot(("p", "r", 2 * power), fresh_kept["p"], fresh["r"])
                dot(("p", "r", 2 * power - 1), fresh_kept["p"], held["r"])
            else:
                dot(
                    ("p", "r", 2 * power - 1),
                    fresh_kept["p"],
                    basis[STEPS + power, at : at + count, :],
                )
        if add_dot:
            flush(new)


def kernel(
    n_lat, n_lon, forcing_hbm, search_hbm, depth_hbm, mask_hbm, fold_hbm,
    wide_basis, seam_basis, sums_out, loaded, mask_in, fold_map,
    centre, side, wide, wide_deep, seam, seam_deep, far, far_deep, far_basis, row_north, row_south,
    fold_rows, packed, got_rows, got_sides, fold_all, deep_packed, got_deep, deep_rows, got_far,
    far_centre, far_side, dots, load_sem, near_send, near_recv, *moment_refs,
):
    rows, width = forcing_hbm.shape
    lat, lon = lax.axis_index("lat"), lax.axis_index("lon")
    top = n_lat - 1
    north, south = lax.rem(lat + 1, n_lat), lax.rem(lat + n_lat - 1, n_lat)
    east, west = lax.rem(lon + 1, n_lon), lax.rem(lon + n_lon - 1, n_lon)
    has_north, has_south = lat < top, lat > 0
    group_rows = rows * GROUP // width
    n_groups = width // GROUP

    barrier = pltpu.get_barrier_semaphore()

    def greet(place):
        pl.semaphore_signal(barrier, inc=1, device_id=place, device_id_type=MESH)

    for source, target, index in (
        (mask_hbm, mask_in, 0), (depth_hbm, loaded.at[0], 1), (search_hbm, loaded.at[1], 1),
        (forcing_hbm, loaded.at[2], 1), (fold_hbm, fold_map, 2),
    ):
        pltpu.make_async_copy(source, target, load_sem.at[index]).start()
    depth_in, search, forcing = loaded.at[0], loaded.at[1], loaded.at[2]
    direct = n_lat * n_lon <= DIRECT_LIMIT
    everyone = [(a, b) for a in range(n_lat) for b in range(n_lon) if a or b]
    everyone.sort(key=lambda d: (d[1] or n_lon, d[0] or n_lat))
    if direct:
        for a, b in everyone:
            greet((lax.rem(lat + a, n_lat), lax.rem(lon + b, n_lon)))
        greeted = len(everyone)
    else:
        for d in range(1, n_lat):
            greet((lax.rem(lat + d, n_lat), lon))
        for d in range(1, n_lon):
            greet((lat, lax.rem(lon + d, n_lon)))
        for place in ((north, east), (north, west), (south, east), (south, west)):
            greet(place)
        greeted = n_lat - 1 + n_lon - 1 + 4

    n_parts = width // GROUP // 2
    part_rows = rows // n_parts
    strip_rows = part_rows + 2 * MARGIN
    seam_rows = strip_rows + 2 * BAND
    patch_rows = group_rows + 2 * MARGIN
    far_tile_rows = max(patch_rows, 2 * BAND)
    clear(rows, wide, wide_deep, wide_basis)
    clear(seam_rows, seam, seam_deep, seam_basis)
    clear(far_tile_rows, far, far_deep, far_basis)
    pltpu.make_async_copy(mask_hbm, mask_in, load_sem.at[0]).wait()
    pltpu.make_async_copy(loaded, loaded, load_sem.at[1]).wait()
    pltpu.make_async_copy(fold_hbm, fold_map, load_sem.at[2]).wait()
    lane_group = lax.broadcasted_iota(jnp.int32, (group_rows, width), 1)
    west_edge = east_edge = None
    for g in range(n_groups):
        here = pl.ds(g * group_rows, group_rows)
        there = pl.ds(PAD + g * group_rows, group_rows)
        flag = mask_in[here, :].astype(jnp.float32)
        deep = depth_in[here, :] * flag
        moving = search[here, :] * flag
        left = forcing[here, :] * flag
        for index, value in enumerate((deep, moving, left)):
            centre[index, there, :] = value
        inner = pl.ds(8 + g * group_rows, group_rows)
        wide[0, inner, :] = deep
        wide_basis[0, inner, :] = moving
        wide_basis[STEPS + 1, inner, :] = left
        inside = lane_group - g * GROUP
        to_west = jnp.where(
            inside < 9,
            turned(deep, g * GROUP),
            jnp.where(inside < 17, turned(moving, g * GROUP + 9), turned(left, g * GROUP + 17)),
        )
        to_east = jnp.where(
            inside < 9,
            turned(deep, g * GROUP + 9),
            jnp.where(inside < 17, turned(moving, g * GROUP + 17), turned(left, g * GROUP + 25)),
        )
        west_edge = to_west if g == 0 else jnp.where(inside >= 0, to_west, west_edge)
        east_edge = to_east if g == 0 else jnp.where(inside >= 0, to_east, east_edge)
    packed[0] = west_edge
    packed[1] = east_edge
    first, last = PAD, PAD + rows
    spans = ((0, 0, LIP), (1, LIP, STEPS), (2, LIP + STEPS, STEPS))
    depth_of = LIP + 2 * STEPS
    for index, at, count in spans:
        row_south[at : at + count, :] = centre[index, first : first + count, :]
        row_north[at : at + count, :] = centre[index, last - count : last, :]

    @pl.when(lat == top)
    def _():
        for index, at, count in spans:
            for r in range(count):
                fold_rows[at + r : at + r + 1, :] = centre[index, last - 1 - r : last - r, :]
        fold_all[lon, 0:depth_of, :] = fold_rows[0:depth_of, :]

    pl.semaphore_wait(barrier, greeted)

    reach = n_lon // 2 + 1
    at_seam, past_seam = lon == n_lon - 1, lon == 0
    on_top = lat == top
    fold_late, fold_early = on_top & (lon > reach), on_top & (lon >= 1) & (lon < n_lon - reach)

    def near(gone, arrived, source, target, place):
        return pltpu.make_async_remote_copy(
            src_ref=source, dst_ref=target, send_sem=near_send.at[gone],
            recv_sem=near_recv.at[arrived], device_id=place, device_id_type=MESH,
        )

    def arrival(index, block):
        return near(0, index, block, block, (lat, lon))

    def departure(index, block):
        return near(index, 0, block, block, (lat, lon))

    tail, head = pl.ds(group_rows - LIP, LIP), pl.ds(0, LIP)
    tall_tail = pl.ds(group_rows - 2 * LIP, 2 * LIP)
    full = pl.ds(0, depth_of)
    near_rows = pl.ds(0, depth_of + LIP)
    got_south, got_north = got_rows.at[0, full], got_rows.at[1, full]
    got_west, got_east = got_sides.at[0], got_sides.at[1]
    corners = [got_rows.at[index // 2, pl.ds(depth_of + LIP * (index % 2), LIP)] for index in range(4)]
    deep_strip = got_deep.at[0:group_rows]
    deep_south = got_deep.at[group_rows : group_rows + LIP]
    deep_north = got_deep.at[group_rows + LIP : group_rows + 2 * LIP]
    far_rows = got_far.at[0 : 3 * LIP]
    far_edges = [got_far.at[at : at + 2 * LIP] for at in (3 * LIP, 5 * LIP)]
    northward = (
        near(0, 0, row_north.at[full], got_south, (north, lon)),
        near(0, 0, packed.at[1, tail], corners[0], (north, east)),
        near(0, 4, packed.at[0, tail], corners[1], (north, west)),
    )
    southward = (
        near(1, 1, row_south.at[full], got_north, (south, lon)),
        near(1, 1, packed.at[1, head], corners[2], (south, east)),
        near(1, 5, packed.at[0, head], corners[3], (south, west)),
    )
    to_east = near(2, 2, packed.at[1], got_west, (lat, east))
    to_west = near(2, 3, packed.at[0], got_east, (lat, west))
    deep_east = near(4, 7, deep_packed, deep_strip, (lat, east))
    deep_up = near(5, 8, deep_packed.at[tail], deep_south, (north, east))
    deep_down = near(6, 9, deep_packed.at[head], deep_north, (south, east))

    def at_reach(step):
        return (lat, lax.rem(lon + step + n_lon, n_lon))

    far_away = near(7, 10, deep_rows, far_rows, at_reach(-reach))
    far_west_edge = near(8, 10, packed.at[1, tall_tail], far_edges[0], at_reach(1 - reach))
    far_east_edge = near(9, 10, packed.at[0, tall_tail], far_edges[1], at_reach(-1 - reach))
    gives_west_edge = on_top & (lon >= reach) & (lon < n_lon - 1)
    gives_east_edge = on_top & ((lon > reach + 1) | (lon == 0))

    def spread(source, slot, send_sem, recv_sem, along_lat):
        size = n_lat if along_lat else n_lon
        me = lat if along_lat else lon
        copies = []
        for d in range(1, size):
            peer = lax.rem(me + d, size)
            copies.append(
                pltpu.make_async_remote_copy(
                    src_ref=source, dst_ref=slot, send_sem=send_sem,
                    recv_sem=recv_sem,
                    device_id=(peer, lon) if along_lat else (lat, peer),
                    device_id_type=MESH,
                )
            )
        return copies

    across = spread(
        fold_rows.at[full], fold_all.at[lon, full], near_send.at[3], near_recv.at[6], False
    )

    to_west.start()
    to_east.start()

    @pl.when(has_north)
    def _():
        for copy in northward:
            copy.start()

    @pl.when(has_south)
    def _():
        for copy in southward:
            copy.start()

    @pl.when(at_seam)
    def _():
        for g in range(n_groups):
            here = pl.ds(PAD + g * group_rows, group_rows)
            inside = lane_group - g * GROUP
            value = jnp.where(
                inside < LIP,
                turned(centre[0, here, :], g * GROUP + 2 * LIP),
                jnp.where(
                    inside < 2 * LIP,
                    turned(centre[1, here, :], g * GROUP + 3 * LIP - 1),
                    turned(centre[2, here, :], g * GROUP + 4 * LIP - 1),
                ),
            )
            if g:
                value = jnp.where(inside >= 0, value, deep_packed[...])
            deep_packed[...] = value
        deep_east.start()

        @pl.when(has_north)
        def _():
            deep_up.start()

        @pl.when(has_south)
        def _():
            deep_down.start()

    @pl.when(on_top)
    def _():
        for index, top_row in enumerate((LIP, STEPS, STEPS)):
            low = last - top_row - LIP
            deep_rows[index * LIP : (index + 1) * LIP, :] = centre[index, low : low + LIP, :]
        for copy in reversed(across):
            copy.start()

    for condition, copy in (
        (fold_late, far_away),
        (gives_west_edge, far_west_edge),
        (gives_east_edge, far_east_edge),
    ):
        @pl.when(condition)
        def _():
            copy.start()

    dot_sums = {}

    def add_dot(key, left, right):
        product = left * right
        for r in range(0, product.shape[0], 8):
            piece = product[r : r + 8, :]
            dot_sums[key] = piece if key not in dot_sums else dot_sums[key] + piece

    def flush(new):
        for key in list(dot_sums):
            total = dot_sums.pop(key)
            spot = order_of()[key]
            dots[spot] = total if new else dots[spot] + total

    lane8 = lax.broadcasted_iota(jnp.int32, (8, width), 1)
    nothing = jnp.zeros((8, width), jnp.float32)

    middle = (lane8 >= LIP) & (lane8 < width - LIP)

    wide_regions = [(LIP, rows - LIP, middle)]
    prepare(rows, wide, wide_deep, wide_basis, wide_regions)
    march(rows, wide, wide_deep, wide_basis, wide_regions, add_dot, flush, True)

    part_spans = ((0, 0, LIP), (1, LIP, STEPS), (2, LIP + STEPS, STEPS))

    def unpack_west(got, target, start, g, count):
        lane = lax.broadcasted_iota(jnp.int32, (count, width), 1)
        for index, offset, cells in part_spans:
            value = turned(got, -g * GROUP - offset - cells)
            target[index, start : start + count, :] = jnp.where(lane >= width - cells, value, 0.0)

    def unpack_east(got, target, start, g, count):
        lane = lax.broadcasted_iota(jnp.int32, (count, width), 1)
        for index, offset, cells in part_spans:
            value = turned(got, -g * GROUP - offset)
            target[index, start : start + count, :] = jnp.where(
                lane < cells, value, target[index, start : start + count, :]
            )

    def unpack_deep(got, start, g, count):
        lane = lax.broadcasted_iota(jnp.int32, (count, width), 1)
        for index, cells in ((0, LIP), (1, STEPS), (2, STEPS)):
            low = width - cells - LIP
            value = turned(got, low - g * GROUP - index * LIP)
            side[index, start : start + count, :] = jnp.where(
                (lane >= low) & (lane < low + LIP), value, side[index, start : start + count, :]
            )

    for index in (0, 1, 2):
        for at in (0, 8, last, last + 8):
            centre[index, at : at + 8, :] = nothing
            side[index, at : at + 8, :] = nothing

    def take_east():
        arrival(3, got_east).wait_recv()
        for g in range(n_groups):
            unpack_east(got_east[...], side, first + g * group_rows, g, group_rows)

        @pl.when(has_south)
        def _():
            arrival(4, corners[1]).wait_recv()
            unpack_east(corners[1][...], side, first - LIP, n_groups - 1, LIP)

        @pl.when(has_north)
        def _():
            arrival(5, corners[3]).wait_recv()
            unpack_east(corners[3][...], side, last, 0, LIP)

    def folded(home):
        total = n_lon * width
        pivot = lax.rem(fold_map[0] - home * width + total, total)
        block, offset = pivot // width, lax.rem(pivot, width)
        lane = lax.broadcasted_iota(jnp.int32, (32, width), 1)
        index = lax.rem(offset - lane + width, width)

        def mirrored(which):
            rows_of = fold_all[lax.rem(block + which + n_lon, n_lon)]
            return jnp.take_along_axis(rows_of, index, axis=1, mode="promise_in_bounds")

        ahead, same, behind, beyond = (mirrored(which) for which in (1, 0, -1, -2))
        close = lane <= offset
        value = jnp.where(close, same, behind)
        halo = jnp.where(
            lane < width // 2, jnp.where(close, behind, beyond), jnp.where(close, ahead, same)
        )
        return value, halo

    def take_fold():
        arrival(6, fold_all.at[0 : n_lon - 1, full]).wait_recv()
        for source, target in zip(folded(lon), (centre, side)):
            for index, at, count in spans:
                target[index, last : last + count, :] = source[at : at + count, :]

    north_at, south_at = strip_rows, strip_rows + BAND
    own = GROUP - LIP
    slot_of = lane8 // GROUP
    slot_lane = lane8 - slot_of * GROUP

    east_half = lane8 < n_parts * GROUP
    strip_at = jnp.where(east_half, slot_lane - (own - LIP), slot_lane - LIP)
    closed = jnp.where(fold_late, 1, 0)
    strip_lanes = (strip_at >= 0) & (strip_at < LIP) & (
        jnp.where(east_half, lon, -1) < n_lon - 1
    )
    last_part = lax.rem(slot_of, n_parts) == n_parts - 1
    north_lanes = strip_lanes & (jnp.where(last_part, closed, 0) == 0)
    band_lanes = jnp.where(middle, closed, 1) == 0

    seam_regions = [
        (MARGIN, MARGIN + part_rows - LIP, strip_lanes),
        (MARGIN + part_rows - LIP, MARGIN + part_rows, north_lanes),
        (north_at + BAND - 2 * LIP, north_at + BAND - LIP, band_lanes),
        (south_at + LIP, south_at + 2 * LIP, middle),
    ]
    def assemble():
        targets = (seam.at[0], seam_basis.at[0], seam_basis.at[STEPS + 1])
        for index, target in enumerate(targets):
            for at in range(0, strip_rows, 8):
                value = None
                for q in range(n_parts):
                    low = PAD + q * part_rows - MARGIN + at
                    inside, outside = centre[index, low : low + 8, :], side[index, low : low + 8, :]
                    east_slot = turned(
                        jnp.where(lane8 >= width - own, inside, outside),
                        q * GROUP - (width - own),
                    )
                    west_slot = turned(
                        jnp.where(lane8 < own, inside, outside), (n_parts + q) * GROUP + LIP
                    )
                    mixed = jnp.where(lane8 < n_parts * GROUP, east_slot, west_slot)
                    value = mixed if q == 0 else jnp.where(
                        lax.rem(slot_of, n_parts) >= q, mixed, value
                    )
                target[8 + at : 16 + at, :] = value
            for at in range(0, BAND, 8):
                low = last + LIP - BAND + at
                target[8 + north_at + at : 16 + north_at + at, :] = centre[index, low : low + 8, :]
                low = first - LIP + at
                target[8 + south_at + at : 16 + south_at + at, :] = centre[index, low : low + 8, :]
        prepare(seam_rows, seam, seam_deep, seam_basis, seam_regions)

    arrival(2, got_west).wait_recv()
    for g in range(n_groups):
        unpack_west(got_west[...], side, first + g * group_rows, g, group_rows)

    @pl.when(has_south)
    def _():
        arrival(0, got_rows.at[0, near_rows]).wait_recv()
        for index, at, count in spans:
            centre[index, first - count : first, :] = got_south[at : at + count, :]
        unpack_west(corners[0][...], side, first - LIP, n_groups - 1, LIP)

    @pl.when(has_north)
    def _():
        arrival(1, got_rows.at[1, near_rows]).wait_recv()
        for index, at, count in spans:
            centre[index, last : last + count, :] = got_north[at : at + count, :]
        unpack_west(corners[2][...], side, last, 0, LIP)

    @pl.when(jnp.logical_not(at_seam))
    def _():
        take_east()

    @pl.when(on_top & (lon <= reach))
    def _():
        take_fold()

    assemble()
    march(seam_rows, seam, seam_deep, seam_basis, seam_regions, add_dot, flush, False)

    far_targets = (far.at[0], far_basis.at[0], far_basis.at[STEPS + 1])

    def march_far(regions):
        prepare(far_tile_rows, far, far_deep, far_basis, regions)
        march(far_tile_rows, far, far_deep, far_basis, regions, add_dot, flush, False)

    @pl.when(past_seam)
    def _():
        arrival(7, deep_strip).wait_recv()
        for g in range(n_groups):
            unpack_deep(deep_strip[...], first + g * group_rows, g, group_rows)

        @pl.when(has_south)
        def _():
            arrival(8, deep_south).wait_recv()
            unpack_deep(deep_south[...], first - LIP, n_groups - 1, LIP)

        @pl.when(has_north)
        def _():
            arrival(9, deep_north).wait_recv()
            unpack_deep(deep_north[...], last, 0, LIP)

        span_lanes = GROUP - 2 * LIP
        for index, target in enumerate(far_targets):
            for at in range(0, patch_rows, 8):
                value = None
                for g in range(n_groups):
                    low = PAD + g * group_rows - MARGIN + at
                    mixed = turned(
                        jnp.where(
                            lane8 < span_lanes,
                            centre[index, low : low + 8, :],
                            side[index, low : low + 8, :],
                        ),
                        g * GROUP + 2 * LIP,
                    )
                    value = mixed if g == 0 else jnp.where(slot_of >= g, mixed, value)
                target[8 + at : 16 + at, :] = value
        patch_lanes = (slot_lane >= LIP) & (slot_lane < 2 * LIP)
        upper = jnp.where(slot_of == n_groups - 1, jnp.where(on_top, 1, 0), 0) == 0
        march_far([
            (MARGIN, MARGIN + group_rows - LIP, patch_lanes),
            (MARGIN + group_rows - LIP, MARGIN + group_rows, patch_lanes & upper),
        ])

    @pl.when(fold_early)
    def _():
        edge_row = BAND - LIP
        for target in (far_centre, far_side):
            for index in (0, 1, 2):
                for at in range(0, BAND, 8):
                    target[index, at : at + 8, :] = nothing
        arrival(10, got_far).wait_recv()
        home = lon + reach
        low = edge_row - 2 * LIP
        unpack_west(far_edges[0][...], far_side, low, n_groups - 1, 2 * LIP)
        unpack_east(far_edges[1][...], far_side, low, n_groups - 1, 2 * LIP)
        mirror = folded(home)
        for index, at, count in spans:
            low = edge_row - count - LIP
            far_centre[index, low : low + LIP, :] = far_rows[index * LIP : (index + 1) * LIP, :]
            for r in range(count):
                far_centre[index, edge_row - 1 - r : edge_row - r, :] = fold_all[
                    home, at + r : at + r + 1, :
                ]
            for source, target in zip(mirror, (far_centre, far_side)):
                target[index, edge_row : edge_row + count, :] = source[at : at + count, :]
        for index, target in enumerate(far_targets):
            for at in range(0, BAND, 8):
                inside, outside = far_centre[index, at : at + 8, :], far_side[index, at : at + 8, :]
                target[8 + at : 16 + at, :] = inside
                spot = 8 + BAND + at
                target[spot : spot + 8, :] = jnp.where(
                    lane8 < GROUP,
                    turned(jnp.where(lane8 >= width - own, inside, outside), own - width),
                    turned(jnp.where(lane8 < own, inside, outside), GROUP + LIP),
                )
        edge_at = jnp.where(slot_of == 0, slot_lane - (own - LIP), slot_lane - LIP)
        edge_lanes = (slot_of < 2) & (edge_at >= 0) & (edge_at < LIP)
        fold_at = BAND - 2 * LIP
        march_far([
            (fold_at, fold_at + LIP, middle),
            (fold_at + BAND, fold_at + BAND + LIP, edge_lanes),
        ])

    def finish_late():
        @pl.when(at_seam | fold_late)
        def _():
            @pl.when(at_seam)
            def _():
                take_east()

            @pl.when(fold_late)
            def _():
                take_fold()

            assemble()
            march(seam_rows, seam, seam_deep, seam_basis, seam_regions, None, None, False)

    number = len(order_of())
    pending = []
    lane = lax.broadcasted_iota(jnp.int32, (8, width), 1)
    home = lane - lax.broadcasted_iota(jnp.int32, (8, width), 0)
    message = jnp.zeros((8, width), jnp.float32)
    for g in range(number // 8):
        grouped = fold_sublanes([dots[8 * g + s] for s in range(8)])
        message = jnp.where(home == 8 * g, jnp.sum(grouped, axis=1, keepdims=True), message)
    message = jnp.sum(message, axis=0, keepdims=True)
    if direct:
        slots, send_sem, recv_sem = moment_refs
        me = lat * n_lon + lon
        slots[me] = message
        copies = [
            pltpu.make_async_remote_copy(
                src_ref=slots.at[me], dst_ref=slots.at[me], send_sem=send_sem,
                recv_sem=recv_sem,
                device_id=(lax.rem(lat + a, n_lat), lax.rem(lon + b, n_lon)),
                device_id_type=MESH,
            )
            for a, b in everyone
        ]
        rounds = ((slots, n_lat * n_lon, copies, send_sem, recv_sem),)
    else:
        slots_lat, slots_lon, lat_send, lat_recv, lon_send, lon_recv = moment_refs
        rounds = (
            (slots_lat, n_lat, None, lat_send, lat_recv, lat, True),
            (slots_lon, n_lon, None, lon_send, lon_recv, lon, False),
        )
    for slots, size, copies, send_sem, recv_sem, *rest in rounds:
        if copies is None:
            me, along_lat = rest
            slots[me] = message
            copies = spread(slots.at[me], slots.at[me], send_sem, recv_sem, along_lat)
        for copy in copies:
            copy.start()
        if not pending:
            finish_late()
        others = slots.at[0 : size - 1]
        whole = pltpu.make_async_remote_copy(
            src_ref=others, dst_ref=others, send_sem=send_sem, recv_sem=recv_sem,
            device_id=(lat, lon), device_id_type=MESH,
        )
        whole.wait_recv()
        terms = [slots[index] for index in range(size)]
        while len(terms) > 1:
            odd = terms[len(terms) // 2 * 2 :]
            terms = [x + y for x, y in zip(terms[0::2], terms[1::2])] + odd
        message = terms[0]
        pending.append(whole)
    sums_out[...] = jnp.broadcast_to(message, (8, width))
    for copy in pending:
        copy.wait_send()
    departure(2, got_sides).wait_send()
    for condition, index, block in (
        (has_north, 0, got_rows.at[0]),
        (has_south, 1, got_rows.at[1]),
        (on_top, 3, fold_all.at[0 : n_lon - 1, full]),
        (at_seam, 4, deep_packed),
        (at_seam & has_north, 5, deep_south),
        (at_seam & has_south, 6, deep_north),
        (fold_late, 7, far_rows),
        (gives_west_edge, 8, far_edges[0]),
        (gives_east_edge, 9, far_edges[1]),
    ):
        @pl.when(condition)
        def _():
            departure(index, block).wait_send()


@functools.cache
def order_of():
    keys = [("p", "p", k) for k in range(2 * STEPS + 1)]
    keys += [("p", "r", k) for k in range(2 * STEPS)]
    keys += [("r", "r", k) for k in range(2 * STEPS - 1)]
    return {key: index for index, key in enumerate(keys)}


def finish(
    sums, wide_basis, seam_basis, out_height, out_residual, moment_rows, patch, results, out_sem
):
    rows, width = out_height.shape
    number = len(order_of())
    n_parts = width // GROUP // 2
    part_rows = rows // n_parts
    north_at = part_rows + 2 * MARGIN
    south_at = north_at + BAND
    seam_rows = south_at + BAND
    own = GROUP - LIP
    lane8 = lax.broadcasted_iota(jnp.int32, (8, width), 1)
    home = lane8 - lax.broadcasted_iota(jnp.int32, (8, width), 0)
    message = sums[...]
    for g in range(number // 8):
        picked = jnp.sum(jnp.where(home == 8 * g, message, 0.0), axis=1, keepdims=True)
        moment_rows[8 * g : 8 * g + 8, :] = jnp.broadcast_to(picked, (8, width))
    moments = {}
    for kind in (("p", "p"), ("p", "r"), ("r", "r")):
        series = []
        for index in range(17 if kind == ("p", "p") else 16 if kind == ("p", "r") else 15):
            spot = order_of()[kind + (index,)]
            value = jnp.broadcast_to(moment_rows[spot : spot + 1, :], (8, width))
            series.append(value if index < 2 else 2.0 * value - series[index % 2])
        moments[kind] = series
    height_coords, residual_coords = coordinates(moments)
    outs = (out_height, out_residual)
    wanted = (height_coords, residual_coords)

    def combined(fields, at):
        totals = [None, None]
        for chain, power in sorted(height_coords | residual_coords):
            slot = power + (0 if chain == "p" else STEPS + 1)
            field = fields[slot, 8 + at : 16 + at, :]
            for which, coords in enumerate(wanted):
                if (chain, power) in coords:
                    term = coords[(chain, power)] * field
                    totals[which] = term if totals[which] is None else totals[which] + term
        stretch = fields[2 * STEPS + 1, 8 + at : 16 + at, :]
        return [stretch * total for total in totals]

    kept_rows = ((MARGIN, part_rows), (north_at + BAND - 2 * LIP, LIP), (south_at + LIP, LIP))
    for start, count in needed(seam_rows, [(low, low + size, None) for low, size in kept_rows], 0):
        for at in range(start - 8, start - 8 + count, 8):
            for which, total in enumerate(combined(seam_basis, at)):
                patch[which, at : at + 8, :] = total
    row8 = lax.broadcasted_iota(jnp.int32, (8, width), 0)
    for at in range(0, rows, 8):
        q = at // part_rows
        for which, total in enumerate(combined(wide_basis, at)):
            for low, high, source in (
                (0, LIP, south_at + LIP),
                (rows - LIP, rows, north_at + BAND - LIP - rows),
            ):
                if low < at + 8 and high > at:
                    edge = patch[which, source + at : source + at + 8, :]
                    if low <= at and high >= at + 8:
                        total = edge
                    else:
                        total = jnp.where((row8 >= low - at) & (row8 < high - at), edge, total)
            spot = at - q * part_rows + MARGIN
            strip = patch[which, spot : spot + 8, :]
            total = jnp.where(lane8 < LIP, turned(strip, -(n_parts + q) * GROUP - LIP), total)
            total = jnp.where(
                lane8 >= width - LIP, turned(strip, width - own - q * GROUP), total
            )
            results[which, at : at + 8, :] = total
        if (at + 8) % SLAB == 0 or at + 8 == rows:
            low = at // SLAB * SLAB
            span = slice(low, at + 8)
            for which, out in enumerate(outs):
                pltpu.make_async_copy(
                    results.at[which, span], out.at[span], out_sem.at[which]
                ).start()
    for which, out in enumerate(outs):
        pltpu.make_async_copy(results.at[which], out, out_sem.at[which]).wait()


def per_device(n_lat, n_lon, forcing, search_direction, ocean_depth, land_mask, fold_map):
    rows, width = forcing.shape
    tall = rows + 2 * PAD
    f32 = jnp.float32
    n_parts = width // GROUP // 2
    seam_rows = rows // n_parts + 2 * MARGIN + 2 * BAND

    def tile(count):
        return [
            pltpu.VMEM((planes, count + 16, width), f32)
            for planes in (5, 4, 2 * STEPS + 2)
        ]

    edge = pltpu.VMEM((32, width), f32)
    group_rows = rows * GROUP // width
    dma = pltpu.SemaphoreType.DMA
    if n_lat * n_lon <= DIRECT_LIMIT:
        moment_refs = [pltpu.VMEM((n_lat * n_lon, 1, width), f32), dma, dma]
    else:
        moment_refs = [pltpu.VMEM((size, 1, width), f32) for size in (n_lat, n_lon)] + [dma] * 4
    block = pl.BlockSpec(memory_space=pltpu.VMEM)
    outs = pl.pallas_call(
        functools.partial(kernel, n_lat, n_lon),
        out_shape=[
            tile(rows)[-1], tile(seam_rows)[-1], pltpu.VMEM((8, width), f32)
        ],
        in_specs=[pl.BlockSpec(memory_space=pl.ANY)] * 5,
        out_specs=[block] * 3,
        scratch_shapes=[
            pltpu.VMEM((3, rows, width), f32), pltpu.VMEM((rows, width), jnp.int32),
            pltpu.SMEM(fold_map.shape, jnp.int32),
            pltpu.VMEM((3, tall, width), f32), pltpu.VMEM((3, tall, width), f32),
            *tile(rows)[:-1],
            *tile(seam_rows)[:-1],
            *tile(max(group_rows + 2 * MARGIN, 2 * BAND)),
            edge, edge, edge,
            pltpu.VMEM((2, group_rows, width), f32),
            pltpu.VMEM((2, 3 * LIP + 2 * STEPS, width), f32),
            pltpu.VMEM((2, group_rows, width), f32),
            pltpu.VMEM((n_lon, 32, width), f32),
            pltpu.VMEM((group_rows, width), f32),
            pltpu.VMEM((group_rows + 2 * LIP, width), f32),
            pltpu.VMEM((3 * LIP, width), f32),
            pltpu.VMEM((7 * LIP, width), f32),
            pltpu.VMEM((3, BAND, width), f32), pltpu.VMEM((3, BAND, width), f32),
            pltpu.VMEM((6 * STEPS, 8, width), f32),
            dma((3,)), dma((10,)), dma((11,)),
            *moment_refs,
        ],
        compiler_params=pltpu.CompilerParams(collective_id=0, has_side_effects=True),
        name="tripole_cg",
    )(forcing, search_direction, ocean_depth, land_mask, fold_map)
    wide_basis, seam_basis, sums = (
        pltpu.with_memory_space_constraint(out, pltpu.VMEM) for out in outs
    )
    return pl.pallas_call(
        finish,
        out_shape=[jax.ShapeDtypeStruct((rows, width), f32)] * 2,
        in_specs=[block] * 3,
        out_specs=[pl.BlockSpec(memory_space=pl.ANY)] * 2,
        scratch_shapes=[
            pltpu.VMEM((6 * STEPS, width), f32),
            pltpu.VMEM((2, seam_rows, width), f32),
            pltpu.VMEM((2, rows, width), f32),
            dma((2,)),
        ],
        name="finish",
    )(sums, wide_basis, seam_basis)


def solution(mesh):
    cells = P("lat", "lon")
    return jax.shard_map(
        functools.partial(per_device, mesh.shape["lat"], mesh.shape["lon"]),
        mesh=mesh,
        in_specs=(cells, cells, cells, cells, P()),
        out_specs=(cells, cells),
        check_vma=False,
    )
```
